8 devices in a mesh: dp: 1 (over z), tp: 8 (over y, x, core).
Axes of the slice: x: 2, y: 2, z: 1, core: 2. Of those that a mesh axis runs over, the one named last changes fastest.
Arguments:
- x_in: bfloat16 [2, 512, 2560], P(None, ('dp', 'tp'))
- y_cot: bfloat16 [2, 512, 2560], P(None, ('dp', 'tp'))
- gain_attn: float32 [2, 2560], replicated
- gain_mlp: float32 [2, 2560], replicated
- w_qkv: bfloat16 [2, 2560, 8, 6, 128], P(None, None, 'tp')
- w_out: bfloat16 [2, 32, 128, 2560], P(None, 'tp')
- w_gate: bfloat16 [2, 2560, 9728], P(None, None, 'tp')
- w_up: bfloat16 [2, 2560, 9728], P(None, None, 'tp')
- w_down: bfloat16 [2, 9728, 2560], P(None, 'tp')
Outputs:
- output 1: bfloat16 [2, 512, 2560], P(None, ('dp', 'tp'))
- output 2: bfloat16 [2, 512, 2560], P(None, ('dp', 'tp'))
- output 3: bfloat16 [2, 2560, 8, 6, 128], P('dp', None, 'tp')
- output 4: bfloat16 [2, 32, 128, 2560], P('dp', 'tp')
- output 5: bfloat16 [2, 2560, 9728], P('dp', None, 'tp')
- output 6: bfloat16 [2, 2560, 9728], P('dp', None, 'tp')
- output 7: bfloat16 [2, 9728, 2560], P('dp', 'tp')
- output 8: float32 [2, 2560], P('dp')
- output 9: float32 [2, 2560], P('dp')
All inputs are finite; a program needn't handle non-finite values.
Results may differ from the reference program's by a relative error of at most 0.02.
Values are sent between devices in bfloat16 or wider.
A program may use at most 1 GiB of HBM per device.

```python
import jax
import jax.numpy as jnp
from jax import lax

D = 2560
FF = 9728
HEADS = 32
KV_HEADS = 8
HEAD = 128
SEQ = 512
LAYERS = 2
MICRO = 2
GROUP = HEADS // KV_HEADS
NORM_EPS = 1e-5


def setup_inputs(seed: int = 0, part: int = 0) -> dict:
    base_key = jax.random.key(seed)
    shared_keys = jax.random.split(base_key, 7)
    part_keys = jax.random.split(jax.random.fold_in(base_key, part), 2)
    x_in = jax.random.normal(part_keys[0], (MICRO, SEQ, D), jnp.float32)
    y_cot = jax.random.normal(part_keys[1], (MICRO, SEQ, D), jnp.float32)
    gain_attn = 1.0 + 0.3 * jax.random.normal(shared_keys[0], (LAYERS, D), jnp.float32)
    gain_mlp = 1.0 + 0.3 * jax.random.normal(shared_keys[1], (LAYERS, D), jnp.float32)
    w_qkv = jax.random.normal(shared_keys[2], (LAYERS, D, KV_HEADS, GROUP + 2, HEAD), jnp.float32) * D ** -0.5
    w_out = jax.random.normal(shared_keys[3], (LAYERS, HEADS, HEAD, D), jnp.float32) * (HEADS * HEAD) ** -0.5
    w_gate = jax.random.normal(shared_keys[4], (LAYERS, D, FF), jnp.float32) * D ** -0.5
    w_up = jax.random.normal(shared_keys[5], (LAYERS, D, FF), jnp.float32) * D ** -0.5
    w_down = jax.random.normal(shared_keys[6], (LAYERS, FF, D), jnp.float32) * FF ** -0.5
    return {'x_in': x_in.astype(jnp.bfloat16), 'y_cot': y_cot.astype(jnp.bfloat16), 'gain_attn': gain_attn, 'gain_mlp': gain_mlp, 'w_qkv': w_qkv.astype(jnp.bfloat16), 'w_out': w_out.astype(jnp.bfloat16), 'w_gate': w_gate.astype(jnp.bfloat16), 'w_up': w_up.astype(jnp.bfloat16), 'w_down': w_down.astype(jnp.bfloat16)}


def rms_norm(row_vals, gain_vec):
    return row_vals * lax.rsqrt(jnp.mean(row_vals * row_vals, axis=-1, keepdims=True) + NORM_EPS) * gain_vec


def group_attention(queries, key_rows, value_rows):
    scores = jnp.einsum('qge,ke->gqk', queries.astype(jnp.float32), key_rows.astype(jnp.float32)) * HEAD ** -0.5
    positions = jnp.arange(SEQ)
    scores = jnp.where(positions[:, None] >= positions[None, :], scores, -1e30)
    prob_b16 = jax.nn.softmax(scores, axis=-1).astype(jnp.bfloat16)
    attn_mix = jnp.einsum('gqk,ke->qge', prob_b16.astype(jnp.float32), value_rows.astype(jnp.float32))
    return attn_mix.astype(jnp.bfloat16)


attention_ckpt = jax.checkpoint(group_attention)


def group_step(group_args):
    return attention_ckpt(group_args[0], group_args[1], group_args[2])


def layer_forward(layer_in, layer_params):
    gain_first, gain_second, qkv_weight, out_weight, gate_weight, up_weight, down_weight = layer_params
    x_f32 = layer_in.astype(jnp.float32)
    normed = rms_norm(x_f32, gain_first).astype(jnp.bfloat16)
    qkv_heads = jnp.einsum('sd,dkje->skje', normed.astype(jnp.float32), qkv_weight).astype(jnp.bfloat16)
    attn_mix = lax.map(group_step, (jnp.swapaxes(qkv_heads[:, :, :GROUP], 0, 1), jnp.swapaxes(qkv_heads[:, :, GROUP], 0, 1), jnp.swapaxes(qkv_heads[:, :, GROUP + 1], 0, 1)))
    attn_sum = jnp.einsum('kqge,kged->qd', attn_mix.astype(jnp.float32), out_weight.reshape(KV_HEADS, GROUP, HEAD, D))
    hidden = (x_f32 + attn_sum.astype(jnp.bfloat16).astype(jnp.float32)).astype(jnp.bfloat16)
    normed_b = rms_norm(hidden.astype(jnp.float32), gain_second).astype(jnp.bfloat16)
    gate_pre = jnp.dot(normed_b.astype(jnp.float32), gate_weight, preferred_element_type=jnp.float32)
    up_proj = jnp.dot(normed_b.astype(jnp.float32), up_weight, preferred_element_type=jnp.float32)
    inner = (jax.nn.silu(gate_pre) * up_proj).astype(jnp.bfloat16)
    down_sum = jnp.dot(inner.astype(jnp.float32), down_weight, preferred_element_type=jnp.float32).astype(jnp.bfloat16)
    return (hidden.astype(jnp.float32) + down_sum.astype(jnp.float32)).astype(jnp.bfloat16)


def stack_forward(layer_in, params):
    def layer_body(carry, layer_params):
        return layer_forward(carry, layer_params), None
    final_rows, unused = lax.scan(layer_body, layer_in, params)
    return final_rows


def reference(x_in, y_cot, gain_attn, gain_mlp, w_qkv, w_out, w_gate, w_up, w_down):
    params = (gain_attn, gain_mlp, w_qkv.astype(jnp.float32), w_out.astype(jnp.float32), w_gate.astype(jnp.float32), w_up.astype(jnp.float32), w_down.astype(jnp.float32))
    first_out, first_pull = jax.vjp(stack_forward, x_in[0], params)
    first_rows, first_grads = first_pull(y_cot[0])
    second_out, second_pull = jax.vjp(stack_forward, x_in[1], params)
    second_rows, second_grads = second_pull(y_cot[1])
    summed = [grad_one + grad_two for grad_one, grad_two in zip(first_grads, second_grads)]
    return (jnp.stack([first_out, second_out]), jnp.stack([first_rows, second_rows]), summed[2].astype(jnp.bfloat16), summed[3].astype(jnp.bfloat16), summed[4].astype(jnp.bfloat16), summed[5].astype(jnp.bfloat16), summed[6].astype(jnp.bfloat16), summed[0], summed[1])
```

```python
import functools

import jax
import jax.numpy as jnp
from jax import lax
from jax.experimental import pallas as pl
from jax.experimental.pallas import tpu as pltpu
from jax.sharding import PartitionSpec as P

NORM_EPS = 1e-5
BF = jnp.bfloat16
F32 = jnp.float32


def rms_scale(row_vals, gain_vec):
    return row_vals * lax.rsqrt(jnp.mean(row_vals * row_vals, axis=-1, keepdims=True) + NORM_EPS) * gain_vec


def norm_apply(row_vals, gain_vec):
    return rms_scale(row_vals.astype(F32), gain_vec).astype(BF)


def norm_backward(row_vals, gain_vec, cot_rows):
    unused, pull = jax.vjp(rms_scale, row_vals.astype(F32), gain_vec)
    return pull(cot_rows.astype(F32))


def block_probs(qkv_ref, blk, rows, groups, hd, scale):
    limit = (blk + 1) * rows
    span = pl.ds(blk * rows, rows)
    q = jnp.concatenate([qkv_ref[span, j * hd:(j + 1) * hd] for j in range(groups)], axis=0)
    k = qkv_ref[0:limit, groups * hd:(groups + 1) * hd]
    s = lax.dot_general(q, k, (((1,), (1,)), ((), ())), preferred_element_type=F32) * scale
    row_pos = lax.rem(lax.broadcasted_iota(jnp.int32, s.shape, 0), rows) + blk * rows
    col_pos = lax.broadcasted_iota(jnp.int32, s.shape, 1)
    s = jnp.where(row_pos >= col_pos, s, -1e30)
    e = jnp.exp(s - jnp.max(s, axis=-1, keepdims=True))
    p = e * (1.0 / jnp.sum(e, axis=-1, keepdims=True))
    return q, k, p, limit, span


def attn_fwd_kernel(qkv_ref, o_ref, *, rows, groups, hd, scale):
    seq = qkv_ref.shape[0]
    for blk in range(seq // rows):
        q, k, p, limit, span = block_probs(qkv_ref, blk, rows, groups, hd, scale)
        v = qkv_ref[0:limit, (groups + 1) * hd:(groups + 2) * hd]
        o = jnp.dot(p.astype(BF), v, preferred_element_type=F32).astype(BF)
        for j in range(groups):
            o_ref[span, j * hd:(j + 1) * hd] = o[j * rows:(j + 1) * rows]


def attn_bwd_kernel(qkv_ref, do_ref, out_ref, dk_ref, dv_ref, *, rows, groups, hd, scale):
    seq = qkv_ref.shape[0]
    blocks = seq // rows
    for blk in reversed(range(blocks)):
        q, k, p, limit, span = block_probs(qkv_ref, blk, rows, groups, hd, scale)
        v = qkv_ref[0:limit, (groups + 1) * hd:(groups + 2) * hd]
        do = jnp.concatenate([do_ref[span, j * hd:(j + 1) * hd] for j in range(groups)], axis=0)
        dp = lax.dot_general(do, v, (((1,), (1,)), ((), ())), preferred_element_type=F32).astype(BF).astype(F32)
        row_dot = jnp.sum(dp * p, axis=-1, keepdims=True)
        ds = (p * (dp - row_dot) * scale).astype(BF)
        dq = jnp.dot(ds, k, preferred_element_type=F32).astype(BF)
        for j in range(groups):
            out_ref[span, j * hd:(j + 1) * hd] = dq[j * rows:(j + 1) * rows]
        dk = lax.dot_general(ds, q, (((0,), (0,)), ((), ())), preferred_element_type=F32)
        dv = lax.dot_general(p.astype(BF), do, (((0,), (0,)), ((), ())), preferred_element_type=F32)
        if blk == blocks - 1:
            dk_ref[...] = dk
            dv_ref[...] = dv
        else:
            dk_ref[0:limit] += dk
            dv_ref[0:limit] += dv
    out_ref[:, groups * hd:(groups + 1) * hd] = dk_ref[...].astype(BF)
    out_ref[:, (groups + 1) * hd:(groups + 2) * hd] = dv_ref[...].astype(BF)


def attention_forward(qkv, groups, hd):
    seq = qkv.shape[0]
    rows = min(128, seq)
    return pl.pallas_call(
        functools.partial(attn_fwd_kernel, rows=rows, groups=groups, hd=hd, scale=hd ** -0.5),
        out_shape=jax.ShapeDtypeStruct((seq, groups * hd), BF),
        in_specs=[pl.BlockSpec(memory_space=pltpu.VMEM)],
        out_specs=pl.BlockSpec(memory_space=pltpu.VMEM),
        name='attn_fwd',
        cost_estimate=pl.CostEstimate(flops=3 * 2 * groups * seq * seq * hd, bytes_accessed=2 * qkv.size, transcendentals=groups * seq * seq),
    )(qkv)


def attention_backward(qkv, grad_mix, groups, hd):
    seq = qkv.shape[0]
    rows = min(128, seq)
    return pl.pallas_call(
        functools.partial(attn_bwd_kernel, rows=rows, groups=groups, hd=hd, scale=hd ** -0.5),
        out_shape=jax.ShapeDtypeStruct(qkv.shape, BF),
        in_specs=[pl.BlockSpec(memory_space=pltpu.VMEM)] * 2,
        out_specs=pl.BlockSpec(memory_space=pltpu.VMEM),
        scratch_shapes=[pltpu.VMEM((seq, hd), F32), pltpu.VMEM((seq, hd), F32)],
        name='attn_bwd',
        cost_estimate=pl.CostEstimate(flops=6 * 2 * groups * seq * seq * hd, bytes_accessed=2 * qkv.size, transcendentals=groups * seq * seq),
    )(qkv, grad_mix)


def weight_grad_kernel(*refs, micro_count):
    out_ref = refs[-1]
    total = None
    for m in range(micro_count):
        term = lax.dot_general(refs[m][...], refs[micro_count + m][...], (((0,), (0,)), ((), ())), preferred_element_type=F32)
        total = term if total is None else total + term
    out_ref[0] = total.astype(BF)


def weight_grad(lefts, rights, stacked, layer_idx, layer_count, tile=256):
    micro_count = len(lefts)
    seq, rows = lefts[0].shape
    cols = rights[0].shape[1]
    whole_left, whole_right = pl.BlockSpec((seq, rows), lambda i: (0, 0)), pl.BlockSpec((seq, cols), lambda i: (0, 0))
    part = pl.BlockSpec((seq, tile), lambda i: (0, i))
    if rows % tile == 0:
        in_specs = [part] * micro_count + [whole_right] * micro_count
        steps, out_spec = rows // tile, pl.BlockSpec((1, tile, cols), lambda i: (layer_idx, i, 0))
    else:
        in_specs = [whole_left] * micro_count + [part] * micro_count
        steps, out_spec = cols // tile, pl.BlockSpec((1, rows, tile), lambda i: (layer_idx, 0, i))
    args = list(lefts) + list(rights)
    aliases = {}
    if stacked is not None:
        in_specs.append(pl.BlockSpec(memory_space=pl.ANY))
        aliases = {len(args): 0}
        args.append(stacked)
    return pl.pallas_call(
        functools.partial(weight_grad_kernel, micro_count=micro_count),
        grid=(steps,),
        out_shape=jax.ShapeDtypeStruct((layer_count, rows, cols), BF),
        in_specs=in_specs,
        out_specs=out_spec,
        input_output_aliases=aliases,
        name='weight_grad',
        cost_estimate=pl.CostEstimate(flops=2 * micro_count * seq * rows * cols, bytes_accessed=2 * (micro_count * seq * (rows + cols) + rows * cols), transcendentals=0),
    )(*args)


def solution(mesh):
    row_spec = P(None, ('dp', 'tp'), None)
    gain_spec = P(None, None)
    qkv_spec = P(None, None, 'tp', None, None)
    head_spec = P(None, 'tp', None, None)
    col_spec = P(None, None, 'tp')
    row_shard_spec = P(None, 'tp', None)
    tp = mesh.shape['tp']
    swap = {flip: [(t, t ^ flip) for t in range(tp)] for flip in (1, 2, 4)}

    def device_program(x_in, y_cot, gain_attn, gain_mlp, w_qkv, w_out, w_gate, w_up, w_down):
        micro_count, shard, width = x_in.shape
        layer_count = w_qkv.shape[0]
        groups = w_qkv.shape[3] - 2
        hd = w_qkv.shape[4]
        half = width // 2
        me = lax.axis_index('tp')
        core, xpos, ypos = me % 2, (me // 2) % 2, me // 4
        wq = [w_qkv[l].reshape(width, (groups + 2) * hd) for l in range(layer_count)]
        wo = [w_out[l].reshape(groups * hd, width) for l in range(layer_count)]

        def pick(arr, idx, axis):
            return lax.dynamic_index_in_dim(arr, idx, axis, keepdims=False)

        def gather(rows):
            return lax.all_gather(rows, 'tp', axis=0, tiled=True)

        def scatter_product(lefts, product):
            def rows_of(which):
                return [pick(a.reshape(tp // 2, 2, shard, a.shape[-1]), which, 1).reshape(tp // 2 * shard, a.shape[-1]) for a in lefts]
            away = lax.ppermute(product(*rows_of(1 - core)), 'tp', swap[1]).reshape(2, 2, shard, width)
            keep = product(*rows_of(core)).reshape(2, 2, shard, width)

            def chip_a(which):
                return pick(keep[..., :half], which, 1) + pick(away[..., :half], which, 1)

            def chip_b(which):
                return pick(keep[..., half:], which, 0) + pick(away[..., half:], which, 0)
            got_a = lax.ppermute(chip_a(1 - xpos), 'tp', swap[2])
            got_b = lax.ppermute(chip_b(1 - ypos), 'tp', swap[4])
            two_a = chip_a(xpos) + got_a
            two_b = chip_b(ypos) + got_b
            last_a = lax.ppermute(pick(two_a, 1 - ypos, 0), 'tp', swap[4])
            last_b = lax.ppermute(pick(two_b, 1 - xpos, 0), 'tp', swap[2])
            return jnp.concatenate([pick(two_a, ypos, 0) + last_a, pick(two_b, xpos, 0) + last_b], axis=-1).astype(BF)

        def mm(a, b):
            return jnp.dot(a, b, preferred_element_type=F32)

        def mm_t(a, b):
            return lax.dot_general(a, b, (((1,), (1,)), ((), ())), preferred_element_type=F32)

        kept = [[None] * layer_count for m in range(micro_count)]
        layer_in = [x_in[m] for m in range(micro_count)]
        for l in range(layer_count):
            for m in range(micro_count):
                u_full = gather(norm_apply(layer_in[m], gain_attn[l]))
                qkv = mm(u_full, wq[l]).astype(BF)
                mix = attention_forward(qkv, groups, hd)
                attn_sum = scatter_product([mix], lambda a: mm(a, wo[l]))
                hidden = (layer_in[m].astype(F32) + attn_sum.astype(F32)).astype(BF)
                kept[m][l] = [layer_in[m], u_full, qkv, mix, hidden]
            for m in range(micro_count):
                hidden = kept[m][l][4]
                v_full = gather(norm_apply(hidden, gain_mlp[l]))
                gate_pre = mm(v_full, w_gate[l])
                up_proj = mm(v_full, w_up[l])
                inner = (jax.nn.silu(gate_pre) * up_proj).astype(BF)
                mlp_sum = scatter_product([inner], lambda a: mm(a, w_down[l]))
                kept[m][l] += [v_full, gate_pre, up_proj, inner]
                layer_in[m] = (hidden.astype(F32) + mlp_sum.astype(F32)).astype(BF)
        y_rows = layer_in

        stacks = [None] * 5
        gains_a, gains_b = [None] * layer_count, [None] * layer_count
        grad_in = [y_cot[m] for m in range(micro_count)]
        for l in reversed(range(layer_count)):
            grads = [None] * micro_count
            for m in range(micro_count):
                x_rows, u_full, qkv, mix, hidden, v_full, gate_pre, up_proj, inner = kept[m][l]
                gy_full = gather(grad_in[m])
                gate_sig = jax.nn.sigmoid(gate_pre)
                gate_act = gate_pre * gate_sig
                grad_inner = mm_t(gy_full, w_down[l]).astype(BF).astype(F32)
                grad_up = (grad_inner * gate_act).astype(BF)
                grad_gate = (grad_inner * up_proj * gate_sig * (1.0 + gate_pre * (1.0 - gate_sig))).astype(BF)
                grad_nb = scatter_product([grad_gate, grad_up], lambda a, b: mm_t(a, w_gate[l]) + mm_t(b, w_up[l]))
                grad_norm, gain_part = norm_backward(hidden, gain_mlp[l], grad_nb)
                gains_b[l] = gain_part if m == 0 else gains_b[l] + gain_part
                grad_hidden = (grad_in[m].astype(F32) + grad_norm).astype(BF)
                grads[m] = [gy_full, grad_up, grad_gate, grad_hidden]
            stacks[2] = weight_grad([kept[m][l][5] for m in range(micro_count)], [grads[m][2] for m in range(micro_count)], stacks[2], l, layer_count)
            stacks[3] = weight_grad([kept[m][l][5] for m in range(micro_count)], [grads[m][1] for m in range(micro_count)], stacks[3], l, layer_count)
            stacks[4] = weight_grad([kept[m][l][8] for m in range(micro_count)], [grads[m][0] for m in range(micro_count)], stacks[4], l, layer_count)
            for m in range(micro_count):
                x_rows, u_full, qkv, mix = kept[m][l][:4]
                grad_hidden = grads[m][3]
                gh_full = gather(grad_hidden)
                grad_mix = mm_t(gh_full, wo[l]).astype(BF)
                grad_qkv = attention_backward(qkv, grad_mix, groups, hd)
                grad_n = scatter_product([grad_qkv], lambda a: mm_t(a, wq[l]))
                grad_norm, gain_part = norm_backward(x_rows, gain_attn[l], grad_n)
                gains_a[l] = gain_part if m == 0 else gains_a[l] + gain_part
                grad_in[m] = (grad_hidden.astype(F32) + grad_norm).astype(BF)
                grads[m] += [gh_full, grad_qkv]
            stacks[1] = weight_grad([kept[m][l][3] for m in range(micro_count)], [grads[m][4] for m in range(micro_count)], stacks[1], l, layer_count)
            stacks[0] = weight_grad([kept[m][l][1] for m in range(micro_count)], [grads[m][5] for m in range(micro_count)], stacks[0], l, layer_count)

        def sum_all(vec):
            for flip in (1, 2, 4):
                vec = vec + lax.ppermute(vec, 'tp', swap[flip])
            return vec
        early = sum_all(jnp.stack(gains_b + gains_a[1:]))
        last = sum_all(gains_a[0][None])
        gain_a = jnp.concatenate([last, early[layer_count:]])
        gain_b = early[:layer_count]
        return (jnp.stack(y_rows), jnp.stack(grad_in), stacks[0].reshape(w_qkv.shape), stacks[1].reshape(w_out.shape),
                stacks[2], stacks[3], stacks[4], gain_a, gain_b)

    return jax.shard_map(device_program, mesh=mesh,
                         in_specs=(row_spec, row_spec, gain_spec, gain_spec, qkv_spec, head_spec, col_spec, col_spec, row_shard_spec),
                         out_specs=(row_spec, row_spec, P('dp', None, 'tp', None, None), P('dp', 'tp', None, None), P('dp', None, 'tp'), P('dp', None, 'tp'), P('dp', 'tp', None), P('dp', None), P('dp', None)),
                         check_vma=False)
```

```python
import functools

import jax
import jax.numpy as jnp
from jax import lax
from jax.experimental import pallas as pl
from jax.experimental.pallas import tpu as pltpu
from jax.sharding import PartitionSpec as P

NORM_EPS = 1e-5
BF = jnp.bfloat16
F32 = jnp.float32


def rms_scale(row_vals, gain_vec):
    return row_vals * lax.rsqrt(jnp.mean(row_vals * row_vals, axis=-1, keepdims=True) + NORM_EPS) * gain_vec


def norm_apply(row_vals, gain_vec):
    return rms_scale(row_vals.astype(F32), gain_vec).astype(BF)


def norm_backward(row_vals, gain_vec, cot_rows):
    unused, pull = jax.vjp(rms_scale, row_vals.astype(F32), gain_vec)
    return pull(cot_rows.astype(F32))


def block_probs(qkv_ref, blk, rows, groups, hd, scale):
    limit = (blk + 1) * rows
    span = pl.ds(blk * rows, rows)
    q = jnp.concatenate([qkv_ref[span, j * hd:(j + 1) * hd] for j in range(groups)], axis=0)
    k = qkv_ref[0:limit, groups * hd:(groups + 1) * hd]
    s = lax.dot_general(q, k, (((1,), (1,)), ((), ())), preferred_element_type=F32) * scale
    row_pos = lax.rem(lax.broadcasted_iota(jnp.int32, s.shape, 0), rows) + blk * rows
    col_pos = lax.broadcasted_iota(jnp.int32, s.shape, 1)
    s = jnp.where(row_pos >= col_pos, s, -1e30)
    e = jnp.exp(s - jnp.max(s, axis=-1, keepdims=True))
    p = e * (1.0 / jnp.sum(e, axis=-1, keepdims=True))
    return q, k, p, limit, span


def attn_fwd_kernel(qkv_ref, o_ref, *, rows, groups, hd, scale):
    seq = qkv_ref.shape[0]
    for blk in range(seq // rows):
        q, k, p, limit, span = block_probs(qkv_ref, blk, rows, groups, hd, scale)
        v = qkv_ref[0:limit, (groups + 1) * hd:(groups + 2) * hd]
        o = jnp.dot(p.astype(BF), v, preferred_element_type=F32).astype(BF)
        for j in range(groups):
            o_ref[span, j * hd:(j + 1) * hd] = o[j * rows:(j + 1) * rows]


def attn_bwd_kernel(qkv_ref, do_ref, out_ref, dk_ref, dv_ref, *, rows, groups, hd, scale):
    seq = qkv_ref.shape[0]
    blocks = seq // rows
    for blk in reversed(range(blocks)):
        q, k, p, limit, span = block_probs(qkv_ref, blk, rows, groups, hd, scale)
        v = qkv_ref[0:limit, (groups + 1) * hd:(groups + 2) * hd]
        do = jnp.concatenate([do_ref[span, j * hd:(j + 1) * hd] for j in range(groups)], axis=0)
        dp = lax.dot_general(do, v, (((1,), (1,)), ((), ())), preferred_element_type=F32).astype(BF).astype(F32)
        row_dot = jnp.sum(dp * p, axis=-1, keepdims=True)
        ds = (p * (dp - row_dot) * scale).astype(BF)
        dq = jnp.dot(ds, k, preferred_element_type=F32).astype(BF)
        for j in range(groups):
            out_ref[span, j * hd:(j + 1) * hd] = dq[j * rows:(j + 1) * rows]
        dk = lax.dot_general(ds, q, (((0,), (0,)), ((), ())), preferred_element_type=F32)
        dv = lax.dot_general(p.astype(BF), do, (((0,), (0,)), ((), ())), preferred_element_type=F32)
        if blk == blocks - 1:
            dk_ref[...] = dk
            dv_ref[...] = dv
        else:
            dk_ref[0:limit] += dk
            dv_ref[0:limit] += dv
    out_ref[:, groups * hd:(groups + 1) * hd] = dk_ref[...].astype(BF)
    out_ref[:, (groups + 1) * hd:(groups + 2) * hd] = dv_ref[...].astype(BF)


def attention_forward(qkv, groups, hd):
    seq = qkv.shape[0]
    rows = min(128, seq)
    return pl.pallas_call(
        functools.partial(attn_fwd_kernel, rows=rows, groups=groups, hd=hd, scale=hd ** -0.5),
        out_shape=jax.ShapeDtypeStruct((seq, groups * hd), BF),
        in_specs=[pl.BlockSpec(memory_space=pltpu.VMEM)],
        out_specs=pl.BlockSpec(memory_space=pltpu.VMEM),
        name='attn_fwd',
        cost_estimate=pl.CostEstimate(flops=3 * 2 * groups * seq * seq * hd, bytes_accessed=2 * qkv.size, transcendentals=groups * seq * seq),
    )(qkv)


def attention_backward(qkv, grad_mix, groups, hd):
    seq = qkv.shape[0]
    rows = min(128, seq)
    return pl.pallas_call(
        functools.partial(attn_bwd_kernel, rows=rows, groups=groups, hd=hd, scale=hd ** -0.5),
        out_shape=jax.ShapeDtypeStruct(qkv.shape, BF),
        in_specs=[pl.BlockSpec(memory_space=pltpu.VMEM)] * 2,
        out_specs=pl.BlockSpec(memory_space=pltpu.VMEM),
        scratch_shapes=[pltpu.VMEM((seq, hd), F32), pltpu.VMEM((seq, hd), F32)],
        name='attn_bwd',
        cost_estimate=pl.CostEstimate(flops=6 * 2 * groups * seq * seq * hd, bytes_accessed=2 * qkv.size, transcendentals=groups * seq * seq),
    )(qkv, grad_mix)


def weight_grad_kernel(*refs, micro_count, slots):
    out_ref = refs[-1]
    total = None
    for m in range(micro_count):
        term = lax.dot_general(refs[m][...], refs[micro_count + m][...], (((0,), (0,)), ((), ())), preferred_element_type=F32)
        total = term if total is None else total + term
    if slots:
        hd = total.shape[1] // slots
        for j in range(slots):
            out_ref[0, j] = total[:, j * hd:(j + 1) * hd].astype(BF)
    else:
        out_ref[0] = total.astype(BF)


def weight_grad(lefts, rights, stacked, layer_idx, layer_count, slots=0, tile=256):
    micro_count = len(lefts)
    seq, rows = lefts[0].shape
    cols = rights[0].shape[1]
    whole_left, whole_right = pl.BlockSpec((seq, rows), lambda i: (0, 0)), pl.BlockSpec((seq, cols), lambda i: (0, 0))
    part = pl.BlockSpec((seq, tile), lambda i: (0, i))
    if rows % tile == 0:
        in_specs = [part] * micro_count + [whole_right] * micro_count
        steps, out_spec = rows // tile, pl.BlockSpec((1, tile, cols), lambda i: (layer_idx, i, 0))
    else:
        in_specs = [whole_left] * micro_count + [part] * micro_count
        steps, out_spec = cols // tile, pl.BlockSpec((1, rows, tile), lambda i: (layer_idx, 0, i))
    args = list(lefts) + list(rights)
    aliases = {}
    shape = (layer_count, rows, cols)
    if slots:
        shape = (layer_count, slots, rows, cols // slots)
        out_spec = pl.BlockSpec((1, slots, tile, cols // slots), lambda i: (layer_idx, 0, i, 0))
    if stacked is not None:
        in_specs.append(pl.BlockSpec(memory_space=pl.ANY))
        aliases = {len(args): 0}
        args.append(stacked)
    return pl.pallas_call(
        functools.partial(weight_grad_kernel, micro_count=micro_count, slots=slots),
        grid=(steps,),
        out_shape=jax.ShapeDtypeStruct(shape, BF),
        in_specs=in_specs,
        out_specs=out_spec,
        input_output_aliases=aliases,
        name='weight_grad',
        cost_estimate=pl.CostEstimate(flops=2 * micro_count * seq * rows * cols, bytes_accessed=2 * (micro_count * seq * (rows + cols) + rows * cols), transcendentals=0),
    )(*args)


def product_scatter_kernel(*refs, left_count, slots, shard, tile, steps):
    lefts, weights = refs[:left_count], refs[left_count:3 * left_count]
    out_ref = refs[3 * left_count]
    rest = refs[3 * left_count + 1:]
    sorted_refs = rest[:left_count]
    acc, send1, recv1, send2, recv2, send3, recv3, sem = rest[left_count:]
    step = pl.program_id(0)
    me = lax.axis_index('tp')
    core, xpos, ypos = lax.rem(me, 2), lax.rem(me // 2, 2), me // 4
    pair, xpeer, ypeer = me + 1 - 2 * core, me + 2 - 4 * xpos, me + 4 - 8 * ypos
    first, second = (xpeer, ypeer), (ypeer, xpeer)

    def copy(stage, side, g):
        src, dst, to = ((send1, recv1, pair), (send2, recv2, first[side]), (send3, recv3, second[side]))[stage]
        return pltpu.make_async_remote_copy(src_ref=src.at[side, g], dst_ref=dst.at[side, g], send_sem=sem.at[2 * stage, side, g],
                                            recv_sem=sem.at[2 * stage + 1, side, g], device_id={'tp': to},
                                            device_id_type=pl.DeviceIdType.MESH)

    def chip(side, mine, other):
        return other * 2 + mine if side == 0 else mine * 2 + other
    here = ((xpos, ypos), (ypos, xpos))

    @pl.when(step == 0)
    def _():
        barrier = pltpu.get_barrier_semaphore()
        for peer in (pair, xpeer, ypeer):
            pl.semaphore_signal(barrier, inc=1, device_id={'tp': peer}, device_id_type=pl.DeviceIdType.MESH)
        for i in range(left_count):
            for c in range(4):
                for part, which in ((0, 1 - core), (1, core)):
                    start = pl.multiple_of(c * 2 * shard + which * shard, shard)
                    sorted_refs[i][(part * 4 + c) * shard:(part * 4 + c + 1) * shard, :] = lefts[i][pl.ds(start, shard), :]
        pl.semaphore_wait(barrier, 3)

    for side in range(2):
        total = None
        for i in range(left_count):
            w_ref = weights[2 * i + side]
            if slots:
                w = jnp.concatenate([w_ref[0, j] for j in range(slots)], axis=1)
                term = lax.dot_general(sorted_refs[i][...], w, (((1,), (1,)), ((), ())), preferred_element_type=F32)
            else:
                term = jnp.dot(sorted_refs[i][...], w_ref[0], preferred_element_type=F32)
            total = term if total is None else total + term
        for c in range(4):
            send1[side, step, c] = total[c * shard:(c + 1) * shard]
            acc[side, step, c] = total[(4 + c) * shard:(5 + c) * shard]
        copy(0, side, step).start()

    def chip_sum(g):
        for side in range(2):
            copy(0, side, g).wait_recv()
            mine = here[side][0]
            for other in range(2):
                away, keep = chip(side, 1 - mine, other), chip(side, mine, other)
                send2[side, g, other] = acc[side, g, away] + recv1[side, g, away]
                acc[side, g, keep] = acc[side, g, keep] + recv1[side, g, keep]
            copy(1, side, g).start()

    @pl.when(step > 0)
    def _():
        chip_sum(step - 1)

    @pl.when(step == steps - 1)
    def _():
        chip_sum(steps - 1)
        for g in range(steps):
            for side in range(2):
                copy(1, side, g).wait_recv()
                mine, other = here[side]
                send3[side, g] = acc[side, g, chip(side, mine, 1 - other)] + recv2[side, g, 1 - other]
                acc[side, g, chip(side, mine, other)] = acc[side, g, chip(side, mine, other)] + recv2[side, g, other]
                copy(2, side, g).start()
        for g in range(steps):
            for side in range(2):
                copy(2, side, g).wait_recv()
                mine, other = here[side]
                col = (side * steps + g) * tile
                out_ref[:, col:col + tile] = (acc[side, g, chip(side, mine, other)] + recv3[side, g]).astype(BF)
        for stage in range(3):
            for g in range(steps):
                for side in range(2):
                    copy(stage, side, g).wait_send()


def product_scatter(lefts, weights, layer_idx, shard, call_id, slots=0, tile=256):
    seq = lefts[0].shape[0]
    width = weights[0].shape[2]
    steps = width // tile // 2
    in_specs = [pl.BlockSpec(a.shape, lambda i: (0, 0)) for a in lefts]
    args = list(lefts)
    for w in weights:
        for side in range(2):
            if slots:
                in_specs.append(pl.BlockSpec((1, slots, tile, w.shape[3]), lambda i, s=side: (layer_idx, 0, s * steps + i, 0)))
            else:
                in_specs.append(pl.BlockSpec((1, w.shape[1], tile), lambda i, s=side: (layer_idx, 0, s * steps + i)))
            args.append(w)
    depth = sum(a.shape[1] for a in lefts)
    return pl.pallas_call(
        functools.partial(product_scatter_kernel, left_count=len(lefts), slots=slots, shard=shard, tile=tile, steps=steps),
        grid=(steps,),
        out_shape=jax.ShapeDtypeStruct((shard, width), BF),
        in_specs=in_specs,
        out_specs=pl.BlockSpec((shard, width), lambda i: (0, 0)),
        scratch_shapes=[pltpu.VMEM(a.shape, BF) for a in lefts] + [
            pltpu.VMEM((2, steps, 4, shard, tile), F32),
            pltpu.VMEM((2, steps, 4, shard, tile), F32),
            pltpu.VMEM((2, steps, 4, shard, tile), F32),
            pltpu.VMEM((2, steps, 2, shard, tile), F32),
            pltpu.VMEM((2, steps, 2, shard, tile), F32),
            pltpu.VMEM((2, steps, shard, tile), F32),
            pltpu.VMEM((2, steps, shard, tile), F32),
            pltpu.SemaphoreType.DMA((6, 2, steps)),
        ],
        compiler_params=pltpu.CompilerParams(collective_id=call_id, has_side_effects=True),
        name='product_scatter',
        cost_estimate=pl.CostEstimate(flops=24 * 2 * seq * 2560 * 512, bytes_accessed=2 * depth * width, transcendentals=0),
    )(*args)


def solution(mesh):
    row_spec = P(None, ('dp', 'tp'), None)
    gain_spec = P(None, None)
    qkv_spec = P(None, None, 'tp', None, None)
    head_spec = P(None, 'tp', None, None)
    col_spec = P(None, None, 'tp')
    row_shard_spec = P(None, 'tp', None)
    tp = mesh.shape['tp']
    swap = {flip: [(t, t ^ flip) for t in range(tp)] for flip in (1, 2, 4)}

    def device_program(x_in, y_cot, gain_attn, gain_mlp, w_qkv, w_out, w_gate, w_up, w_down):
        micro_count, shard, width = x_in.shape
        layer_count = w_qkv.shape[0]
        groups = w_qkv.shape[3] - 2
        hd = w_qkv.shape[4]
        slots = groups + 2
        wq = jnp.transpose(w_qkv[:, :, 0], (0, 2, 1, 3))
        wo = w_out.reshape(layer_count, groups * hd, width)
        wg, wu = jnp.swapaxes(w_gate, 1, 2), jnp.swapaxes(w_up, 1, 2)

        def gather(rows):
            return lax.all_gather(rows, 'tp', axis=0, tiled=True)
        calls = iter(range(1, 100))

        def scatter_product(lefts, weights, layer_idx, slots=0):
            return product_scatter(lefts, weights, layer_idx, shard, next(calls), slots=slots)

        def mm_t(a, b):
            return lax.dot_general(a, b, (((1,), (1,)), ((), ())), preferred_element_type=F32)

        kept = [[None] * layer_count for m in range(micro_count)]
        layer_in = [x_in[m] for m in range(micro_count)]
        for l in range(layer_count):
            for m in range(micro_count):
                u_full = gather(norm_apply(layer_in[m], gain_attn[l]))
                qkv = jnp.einsum('sd,jde->sje', u_full, wq[l], preferred_element_type=F32).astype(BF).reshape(-1, slots * hd)
                mix = attention_forward(qkv, groups, hd)
                attn_sum = scatter_product([mix], [wo], l)
                hidden = (layer_in[m].astype(F32) + attn_sum.astype(F32)).astype(BF)
                kept[m][l] = [layer_in[m], u_full, qkv, mix, hidden]
            for m in range(micro_count):
                hidden = kept[m][l][4]
                v_full = gather(norm_apply(hidden, gain_mlp[l]))
                gate_pre = mm_t(v_full, wg[l])
                up_proj = mm_t(v_full, wu[l])
                inner = (jax.nn.silu(gate_pre) * up_proj).astype(BF)
                mlp_sum = scatter_product([inner], [w_down], l)
                kept[m][l] += [v_full, gate_pre, up_proj, inner]
                layer_in[m] = (hidden.astype(F32) + mlp_sum.astype(F32)).astype(BF)
        y_rows = layer_in

        stacks = [None] * 5
        gains_a, gains_b = [None] * layer_count, [None] * layer_count
        grad_in = [y_cot[m] for m in range(micro_count)]
        for l in reversed(range(layer_count)):
            grads = [None] * micro_count
            for m in range(micro_count):
                x_rows, u_full, qkv, mix, hidden, v_full, gate_pre, up_proj, inner = kept[m][l]
                gy_full = gather(grad_in[m])
                gate_sig = jax.nn.sigmoid(gate_pre)
                gate_act = gate_pre * gate_sig
                grad_inner = mm_t(gy_full, w_down[l]).astype(BF).astype(F32)
                grad_up = (grad_inner * gate_act).astype(BF)
                grad_gate = (grad_inner * up_proj * gate_sig * (1.0 + gate_pre * (1.0 - gate_sig))).astype(BF)
                grad_nb = scatter_product([grad_gate, grad_up], [wg, wu], l)
                grad_norm, gain_part = norm_backward(hidden, gain_mlp[l], grad_nb)
                gains_b[l] = gain_part if m == 0 else gains_b[l] + gain_part
                grad_hidden = (grad_in[m].astype(F32) + grad_norm).astype(BF)
                grads[m] = [gy_full, grad_up, grad_gate, grad_hidden]
            stacks[2] = weight_grad([grads[m][2] for m in range(micro_count)], [kept[m][l][5] for m in range(micro_count)], stacks[2], l, layer_count)
            stacks[3] = weight_grad([grads[m][1] for m in range(micro_count)], [kept[m][l][5] for m in range(micro_count)], stacks[3], l, layer_count)
            stacks[4] = weight_grad([kept[m][l][8] for m in range(micro_count)], [grads[m][0] for m in range(micro_count)], stacks[4], l, layer_count)
            for m in range(micro_count):
                x_rows, u_full, qkv, mix = kept[m][l][:4]
                grad_hidden = grads[m][3]
                gh_full = gather(grad_hidden)
                grad_mix = mm_t(gh_full, wo[l]).astype(BF)
                grad_qkv = attention_backward(qkv, grad_mix, groups, hd)
                grad_n = scatter_product([grad_qkv], [wq], l, slots)
                grad_norm, gain_part = norm_backward(x_rows, gain_attn[l], grad_n)
                gains_a[l] = gain_part if m == 0 else gains_a[l] + gain_part
                grad_in[m] = (grad_hidden.astype(F32) + grad_norm).astype(BF)
                grads[m] += [gh_full, grad_qkv]
            stacks[1] = weight_grad([kept[m][l][3] for m in range(micro_count)], [grads[m][4] for m in range(micro_count)], stacks[1], l, layer_count)
            stacks[0] = weight_grad([kept[m][l][1] for m in range(micro_count)], [grads[m][5] for m in range(micro_count)], stacks[0], l, layer_count, slots)

        def sum_all(vec):
            for flip in (1, 2, 4):
                vec = vec + lax.ppermute(vec, 'tp', swap[flip])
            return vec
        gains = sum_all(jnp.stack([jnp.stack(gains_a), jnp.stack(gains_b)]))
        return (jnp.stack(y_rows), jnp.stack(grad_in), jnp.transpose(stacks[0], (0, 2, 1, 3))[:, :, None], stacks[1].reshape(w_out.shape),
                jnp.swapaxes(stacks[2], 1, 2), jnp.swapaxes(stacks[3], 1, 2), stacks[4], gains[0], gains[1])

    return jax.shard_map(device_program, mesh=mesh,
                         in_specs=(row_spec, row_spec, gain_spec, gain_spec, qkv_spec, head_spec, col_spec, col_spec, row_shard_spec),
                         out_specs=(row_spec, row_spec, P('dp', None, 'tp', None, None), P('dp', 'tp', None, None), P('dp', None, 'tp'), P('dp', None, 'tp'), P('dp', 'tp', None), P('dp', None), P('dp', None)),
                         check_vma=False)
```

```python
import functools

import jax
import jax.numpy as jnp
from jax import lax
from jax.experimental import pallas as pl
from jax.experimental.pallas import tpu as pltpu
from jax.sharding import PartitionSpec as P

NORM_EPS = 1e-5
BF = jnp.bfloat16
F32 = jnp.float32


def rms_scale(row_vals, gain_vec):
    return row_vals * lax.rsqrt(jnp.mean(row_vals * row_vals, axis=-1, keepdims=True) + NORM_EPS) * gain_vec


def norm_apply(row_vals, gain_vec):
    return rms_scale(row_vals.astype(F32), gain_vec).astype(BF)


def norm_backward(row_vals, gain_vec, cot_rows):
    unused, pull = jax.vjp(rms_scale, row_vals.astype(F32), gain_vec)
    return pull(cot_rows.astype(F32))


def block_probs(qkv_ref, blk, rows, groups, hd, scale):
    limit = (blk + 1) * rows
    span = pl.ds(blk * rows, rows)
    q = jnp.concatenate([qkv_ref[span, j * hd:(j + 1) * hd] for j in range(groups)], axis=0)
    k = qkv_ref[0:limit, groups * hd:(groups + 1) * hd]
    s = lax.dot_general(q, k, (((1,), (1,)), ((), ())), preferred_element_type=F32) * scale
    row_pos = lax.rem(lax.broadcasted_iota(jnp.int32, s.shape, 0), rows) + blk * rows
    col_pos = lax.broadcasted_iota(jnp.int32, s.shape, 1)
    s = jnp.where(row_pos >= col_pos, s, -1e30)
    e = jnp.exp(s - jnp.max(s, axis=-1, keepdims=True))
    p = e * (1.0 / jnp.sum(e, axis=-1, keepdims=True))
    return q, k, p, limit, span


def attention_forward_into(qkv_ref, o_ref, rows, groups, hd, scale):
    seq = qkv_ref.shape[0]
    for blk in range(seq // rows):
        q, k, p, limit, span = block_probs(qkv_ref, blk, rows, groups, hd, scale)
        v = qkv_ref[0:limit, (groups + 1) * hd:(groups + 2) * hd]
        o = jnp.dot(p.astype(BF), v, preferred_element_type=F32).astype(BF)
        for j in range(groups):
            o_ref[span, j * hd:(j + 1) * hd] = o[j * rows:(j + 1) * rows]


def attention_backward_into(qkv_ref, do_ref, out_ref, dk_ref, dv_ref, rows, groups, hd, scale):
    seq = qkv_ref.shape[0]
    blocks = seq // rows
    for blk in reversed(range(blocks)):
        q, k, p, limit, span = block_probs(qkv_ref, blk, rows, groups, hd, scale)
        v = qkv_ref[0:limit, (groups + 1) * hd:(groups + 2) * hd]
        do = jnp.concatenate([do_ref[span, j * hd:(j + 1) * hd] for j in range(groups)], axis=0)
        dp = lax.dot_general(do, v, (((1,), (1,)), ((), ())), preferred_element_type=F32).astype(BF).astype(F32)
        row_dot = jnp.sum(dp * p, axis=-1, keepdims=True)
        ds = (p * (dp - row_dot) * scale).astype(BF)
        dq = jnp.dot(ds, k, preferred_element_type=F32).astype(BF)
        for j in range(groups):
            out_ref[span, j * hd:(j + 1) * hd] = dq[j * rows:(j + 1) * rows]
        dk = lax.dot_general(ds, q, (((0,), (0,)), ((), ())), preferred_element_type=F32)
        dv = lax.dot_general(p.astype(BF), do, (((0,), (0,)), ((), ())), preferred_element_type=F32)
        if blk == blocks - 1:
            dk_ref[...] = dk
            dv_ref[...] = dv
        else:
            dk_ref[0:limit] += dk
            dv_ref[0:limit] += dv
    out_ref[:, groups * hd:(groups + 1) * hd] = dk_ref[...].astype(BF)
    out_ref[:, (groups + 1) * hd:(groups + 2) * hd] = dv_ref[...].astype(BF)


def accumulate(step, acc_ref, term):
    @pl.when(step == 0)
    def _():
        acc_ref[...] = term

    @pl.when(step > 0)
    def _():
        acc_ref[...] += term


def dot_tt(a, b):
    return lax.dot_general(a, b, (((1,), (1,)), ((), ())), preferred_element_type=F32)


def qkv_attn_kernel(u_ref, w_ref, token_ref, qkv_ref, o_ref, acc_ref, *, rows, groups, hd, scale):
    step = pl.program_id(0)
    w = jnp.concatenate([w_ref[0, j] for j in range(groups + 2)], axis=1)
    accumulate(step, acc_ref, jnp.dot(u_ref[...], w, preferred_element_type=F32))

    @pl.when(step == pl.num_programs(0) - 1)
    def _():
        qkv_ref[...] = acc_ref[...].astype(BF)
        attention_forward_into(qkv_ref, o_ref, rows, groups, hd, scale)


def gate_up_kernel(v_ref, wg_ref, wu_ref, token_ref, gate_ref, up_ref, inner_ref):
    step = pl.program_id(0)
    accumulate(step, gate_ref, dot_tt(v_ref[...], wg_ref[0]))
    accumulate(step, up_ref, dot_tt(v_ref[...], wu_ref[0]))

    @pl.when(step == pl.num_programs(0) - 1)
    def _():
        @pl.loop(0, gate_ref.shape[0] // 32)
        def _(i):
            span = pl.ds(pl.multiple_of(i * 32, 32), 32)
            gate = gate_ref[span, :]
            inner_ref[span, :] = (gate * jax.nn.sigmoid(gate) * up_ref[span, :]).astype(BF)


def inner_grad_kernel(gy_ref, wd_ref, gate_ref, up_ref, token_ref, gg_ref, gu_ref, acc_ref):
    step = pl.program_id(0)
    accumulate(step, acc_ref, dot_tt(gy_ref[...], wd_ref[0]))

    @pl.when(step == pl.num_programs(0) - 1)
    def _():
        @pl.loop(0, gate_ref.shape[0] // 32)
        def _(i):
            span = pl.ds(pl.multiple_of(i * 32, 32), 32)
            gate, up = gate_ref[span, :], up_ref[span, :]
            sig = jax.nn.sigmoid(gate)
            gi = acc_ref[span, :].astype(BF).astype(F32)
            gu_ref[span, :] = (gi * (gate * sig)).astype(BF)
            gg_ref[span, :] = (gi * up * sig * (1.0 + gate * (1.0 - sig))).astype(BF)


def mix_grad_kernel(gh_ref, wo_ref, qkv_ref, token_ref, out_ref, acc_ref, do_ref, dk_ref, dv_ref, *, rows, groups, hd, scale):
    step = pl.program_id(0)
    accumulate(step, acc_ref, dot_tt(gh_ref[...], wo_ref[0]))

    @pl.when(step == pl.num_programs(0) - 1)
    def _():
        do_ref[...] = acc_ref[...].astype(BF)
        attention_backward_into(qkv_ref, do_ref, out_ref, dk_ref, dv_ref, rows, groups, hd, scale)


def whole(shape):
    return pl.BlockSpec(shape, lambda i: (0,) * len(shape))


ANY = pl.BlockSpec(memory_space=pl.ANY)


def segment_call(kernel, name, left, extra, extra_specs, out_shapes, scratch, flops, chunk=512):
    seq, width = left.shape
    return pl.pallas_call(
        kernel,
        grid=(width // chunk,),
        out_shape=[jax.ShapeDtypeStruct(*o) for o in out_shapes],
        in_specs=[pl.BlockSpec((seq, chunk), lambda i: (0, i))] + extra_specs,
        out_specs=[whole(o[0]) for o in out_shapes],
        scratch_shapes=scratch,
        name=name,
        cost_estimate=pl.CostEstimate(flops=8 * flops, bytes_accessed=2 * left.size, transcendentals=0),
    )(left, *extra)


def qkv_attention(u_full, wq, layer_idx, token, groups, hd, chunk=512):
    seq, width = u_full.shape
    slots = groups + 2
    return segment_call(
        functools.partial(qkv_attn_kernel, rows=min(128, seq), groups=groups, hd=hd, scale=hd ** -0.5), 'qkv_attn', u_full,
        [wq, token], [pl.BlockSpec((1, slots, chunk, hd), lambda i: (layer_idx, 0, i, 0)), ANY],
        [((seq, slots * hd), BF), ((seq, groups * hd), BF)], [pltpu.VMEM((seq, slots * hd), F32)], 4 * seq * width * slots * hd)


def gate_up(v_full, wg, wu, layer_idx, token, chunk=512):
    seq, width = v_full.shape
    cols = wg.shape[1]
    w_spec = pl.BlockSpec((1, cols, chunk), lambda i: (layer_idx, 0, i))
    return segment_call(gate_up_kernel, 'gate_up', v_full, [wg, wu, token], [w_spec, w_spec, ANY],
                        [((seq, cols), F32), ((seq, cols), F32), ((seq, cols), BF)], [], 4 * seq * width * cols)


def inner_grad(gy_full, wd, gate, up, layer_idx, token, chunk=512):
    seq, width = gy_full.shape
    cols = wd.shape[1]
    return segment_call(inner_grad_kernel, 'inner_grad', gy_full, [wd, gate, up, token],
                        [pl.BlockSpec((1, cols, chunk), lambda i: (layer_idx, 0, i)), whole(gate.shape), whole(up.shape), ANY],
                        [((seq, cols), BF), ((seq, cols), BF)], [pltpu.VMEM((seq, cols), F32)], 4 * seq * width * cols)


def mix_grad(gh_full, wo, qkv, layer_idx, token, groups, hd, chunk=512):
    seq, width = gh_full.shape
    heads = groups * hd
    return segment_call(
        functools.partial(mix_grad_kernel, rows=min(128, seq), groups=groups, hd=hd, scale=hd ** -0.5), 'mix_grad', gh_full,
        [wo, qkv, token], [pl.BlockSpec((1, heads, chunk), lambda i: (layer_idx, 0, i)), whole(qkv.shape), ANY],
        [(qkv.shape, BF)], [pltpu.VMEM((seq, heads), F32), pltpu.VMEM((seq, heads), BF), pltpu.VMEM((seq, hd), F32), pltpu.VMEM((seq, hd), F32)],
        8 * seq * width * heads)[0]


class WeightGrad:
    def __init__(self, lefts, rights, stacked, layer_idx, layer_count, slots=0, tile=256):
        self.lefts, self.rights, self.stacked = list(lefts), list(rights), stacked
        self.layer_idx, self.slots, self.tile = layer_idx, slots, tile
        self.seq, rows = lefts[0].shape
        cols = rights[0].shape[1]
        self.steps = (rows if slots else cols) // tile
        self.shape = (layer_count, slots, rows, cols // slots) if slots else (layer_count, rows, cols)
        self.flops = 2 * len(self.lefts) * self.seq * rows * cols
        self.ref_count = len(self.lefts) * 2 + (stacked is not None)

    def specs(self, at):
        rows, cols = self.lefts[0].shape[1], self.rights[0].shape[1]
        count, layer_idx = len(self.lefts), self.layer_idx
        part = pl.BlockSpec((self.seq, self.tile), lambda i: (0, at(i)))
        if self.slots:
            ins = [part] * count + [whole((self.seq, cols))] * count
            out = pl.BlockSpec((1, self.slots, self.tile, cols // self.slots), lambda i: (layer_idx, 0, at(i), 0))
        else:
            ins = [whole((self.seq, rows))] * count + [part] * count
            out = pl.BlockSpec((1, rows, self.tile), lambda i: (layer_idx, 0, at(i)))
        args = self.lefts + self.rights
        if self.stacked is not None:
            ins.append(ANY)
            args = args + [self.stacked]
        return ins, args, out

    def compute(self, refs, out_ref):
        count = len(self.lefts)
        total = None
        for m in range(count):
            term = lax.dot_general(refs[m][...], refs[count + m][...], (((0,), (0,)), ((), ())), preferred_element_type=F32)
            total = term if total is None else total + term
        if self.slots:
            hd = total.shape[1] // self.slots
            for j in range(self.slots):
                out_ref[0, j] = total[:, j * hd:(j + 1) * hd].astype(BF)
        else:
            out_ref[0] = total.astype(BF)


def weight_grad(job):
    ins, args, out = job.specs(lambda i: i)

    def kernel(*refs):
        job.compute(refs[:-1], refs[-1])
    return pl.pallas_call(
        kernel, grid=(job.steps,), out_shape=jax.ShapeDtypeStruct(job.shape, BF), in_specs=ins, out_specs=out,
        input_output_aliases={len(args) - 1: 0} if job.stacked is not None else {}, name='weight_grad',
        cost_estimate=pl.CostEstimate(flops=8 * job.flops, bytes_accessed=0, transcendentals=0),
    )(*args)


def product_scatter_kernel(*refs, left_count, slots, shard, tile, steps, before, after):
    lefts, weights = refs[:left_count], refs[left_count:3 * left_count]
    jobs = before + after
    taken = 3 * left_count
    job_refs = []
    for job in jobs:
        job_refs.append(refs[taken:taken + job.ref_count])
        taken += job.ref_count
    out_ref = refs[taken]
    job_outs = refs[taken + 1:taken + 1 + len(jobs)]
    rest = refs[taken + 1 + len(jobs):]
    sorted_refs = rest[:left_count]
    acc, send1, recv1, send2, recv2, send3, recv3, sem = rest[left_count:]
    step = pl.program_id(0)
    me = lax.axis_index('tp')
    core, xpos, ypos = lax.rem(me, 2), lax.rem(me // 2, 2), me // 4
    pair, xpeer, ypeer = me + 1 - 2 * core, me + 2 - 4 * xpos, me + 4 - 8 * ypos
    first, second = (xpeer, ypeer), (ypeer, xpeer)

    def copy(stage, side, g):
        src, dst, to = ((send1, recv1, pair), (send2, recv2, first[side]), (send3, recv3, second[side]))[stage]
        return pltpu.make_async_remote_copy(src_ref=src.at[side, g], dst_ref=dst.at[side, g], send_sem=sem.at[2 * stage, side, g],
                                            recv_sem=sem.at[2 * stage + 1, side, g], device_id={'tp': to},
                                            device_id_type=pl.DeviceIdType.MESH)

    def chip(side, mine, other):
        return other * 2 + mine if side == 0 else mine * 2 + other
    here = ((xpos, ypos), (ypos, xpos))

    @pl.when(step == 0)
    def _():
        barrier = pltpu.get_barrier_semaphore()
        for peer in (pair, xpeer, ypeer):
            pl.semaphore_signal(barrier, inc=1, device_id={'tp': peer}, device_id_type=pl.DeviceIdType.MESH)
        for i in range(left_count):
            for c in range(4):
                for part, which in ((0, 1 - core), (1, core)):
                    start = pl.multiple_of(c * 2 * shard + which * shard, shard)
                    sorted_refs[i][(part * 4 + c) * shard:(part * 4 + c + 1) * shard, :] = lefts[i][pl.ds(start, shard), :]
        pl.semaphore_wait(barrier, 3)

    def produce():
        for side in range(2):
            total = None
            for i in range(left_count):
                w_ref = weights[2 * i + side]
                if slots:
                    w = jnp.concatenate([w_ref[0, j] for j in range(slots)], axis=1)
                    term = dot_tt(sorted_refs[i][...], w)
                else:
                    term = jnp.dot(sorted_refs[i][...], w_ref[0], preferred_element_type=F32)
                total = term if total is None else total + term
            for c in range(4):
                send1[side, step, c] = total[c * shard:(c + 1) * shard]
                acc[side, step, c] = total[(4 + c) * shard:(5 + c) * shard]
            copy(0, side, step).start()

    def chip_sum(g):
        for side in range(2):
            copy(0, side, g).wait_recv()
            mine = here[side][0]
            for other in range(2):
                away, keep = chip(side, 1 - mine, other), chip(side, mine, other)
                send2[side, g, other] = acc[side, g, away] + recv1[side, g, away]
                acc[side, g, keep] = acc[side, g, keep] + recv1[side, g, keep]
            copy(1, side, g).start()

    def second_link():
        for g in range(steps):
            for side in range(2):
                copy(1, side, g).wait_recv()
                mine, other = here[side]
                send3[side, g] = acc[side, g, chip(side, mine, 1 - other)] + recv2[side, g, 1 - other]
                acc[side, g, chip(side, mine, other)] = acc[side, g, chip(side, mine, other)] + recv2[side, g, other]
                copy(2, side, g).start()

    def finish():
        for g in range(steps):
            for side in range(2):
                copy(2, side, g).wait_recv()
                mine, other = here[side]
                col = (side * steps + g) * tile
                out_ref[:, col:col + tile] = (acc[side, g, chip(side, mine, other)] + recv3[side, g]).astype(BF)
        for stage in range(3):
            for g in range(steps):
                for side in range(2):
                    copy(stage, side, g).wait_send()

    @pl.when(step < steps)
    def _():
        produce()

    @pl.when((step > 0) & (step < steps))
    def _():
        chip_sum(step - 1)

    @pl.when(step == steps - 1)
    def _():
        chip_sum(steps - 1)

    start = steps
    for n, job in enumerate(jobs):
        if n == len(before):
            @pl.when(step == start - 1)
            def _():
                second_link()

        @pl.when((step >= start) & (step < start + job.steps))
        def _(job=job, n=n):
            job.compute(job_refs[n], job_outs[n])
        start += job.steps

    @pl.when(step == start - 1)
    def _():
        if not after:
            second_link()
        finish()


def product_scatter(lefts, weights, layer_idx, shard, call_id, slots=0, before=(), after=(), tile=256):
    seq = lefts[0].shape[0]
    width = weights[0].shape[2]
    steps = width // tile // 2
    jobs = tuple(before) + tuple(after)
    in_specs = [whole(a.shape) for a in lefts]
    args = list(lefts)
    for w in weights:
        for side in range(2):
            if slots:
                in_specs.append(pl.BlockSpec((1, slots, tile, w.shape[3]),
                                             lambda i, s=side: (layer_idx, 0, s * steps + jnp.minimum(i, steps - 1), 0)))
            else:
                in_specs.append(pl.BlockSpec((1, w.shape[1], tile), lambda i, s=side: (layer_idx, 0, s * steps + jnp.minimum(i, steps - 1))))
            args.append(w)
    out_shapes, out_specs, aliases = [jax.ShapeDtypeStruct((shard, width), BF)], [whole((shard, width))], {}
    start = steps
    for n, job in enumerate(jobs):
        ins, job_args, out = job.specs(lambda i, start=start, last=job.steps - 1: jnp.clip(i - start, 0, last))
        in_specs += ins
        args += job_args
        if job.stacked is not None:
            aliases[len(args) - 1] = 1 + n
        out_specs.append(out)
        out_shapes.append(jax.ShapeDtypeStruct(job.shape, BF))
        start += job.steps
    depth = sum(a.shape[1] for a in lefts)
    return pl.pallas_call(
        functools.partial(product_scatter_kernel, left_count=len(lefts), slots=slots, shard=shard, tile=tile, steps=steps,
                          before=tuple(before), after=tuple(after)),
        grid=(start,),
        out_shape=out_shapes,
        in_specs=in_specs,
        out_specs=out_specs,
        input_output_aliases=aliases,
        scratch_shapes=[pltpu.VMEM(a.shape, BF) for a in lefts] + [
            pltpu.VMEM((2, steps, 4, shard, tile), F32),
            pltpu.VMEM((2, steps, 4, shard, tile), F32),
            pltpu.VMEM((2, steps, 4, shard, tile), F32),
            pltpu.VMEM((2, steps, 2, shard, tile), F32),
            pltpu.VMEM((2, steps, 2, shard, tile), F32),
            pltpu.VMEM((2, steps, shard, tile), F32),
            pltpu.VMEM((2, steps, shard, tile), F32),
            pltpu.SemaphoreType.DMA((6, 2, steps)),
        ],
        compiler_params=pltpu.CompilerParams(collective_id=call_id, has_side_effects=True),
        name='product_scatter',
        cost_estimate=pl.CostEstimate(flops=24 * 2 * seq * 2560 * 512, bytes_accessed=2 * depth * width, transcendentals=0),
    )(*args)


def solution(mesh):
    row_spec = P(None, ('dp', 'tp'), None)
    gain_spec = P(None, None)
    qkv_spec = P(None, None, 'tp', None, None)
    head_spec = P(None, 'tp', None, None)
    col_spec = P(None, None, 'tp')
    row_shard_spec = P(None, 'tp', None)
    tp = mesh.shape['tp']
    swap = {flip: [(t, t ^ flip) for t in range(tp)] for flip in (1, 2, 4)}

    def device_program(x_in, y_cot, gain_attn, gain_mlp, w_qkv, w_out, w_gate, w_up, w_down):
        micro_count, shard, width = x_in.shape
        layer_count = w_qkv.shape[0]
        groups = w_qkv.shape[3] - 2
        hd = w_qkv.shape[4]
        slots = groups + 2
        wq = jnp.transpose(w_qkv[:, :, 0], (0, 2, 1, 3))
        wo = w_out.reshape(layer_count, groups * hd, width)
        wg, wu = jnp.swapaxes(w_gate, 1, 2), jnp.swapaxes(w_up, 1, 2)

        def gather(rows):
            return lax.all_gather(rows, 'tp', axis=0, tiled=True)
        calls = iter(range(1, 100))

        def scatter_product(lefts, weights, layer_idx, slots=0, before=(), after=()):
            return product_scatter(lefts, weights, layer_idx, shard, next(calls), slots=slots, before=before, after=after)

        micros = range(micro_count)
        kept = [[{} for l in range(layer_count)] for m in micros]
        layer_in = [x_in[m] for m in micros]
        full = [gather(norm_apply(layer_in[m], gain_attn[0])) for m in micros]
        token = layer_in[0]
        gy_full = [[None] * layer_count for m in micros]
        for l in range(layer_count):
            for m in micros:
                keep = kept[m][l]
                keep['x'], keep['u'] = layer_in[m], full[m]
                keep['qkv'], keep['mix'] = qkv_attention(full[m], wq, l, token, groups, hd)
                attn_sum = scatter_product([keep['mix']], [wo], l)[0]
                keep['h'] = (layer_in[m].astype(F32) + attn_sum.astype(F32)).astype(BF)
                token = norm_apply(keep['h'], gain_mlp[l])
                full[m] = gather(token)
            for m in micros:
                keep = kept[m][l]
                keep['v'] = full[m]
                keep['gate'], keep['up'], keep['inner'] = gate_up(full[m], wg, wu, l, token)
                mlp_sum = scatter_product([keep['inner']], [w_down], l)[0]
                layer_in[m] = (keep['h'].astype(F32) + mlp_sum.astype(F32)).astype(BF)
                if l + 1 < layer_count:
                    token = norm_apply(layer_in[m], gain_attn[l + 1])
                    full[m] = gather(token)
                else:
                    token = mlp_sum
        y_rows = layer_in

        stacks = [None] * 5
        waiting = []

        def add_job(which, lefts, rights, l, slots=0):
            waiting.append((which, lefts, rights, l, slots))

        def make_jobs(count):
            picked = [waiting.pop(0) for i in range(min(count, len(waiting)))]
            return [p[0] for p in picked], [WeightGrad(p[1], p[2], stacks[p[0]], p[3], layer_count, p[4]) for p in picked]

        def scatter_with_jobs(lefts, weights, l, slots, before, after):
            which_b, jobs_b = make_jobs(before)
            which_a, jobs_a = make_jobs(after)
            out = scatter_product(lefts, weights, l, slots, jobs_b, jobs_a)
            for which, arr in zip(which_b + which_a, out[1:]):
                stacks[which] = arr
            return out[0]

        gains_a, gains_b = [None] * layer_count, [None] * layer_count
        grad_in = [y_cot[m] for m in micros]
        for l in reversed(range(layer_count)):
            for m in micros:
                keep = kept[m][l]
                keep['gy'] = full[m] if l + 1 < layer_count else gather(grad_in[m])
                keep['gg'], keep['gu'] = inner_grad(keep['gy'], w_down, keep['gate'], keep['up'], l, token)
                if m == micro_count - 1:
                    add_job(2, [kept[i][l]['gg'] for i in micros], [kept[i][l]['v'] for i in micros], l)
                    add_job(3, [kept[i][l]['gu'] for i in micros], [kept[i][l]['v'] for i in micros], l)
                    add_job(4, [kept[i][l]['inner'] for i in micros], [kept[i][l]['gy'] for i in micros], l)
                grad_nb = scatter_with_jobs([keep['gg'], keep['gu']], [wg, wu], l, 0, 1, 0 if l + 1 < layer_count and m else 1 if m == 0 else 0)
                grad_norm, gain_part = norm_backward(keep['h'], gain_mlp[l], grad_nb)
                gains_b[l] = gain_part if m == 0 else gains_b[l] + gain_part
                keep['ghr'] = token = (grad_in[m].astype(F32) + grad_norm).astype(BF)
                full[m] = gather(token)
            for m in micros:
                keep = kept[m][l]
                keep['gh'] = full[m]
                keep['gq'] = mix_grad(full[m], wo, keep['qkv'], l, token, groups, hd)
                if m == micro_count - 1:
                    add_job(1, [kept[i][l]['mix'] for i in micros], [kept[i][l]['gh'] for i in micros], l)
                last = l == 0 and m == micro_count - 1
                grad_n = scatter_with_jobs([keep['gq']], [wq], l, slots, 1, 1 if last else 0)
                if m == micro_count - 1:
                    add_job(0, [kept[i][l]['u'] for i in micros], [kept[i][l]['gq'] for i in micros], l, slots)
                grad_norm, gain_part = norm_backward(keep['x'], gain_attn[l], grad_n)
                gains_a[l] = gain_part if m == 0 else gains_a[l] + gain_part
                grad_in[m] = token = (keep['ghr'].astype(F32) + grad_norm).astype(BF)
                if l > 0:
                    full[m] = gather(token)
        while waiting:
            which, jobs = make_jobs(1)
            stacks[which[0]] = weight_grad(jobs[0])

        def sum_all(vec):
            for flip in (1, 2, 4):
                vec = vec + lax.ppermute(vec, 'tp', swap[flip])
            return vec
        gains = sum_all(jnp.stack([jnp.stack(gains_a), jnp.stack(gains_b)]))
        return (jnp.stack(y_rows), jnp.stack(grad_in), jnp.transpose(stacks[0], (0, 2, 1, 3))[:, :, None], stacks[1].reshape(w_out.shape),
                jnp.swapaxes(stacks[2], 1, 2), jnp.swapaxes(stacks[3], 1, 2), stacks[4], gains[0], gains[1])

    return jax.shard_map(device_program, mesh=mesh,
                         in_specs=(row_spec, row_spec, gain_spec, gain_spec, qkv_spec, head_spec, col_spec, col_spec, row_shard_spec),
                         out_specs=(row_spec, row_spec, P('dp', None, 'tp', None, None), P('dp', 'tp', None, None), P('dp', None, 'tp'), P('dp', None, 'tp'), P('dp', 'tp', None), P('dp', None), P('dp', None)),
                         check_vma=False)
```

```python
import functools

import jax
import jax.numpy as jnp
from jax import lax
from jax.experimental import pallas as pl
from jax.experimental.pallas import tpu as pltpu
from jax.sharding import PartitionSpec as P

NORM_EPS = 1e-5
BF = jnp.bfloat16
F32 = jnp.float32


def rms_scale(row_vals, gain_vec):
    return row_vals * lax.rsqrt(jnp.mean(row_vals * row_vals, axis=-1, keepdims=True) + NORM_EPS) * gain_vec


def norm_apply(row_vals, gain_vec):
    return rms_scale(row_vals.astype(F32), gain_vec).astype(BF)


def block_probs(qkv_ref, blk, rows, groups, hd, scale):
    limit = (blk + 1) * rows
    span = pl.ds(blk * rows, rows)
    q = jnp.concatenate([qkv_ref[span, j * hd:(j + 1) * hd] for j in range(groups)], axis=0)
    k = qkv_ref[0:limit, groups * hd:(groups + 1) * hd]
    s = lax.dot_general(q, k, (((1,), (1,)), ((), ())), preferred_element_type=F32) * scale
    row_pos = lax.rem(lax.broadcasted_iota(jnp.int32, s.shape, 0), rows) + blk * rows
    col_pos = lax.broadcasted_iota(jnp.int32, s.shape, 1)
    s = jnp.where(row_pos >= col_pos, s, -1e30)
    e = jnp.exp(s - jnp.max(s, axis=-1, keepdims=True))
    p = e * (1.0 / jnp.sum(e, axis=-1, keepdims=True))
    return q, k, p, limit, span


def attention_forward_into(qkv_ref, o_ref, rows, groups, hd, scale):
    seq = qkv_ref.shape[0]
    for blk in range(seq // rows):
        q, k, p, limit, span = block_probs(qkv_ref, blk, rows, groups, hd, scale)
        v = qkv_ref[0:limit, (groups + 1) * hd:(groups + 2) * hd]
        o = jnp.dot(p.astype(BF), v, preferred_element_type=F32).astype(BF)
        for j in range(groups):
            o_ref[span, j * hd:(j + 1) * hd] = o[j * rows:(j + 1) * rows]


def attention_backward_into(qkv_ref, do_ref, out_ref, dk_ref, dv_ref, rows, groups, hd, scale):
    seq = qkv_ref.shape[0]
    blocks = seq // rows
    for blk in reversed(range(blocks)):
        q, k, p, limit, span = block_probs(qkv_ref, blk, rows, groups, hd, scale)
        v = qkv_ref[0:limit, (groups + 1) * hd:(groups + 2) * hd]
        do = jnp.concatenate([do_ref[span, j * hd:(j + 1) * hd] for j in range(groups)], axis=0)
        dp = lax.dot_general(do, v, (((1,), (1,)), ((), ())), preferred_element_type=F32).astype(BF).astype(F32)
        row_dot = jnp.sum(dp * p, axis=-1, keepdims=True)
        ds = (p * (dp - row_dot) * scale).astype(BF)
        dq = jnp.dot(ds, k, preferred_element_type=F32).astype(BF)
        for j in range(groups):
            out_ref[span, j * hd:(j + 1) * hd] = dq[j * rows:(j + 1) * rows]
        dk = lax.dot_general(ds, q, (((0,), (0,)), ((), ())), preferred_element_type=F32)
        dv = lax.dot_general(p.astype(BF), do, (((0,), (0,)), ((), ())), preferred_element_type=F32)
        if blk == blocks - 1:
            dk_ref[...] = dk
            dv_ref[...] = dv
        else:
            dk_ref[0:limit] += dk
            dv_ref[0:limit] += dv
    out_ref[:, groups * hd:(groups + 1) * hd] = dk_ref[...].astype(BF)
    out_ref[:, (groups + 1) * hd:(groups + 2) * hd] = dv_ref[...].astype(BF)


def accumulate(step, acc_ref, term):
    @pl.when(step == 0)
    def _():
        acc_ref[...] = term

    @pl.when(step > 0)
    def _():
        acc_ref[...] += term


def dot_tt(a, b):
    return lax.dot_general(a, b, (((1,), (1,)), ((), ())), preferred_element_type=F32)


def qkv_attn_kernel(u_ref, w_ref, token_ref, qkv_ref, o_ref, acc_ref, *, rows, groups, hd, scale):
    step = pl.program_id(0)
    w = jnp.concatenate([w_ref[0, j] for j in range(groups + 2)], axis=1)
    accumulate(step, acc_ref, jnp.dot(u_ref[...], w, preferred_element_type=F32))

    @pl.when(step == pl.num_programs(0) - 1)
    def _():
        qkv_ref[...] = acc_ref[...].astype(BF)
        attention_forward_into(qkv_ref, o_ref, rows, groups, hd, scale)


def gate_up_kernel(v_ref, wg_ref, wu_ref, token_ref, gate_ref, up_ref, inner_t_ref, inner_ref):
    step = pl.program_id(0)
    accumulate(step, gate_ref, dot_tt(wg_ref[0], v_ref[...]))
    accumulate(step, up_ref, dot_tt(wu_ref[0], v_ref[...]))

    @pl.when(step == pl.num_programs(0) - 1)
    def _():
        @pl.loop(0, gate_ref.shape[0] // 32)
        def _(i):
            span = pl.ds(pl.multiple_of(i * 32, 32), 32)
            gate = gate_ref[span, :]
            inner_t_ref[span, :] = (gate * jax.nn.sigmoid(gate) * up_ref[span, :]).astype(BF)
        inner_ref[...] = inner_t_ref[...].T


def inner_grad_kernel(gy_ref, wd_ref, gate_ref, up_ref, token_ref, ggt_ref, gut_ref, gg_ref, gu_ref, acc_ref):
    step = pl.program_id(0)
    accumulate(step, acc_ref, dot_tt(wd_ref[0], gy_ref[...]))

    @pl.when(step == pl.num_programs(0) - 1)
    def _():
        @pl.loop(0, gate_ref.shape[0] // 32)
        def _(i):
            span = pl.ds(pl.multiple_of(i * 32, 32), 32)
            gate, up = gate_ref[span, :], up_ref[span, :]
            sig = jax.nn.sigmoid(gate)
            gi = acc_ref[span, :].astype(BF).astype(F32)
            gut_ref[span, :] = (gi * (gate * sig)).astype(BF)
            ggt_ref[span, :] = (gi * up * sig * (1.0 + gate * (1.0 - sig))).astype(BF)
        gg_ref[...] = ggt_ref[...].T
        gu_ref[...] = gut_ref[...].T


def mix_grad_kernel(gh_ref, wo_ref, qkv_ref, token_ref, out_ref, acc_ref, do_ref, dk_ref, dv_ref, *, rows, groups, hd, scale):
    step = pl.program_id(0)
    accumulate(step, acc_ref, dot_tt(gh_ref[...], wo_ref[0]))

    @pl.when(step == pl.num_programs(0) - 1)
    def _():
        do_ref[...] = acc_ref[...].astype(BF)
        attention_backward_into(qkv_ref, do_ref, out_ref, dk_ref, dv_ref, rows, groups, hd, scale)


def whole(shape):
    return pl.BlockSpec(shape, lambda i: (0,) * len(shape))


ANY = pl.BlockSpec(memory_space=pl.ANY)


def segment_call(kernel, name, left, extra, extra_specs, out_shapes, scratch, flops, chunk=512):
    seq, width = left.shape
    return pl.pallas_call(
        kernel,
        grid=(width // chunk,),
        out_shape=[jax.ShapeDtypeStruct(*o) for o in out_shapes],
        in_specs=[pl.BlockSpec((seq, chunk), lambda i: (0, i))] + extra_specs,
        out_specs=[whole(o[0]) for o in out_shapes],
        scratch_shapes=scratch,
        name=name,
        cost_estimate=pl.CostEstimate(flops=8 * flops, bytes_accessed=2 * left.size, transcendentals=0),
    )(left, *extra)


def qkv_attention(u_full, wq, layer_idx, token, groups, hd, chunk=512):
    seq, width = u_full.shape
    slots = groups + 2
    return segment_call(
        functools.partial(qkv_attn_kernel, rows=min(128, seq), groups=groups, hd=hd, scale=hd ** -0.5), 'qkv_attn', u_full,
        [wq, token], [pl.BlockSpec((1, slots, chunk, hd), lambda i: (layer_idx, 0, i, 0)), ANY],
        [((seq, slots * hd), BF), ((seq, groups * hd), BF)], [pltpu.VMEM((seq, slots * hd), F32)], 4 * seq * width * slots * hd)


def gate_up(v_full, wg, wu, layer_idx, token, chunk=512):
    seq, width = v_full.shape
    cols = wg.shape[1]
    w_spec = pl.BlockSpec((1, cols, chunk), lambda i: (layer_idx, 0, i))
    return segment_call(gate_up_kernel, 'gate_up', v_full, [wg, wu, token], [w_spec, w_spec, ANY],
                        [((cols, seq), F32), ((cols, seq), F32), ((cols, seq), BF), ((seq, cols), BF)], [], 4 * seq * width * cols)


def inner_grad(gy_full, wd, gate, up, layer_idx, token, chunk=512):
    seq, width = gy_full.shape
    cols = wd.shape[1]
    return segment_call(inner_grad_kernel, 'inner_grad', gy_full, [wd, gate, up, token],
                        [pl.BlockSpec((1, cols, chunk), lambda i: (layer_idx, 0, i)), whole(gate.shape), whole(up.shape), ANY],
                        [((cols, seq), BF), ((cols, seq), BF), ((seq, cols), BF), ((seq, cols), BF)], [pltpu.VMEM((cols, seq), F32)], 4 * seq * width * cols)


def mix_grad(gh_full, wo, qkv, layer_idx, token, groups, hd, chunk=512):
    seq, width = gh_full.shape
    heads = groups * hd
    return segment_call(
        functools.partial(mix_grad_kernel, rows=min(128, seq), groups=groups, hd=hd, scale=hd ** -0.5), 'mix_grad', gh_full,
        [wo, qkv, token], [pl.BlockSpec((1, heads, chunk), lambda i: (layer_idx, 0, i)), whole(qkv.shape), ANY],
        [(qkv.shape, BF)], [pltpu.VMEM((seq, heads), F32), pltpu.VMEM((seq, heads), BF), pltpu.VMEM((seq, hd), F32), pltpu.VMEM((seq, hd), F32)],
        8 * seq * width * heads)[0]


class WeightGrad:
    def __init__(self, lefts, rights, stacked, layer_idx, layer_count, slots=0, flipped=False, tile=256):
        self.lefts, self.rights, self.stacked = list(lefts), list(rights), stacked
        self.layer_idx, self.slots, self.tile = layer_idx, slots, tile
        self.flipped = flipped
        self.seq = rights[0].shape[0]
        self.rows = rows = lefts[0].shape[0 if flipped else 1]
        cols = rights[0].shape[1]
        self.steps = (rows if slots else cols) // tile
        self.shape = (layer_count, slots, rows, cols // slots) if slots else (layer_count, rows, cols)
        self.flops = 2 * len(self.lefts) * self.seq * rows * cols
        self.ref_count = len(self.lefts) * 2 + (stacked is not None)

    def specs(self, at):
        rows, cols = self.rows, self.rights[0].shape[1]
        count, layer_idx = len(self.lefts), self.layer_idx
        part = pl.BlockSpec((self.seq, self.tile), lambda i: (0, at(i)))
        if self.slots:
            ins = [part] * count + [whole((self.seq, cols))] * count
            out = pl.BlockSpec((1, self.slots, self.tile, cols // self.slots), lambda i: (layer_idx, 0, at(i), 0))
        else:
            ins = [whole(self.lefts[0].shape)] * count + [part] * count
            out = pl.BlockSpec((1, rows, self.tile), lambda i: (layer_idx, 0, at(i)))
        args = self.lefts + self.rights
        if self.stacked is not None:
            ins.append(ANY)
            args = args + [self.stacked]
        return ins, args, out

    def compute(self, refs, out_ref):
        count = len(self.lefts)
        total = None
        for m in range(count):
            lhs_dim = 1 if self.flipped else 0
            term = lax.dot_general(refs[m][...], refs[count + m][...], (((lhs_dim,), (0,)), ((), ())), preferred_element_type=F32)
            total = term if total is None else total + term
        if self.slots:
            hd = total.shape[1] // self.slots
            for j in range(self.slots):
                out_ref[0, j] = total[:, j * hd:(j + 1) * hd].astype(BF)
        else:
            out_ref[0] = total.astype(BF)


def weight_grad(job):
    ins, args, out = job.specs(lambda i: i)

    def kernel(*refs):
        job.compute(refs[:-1], refs[-1])
    return pl.pallas_call(
        kernel, grid=(job.steps,), out_shape=jax.ShapeDtypeStruct(job.shape, BF), in_specs=ins, out_specs=out,
        input_output_aliases={len(args) - 1: 0} if job.stacked is not None else {}, name='weight_grad',
        cost_estimate=pl.CostEstimate(flops=8 * job.flops, bytes_accessed=0, transcendentals=0),
    )(*args)


TAIL_INS = {'add': 1, 'norm': 2, 'back': 3}
TAIL_OUTS = {'add': 1, 'norm': 2, 'back': 2}


def row_tail(tail, sum_ref, ins, outs):
    chunk = 16

    @pl.loop(0, sum_ref.shape[0] // chunk)
    def _(i):
        span = pl.ds(pl.multiple_of(i * chunk, chunk), chunk)
        value = sum_ref[span, :].astype(F32)
        row = ins[0][span, :].astype(F32)
        if tail == 'back':
            gain = ins[2][...]
            x = ins[1][span, :].astype(F32)
            r = lax.rsqrt(jnp.mean(x * x, axis=-1, keepdims=True) + NORM_EPS)
            scaled = value * gain
            slope = jnp.mean(x * scaled, axis=-1, keepdims=True)
            outs[0][span, :] = (row + (r * scaled - x * (r * r * r * slope))).astype(BF)
            part = jnp.sum(value * (x * r), axis=0, keepdims=True)

            @pl.when(i == 0)
            def _():
                outs[1][...] = part

            @pl.when(i > 0)
            def _():
                outs[1][...] += part
        else:
            total = (row + value).astype(BF)
            outs[0][span, :] = total
            if tail == 'norm':
                x = total.astype(F32)
                r = lax.rsqrt(jnp.mean(x * x, axis=-1, keepdims=True) + NORM_EPS)
                outs[1][span, :] = (x * r * ins[1][...]).astype(BF)


def product_scatter_kernel(*refs, left_count, slots, shard, tile, steps, y_first, tail, before, after):
    lefts, weights = refs[:left_count], refs[left_count:3 * left_count]
    jobs = before + after
    taken = 3 * left_count
    tail_ins = refs[taken:taken + TAIL_INS[tail]]
    taken += TAIL_INS[tail]
    job_refs = []
    for job in jobs:
        job_refs.append(refs[taken:taken + job.ref_count])
        taken += job.ref_count
    tail_outs = refs[taken:taken + TAIL_OUTS[tail]]
    taken += TAIL_OUTS[tail]
    job_outs = refs[taken:taken + len(jobs)]
    rest = refs[taken + len(jobs):]
    sorted_refs = rest[:left_count]
    acc, send1, recv1, send2, recv2, send3, recv3, sum_ref, sem = rest[left_count:]
    step = pl.program_id(0)
    me = lax.axis_index('tp')
    core, xpos, ypos = lax.rem(me, 2), lax.rem(me // 2, 2), me // 4
    pair, xpeer, ypeer = me + 1 - 2 * core, me + 2 - 4 * xpos, me + 4 - 8 * ypos

    def route(side, g):
        flag = jnp.where(g < y_first, side, 0) if not isinstance(g, int) else side * int(g < y_first)
        mine, other = xpos + flag * (ypos - xpos), ypos + flag * (xpos - ypos)
        first, second = xpeer + flag * (ypeer - xpeer), ypeer + flag * (xpeer - ypeer)
        return flag, mine, other, first, second

    def copy(stage, side, g):
        flag, mine, other, first, second = route(side, g)
        src, dst, to = ((send1, recv1, pair), (send2, recv2, first), (send3, recv3, second))[stage]
        return pltpu.make_async_remote_copy(src_ref=src.at[side, g], dst_ref=dst.at[side, g], send_sem=sem.at[2 * stage, side, g],
                                            recv_sem=sem.at[2 * stage + 1, side, g], device_id={'tp': to},
                                            device_id_type=pl.DeviceIdType.MESH)

    def chip(flag, mine, other):
        return (1 + flag) * mine + (2 - flag) * other

    @pl.when(step == 0)
    def _():
        barrier = pltpu.get_barrier_semaphore()
        for peer in (pair, xpeer, ypeer):
            pl.semaphore_signal(barrier, inc=1, device_id={'tp': peer}, device_id_type=pl.DeviceIdType.MESH)
        for i in range(left_count):
            for c in range(4):
                for part, which in ((0, 1 - core), (1, core)):
                    start = pl.multiple_of(c * 2 * shard + which * shard, shard)
                    sorted_refs[i][(part * 4 + c) * shard:(part * 4 + c + 1) * shard, :] = lefts[i][pl.ds(start, shard), :]
        pl.semaphore_wait(barrier, 3)

    def produce():
        for side in range(2):
            total = None
            for i in range(left_count):
                w_ref = weights[2 * i + side]
                if slots:
                    w = jnp.concatenate([w_ref[0, j] for j in range(slots)], axis=1)
                    term = dot_tt(sorted_refs[i][...], w)
                else:
                    term = jnp.dot(sorted_refs[i][...], w_ref[0], preferred_element_type=F32)
                total = term if total is None else total + term
            for c in range(4):
                send1[side, step, c] = total[c * shard:(c + 1) * shard]
                acc[side, step, c] = total[(4 + c) * shard:(5 + c) * shard]
            copy(0, side, step).start()

    def chip_sum(g):
        for side in range(2):
            copy(0, side, g).wait_recv()
            flag, mine = route(side, g)[:2]
            for other in range(2):
                away, keep = chip(flag, 1 - mine, other), chip(flag, mine, other)
                send2[side, g, other] = acc[side, g, away] + recv1[side, g, away]
                acc[side, g, keep] = acc[side, g, keep] + recv1[side, g, keep]
            copy(1, side, g).start()

    def second_link():
        for g in range(steps):
            for side in range(2):
                copy(1, side, g).wait_recv()
                flag, mine, other = route(side, g)[:3]
                send3[side, g] = acc[side, g, chip(flag, mine, 1 - other)] + recv2[side, g, 1 - other]
                acc[side, g, chip(flag, mine, other)] = acc[side, g, chip(flag, mine, other)] + recv2[side, g, other]
                copy(2, side, g).start()

    def finish():
        for g in range(steps):
            for side in range(2):
                copy(2, side, g).wait_recv()
                flag, mine, other = route(side, g)[:3]
                col = (side * steps + g) * tile
                sum_ref[:, col:col + tile] = (acc[side, g, chip(flag, mine, other)] + recv3[side, g]).astype(BF)
        row_tail(tail, sum_ref, tail_ins, tail_outs)
        for stage in range(3):
            for g in range(steps):
                for side in range(2):
                    copy(stage, side, g).wait_send()

    @pl.when(step < steps)
    def _():
        produce()

    @pl.when((step > 0) & (step < steps))
    def _():
        chip_sum(step - 1)

    @pl.when(step == steps - 1)
    def _():
        chip_sum(steps - 1)

    start = steps
    for n, job in enumerate(jobs):
        if n == len(before):
            @pl.when(step == start - 1)
            def _():
                second_link()

        @pl.when((step >= start) & (step < start + job.steps))
        def _(job=job, n=n):
            job.compute(job_refs[n], job_outs[n])
        start += job.steps

    @pl.when(step == start - 1)
    def _():
        if not after:
            second_link()
        finish()


def product_scatter(lefts, weights, layer_idx, shard, call_id, tail, tail_ins, slots=0, before=(), after=(), y_first=3, tile=256):
    seq = lefts[0].shape[0]
    width = weights[0].shape[2]
    steps = width // tile // 2
    jobs = tuple(before) + tuple(after)
    in_specs = [whole(a.shape) for a in lefts]
    args = list(lefts)
    for w in weights:
        for side in range(2):
            if slots:
                in_specs.append(pl.BlockSpec((1, slots, tile, w.shape[3]),
                                             lambda i, s=side: (layer_idx, 0, s * steps + jnp.minimum(i, steps - 1), 0)))
            else:
                in_specs.append(pl.BlockSpec((1, w.shape[1], tile), lambda i, s=side: (layer_idx, 0, s * steps + jnp.minimum(i, steps - 1))))
            args.append(w)
    in_specs += [whole(a.shape) for a in tail_ins]
    args += list(tail_ins)
    second = {'add': [], 'norm': [((shard, width), BF)], 'back': [((1, width), F32)]}[tail]
    out_shapes = [jax.ShapeDtypeStruct(*o) for o in [((shard, width), BF)] + second]
    out_specs, aliases = [whole(o.shape) for o in out_shapes], {}
    tail_count = len(out_shapes)
    start = steps
    for n, job in enumerate(jobs):
        ins, job_args, out = job.specs(lambda i, start=start, last=job.steps - 1: jnp.clip(i - start, 0, last))
        in_specs += ins
        args += job_args
        if job.stacked is not None:
            aliases[len(args) - 1] = tail_count + n
        out_specs.append(out)
        out_shapes.append(jax.ShapeDtypeStruct(job.shape, BF))
        start += job.steps
    depth = sum(a.shape[1] for a in lefts)
    return pl.pallas_call(
        functools.partial(product_scatter_kernel, left_count=len(lefts), slots=slots, shard=shard, tile=tile, steps=steps,
                          y_first=y_first, tail=tail, before=tuple(before), after=tuple(after)),
        grid=(start,),
        out_shape=out_shapes,
        in_specs=in_specs,
        out_specs=out_specs,
        input_output_aliases=aliases,
        scratch_shapes=[pltpu.VMEM(a.shape, BF) for a in lefts] + [
            pltpu.VMEM((2, steps, 4, shard, tile), F32),
            pltpu.VMEM((2, steps, 4, shard, tile), F32),
            pltpu.VMEM((2, steps, 4, shard, tile), F32),
            pltpu.VMEM((2, steps, 2, shard, tile), F32),
            pltpu.VMEM((2, steps, 2, shard, tile), F32),
            pltpu.VMEM((2, steps, shard, tile), F32),
            pltpu.VMEM((2, steps, shard, tile), F32),
            pltpu.VMEM((shard, width), BF),
            pltpu.SemaphoreType.DMA((6, 2, steps)),
        ],
        compiler_params=pltpu.CompilerParams(collective_id=call_id, has_side_effects=True),
        name='product_scatter',
        cost_estimate=pl.CostEstimate(flops=24 * 2 * seq * 2560 * 512, bytes_accessed=2 * depth * width, transcendentals=0),
    )(*args)


def solution(mesh):
    row_spec = P(None, ('dp', 'tp'), None)
    gain_spec = P(None, None)
    qkv_spec = P(None, None, 'tp', None, None)
    head_spec = P(None, 'tp', None, None)
    col_spec = P(None, None, 'tp')
    row_shard_spec = P(None, 'tp', None)
    tp = mesh.shape['tp']
    swap = {flip: [(t, t ^ flip) for t in range(tp)] for flip in (1, 2, 4)}

    def device_program(x_in, y_cot, gain_attn, gain_mlp, w_qkv, w_out, w_gate, w_up, w_down):
        micro_count, shard, width = x_in.shape
        layer_count = w_qkv.shape[0]
        groups = w_qkv.shape[3] - 2
        hd = w_qkv.shape[4]
        slots = groups + 2
        wq = jnp.transpose(w_qkv[:, :, 0], (0, 2, 1, 3))
        wo = w_out.reshape(layer_count, groups * hd, width)
        wg, wu = jnp.swapaxes(w_gate, 1, 2), jnp.swapaxes(w_up, 1, 2)

        def gather(rows):
            return lax.all_gather(rows, 'tp', axis=0, tiled=True)
        calls = iter(range(1, 100))

        def scatter_product(lefts, weights, layer_idx, tail, tail_ins, slots=0, before=(), after=()):
            return product_scatter(lefts, weights, layer_idx, shard, next(calls), tail, tail_ins, slots=slots, before=before, after=after)

        micros = range(micro_count)
        kept = [[{} for l in range(layer_count)] for m in micros]
        layer_in = [x_in[m] for m in micros]
        full = [gather(norm_apply(layer_in[m], gain_attn[0])) for m in micros]
        token = layer_in[0]
        gain_a, gain_b = gain_attn[:, None], gain_mlp[:, None]
        for l in range(layer_count):
            for m in micros:
                keep = kept[m][l]
                keep['x'], keep['u'] = layer_in[m], full[m]
                keep['qkv'], keep['mix'] = qkv_attention(full[m], wq, l, token, groups, hd)
                keep['h'], token = scatter_product([keep['mix']], [wo], l, 'norm', [layer_in[m], gain_b[l]])
                full[m] = gather(token)
            for m in micros:
                keep = kept[m][l]
                keep['v'] = full[m]
                keep['gate'], keep['up'], keep['inner_t'], inner = gate_up(full[m], wg, wu, l, token)
                if l + 1 < layer_count:
                    layer_in[m], token = scatter_product([inner], [w_down], l, 'norm', [keep['h'], gain_a[l + 1]])
                    full[m] = gather(token)
                else:
                    layer_in[m] = token = scatter_product([inner], [w_down], l, 'add', [keep['h']])[0]
        y_rows = layer_in

        stacks = [None] * 5
        waiting = []

        def make_jobs(count):
            picked = [waiting.pop(0) for i in range(min(count, len(waiting)))]
            return [p[0] for p in picked], [WeightGrad(p[1], p[2], stacks[p[0]], p[3], layer_count, *p[4:]) for p in picked]

        def scatter_with_jobs(lefts, weights, l, tail_ins, slots, before, after):
            which_b, jobs_b = make_jobs(before)
            which_a, jobs_a = make_jobs(after)
            rows, gain_part, *filled = scatter_product(lefts, weights, l, 'back', tail_ins, slots, jobs_b, jobs_a)
            for which, arr in zip(which_b + which_a, filled):
                stacks[which] = arr
            return rows, gain_part

        gains_a, gains_b = [None] * layer_count, [None] * layer_count
        grad_in = [y_cot[m] for m in micros]
        for l in reversed(range(layer_count)):
            for m in micros:
                keep = kept[m][l]
                last_m = m == micro_count - 1
                keep['gy'] = full[m] if l + 1 < layer_count else gather(grad_in[m])
                keep['gg_t'], keep['gu_t'], gg, gu = inner_grad(keep['gy'], w_down, keep['gate'], keep['up'], l, token)
                if last_m:
                    for which, left, right in ((2, 'gg_t', 'v'), (3, 'gu_t', 'v'), (4, 'inner_t', 'gy')):
                        waiting.append((which, [kept[i][l][left] for i in micros], [kept[i][l][right] for i in micros], l, 0, True))
                keep['ghr'], gain_part = scatter_with_jobs([gg, gu], [wg, wu], l, [grad_in[m], keep['h'], gain_b[l]], 0, 1, 0 if last_m else 1)
                gains_b[l] = gain_part if m == 0 else gains_b[l] + gain_part
                token = keep['ghr']
                full[m] = gather(token)
            for m in micros:
                keep = kept[m][l]
                last_m = m == micro_count - 1
                keep['gh'] = full[m]
                keep['gq'] = mix_grad(full[m], wo, keep['qkv'], l, token, groups, hd)
                if last_m:
                    waiting.append((1, [kept[i][l]['mix'] for i in micros], [kept[i][l]['gh'] for i in micros], l))
                    waiting.append((0, [kept[i][l]['u'] for i in micros], [kept[i][l]['gq'] for i in micros], l, slots))
                final = l == 0 and last_m
                grad_in[m], gain_part = scatter_with_jobs([keep['gq']], [wq], l, [keep['ghr'], keep['x'], gain_a[l]], slots,
                                                          2 if final else 1, 1 if final else 0)
                gains_a[l] = gain_part if m == 0 else gains_a[l] + gain_part
                token = grad_in[m]
                if l > 0:
                    full[m] = gather(token)
        while waiting:
            which, jobs = make_jobs(1)
            stacks[which[0]] = weight_grad(jobs[0])

        def sum_all(vec):
            for flip in (1, 2, 4):
                vec = vec + lax.ppermute(vec, 'tp', swap[flip])
            return vec
        gains = sum_all(jnp.concatenate(gains_a + gains_b))
        return (jnp.stack(y_rows), jnp.stack(grad_in), jnp.transpose(stacks[0], (0, 2, 1, 3))[:, :, None], stacks[1].reshape(w_out.shape),
                jnp.swapaxes(stacks[2], 1, 2), jnp.swapaxes(stacks[3], 1, 2), stacks[4], gains[:layer_count], gains[layer_count:])

    return jax.shard_map(device_program, mesh=mesh,
                         in_specs=(row_spec, row_spec, gain_spec, gain_spec, qkv_spec, head_spec, col_spec, col_spec, row_shard_spec),
                         out_specs=(row_spec, row_spec, P('dp', None, 'tp', None, None), P('dp', 'tp', None, None), P('dp', None, 'tp'), P('dp', None, 'tp'), P('dp', 'tp', None), P('dp', None), P('dp', None)),
                         check_vma=False)
```

```python
import functools

import jax
import jax.numpy as jnp
from jax import lax
from jax.experimental import pallas as pl
from jax.experimental.pallas import tpu as pltpu
from jax.sharding import PartitionSpec as P

NORM_EPS = 1e-5
BF = jnp.bfloat16
F32 = jnp.float32


def rms_scale(row_vals, gain_vec):
    return row_vals * lax.rsqrt(jnp.mean(row_vals * row_vals, axis=-1, keepdims=True) + NORM_EPS) * gain_vec


def norm_apply(row_vals, gain_vec):
    return rms_scale(row_vals.astype(F32), gain_vec).astype(BF)


def block_probs(qkv_ref, blk, rows, groups, hd, scale):
    limit = (blk + 1) * rows
    span = pl.ds(blk * rows, rows)
    q = jnp.concatenate([qkv_ref[span, j * hd:(j + 1) * hd] for j in range(groups)], axis=0)
    k = qkv_ref[0:limit, groups * hd:(groups + 1) * hd]
    s = lax.dot_general(q, k, (((1,), (1,)), ((), ())), preferred_element_type=F32) * scale
    row_pos = lax.rem(lax.broadcasted_iota(jnp.int32, s.shape, 0), rows) + blk * rows
    col_pos = lax.broadcasted_iota(jnp.int32, s.shape, 1)
    s = jnp.where(row_pos >= col_pos, s, -1e30)
    e = jnp.exp(s - jnp.max(s, axis=-1, keepdims=True))
    p = e * (1.0 / jnp.sum(e, axis=-1, keepdims=True))
    return q, k, p, limit, span


def attention_forward_into(qkv_ref, o_ref, rows, groups, hd, scale):
    seq = qkv_ref.shape[0]
    for blk in range(seq // rows):
        q, k, p, limit, span = block_probs(qkv_ref, blk, rows, groups, hd, scale)
        v = qkv_ref[0:limit, (groups + 1) * hd:(groups + 2) * hd]
        o = jnp.dot(p.astype(BF), v, preferred_element_type=F32).astype(BF)
        for j in range(groups):
            o_ref[span, j * hd:(j + 1) * hd] = o[j * rows:(j + 1) * rows]


def attention_backward_into(qkv_ref, do_ref, out_ref, dk_ref, dv_ref, rows, groups, hd, scale):
    seq = qkv_ref.shape[0]
    blocks = seq // rows
    for blk in reversed(range(blocks)):
        q, k, p, limit, span = block_probs(qkv_ref, blk, rows, groups, hd, scale)
        v = qkv_ref[0:limit, (groups + 1) * hd:(groups + 2) * hd]
        do = jnp.concatenate([do_ref[span, j * hd:(j + 1) * hd] for j in range(groups)], axis=0)
        dp = lax.dot_general(do, v, (((1,), (1,)), ((), ())), preferred_element_type=F32).astype(BF).astype(F32)
        row_dot = jnp.sum(dp * p, axis=-1, keepdims=True)
        ds = (p * (dp - row_dot) * scale).astype(BF)
        dq = jnp.dot(ds, k, preferred_element_type=F32).astype(BF)
        for j in range(groups):
            out_ref[span, j * hd:(j + 1) * hd] = dq[j * rows:(j + 1) * rows]
        dk = lax.dot_general(ds, q, (((0,), (0,)), ((), ())), preferred_element_type=F32)
        dv = lax.dot_general(p.astype(BF), do, (((0,), (0,)), ((), ())), preferred_element_type=F32)
        if blk == blocks - 1:
            dk_ref[...] = dk
            dv_ref[...] = dv
        else:
            dk_ref[0:limit] += dk
            dv_ref[0:limit] += dv
    out_ref[:, groups * hd:(groups + 1) * hd] = dk_ref[...].astype(BF)
    out_ref[:, (groups + 1) * hd:(groups + 2) * hd] = dv_ref[...].astype(BF)


def accumulate(step, acc_ref, term):
    @pl.when(step == 0)
    def _():
        acc_ref[...] = term

    @pl.when(step > 0)
    def _():
        acc_ref[...] += term


def dot_tt(a, b):
    return lax.dot_general(a, b, (((1,), (1,)), ((), ())), preferred_element_type=F32)


def qkv_attn_body(j, last, left, ins, outs, scratch, heads):
    (w_ref,), (qkv_ref, o_ref), (acc_ref,) = ins, outs, scratch
    rows, groups, hd, scale = heads
    w = jnp.concatenate([w_ref[0, i] for i in range(groups + 2)], axis=1)
    accumulate(j, acc_ref, jnp.dot(left, w, preferred_element_type=F32))

    @pl.when(j == last)
    def _():
        qkv_ref[...] = acc_ref[...].astype(BF)
        attention_forward_into(qkv_ref, o_ref, rows, groups, hd, scale)


def gate_up_body(j, last, left, ins, outs, scratch, heads):
    (wg_ref, wu_ref), (gate_ref, up_ref, inner_t_ref, inner_ref) = ins, outs
    accumulate(j, gate_ref, dot_tt(wg_ref[0], left))
    accumulate(j, up_ref, dot_tt(wu_ref[0], left))

    @pl.when(j == last)
    def _():
        @pl.loop(0, gate_ref.shape[0] // 32)
        def _(i):
            span = pl.ds(pl.multiple_of(i * 32, 32), 32)
            gate = gate_ref[span, :]
            inner_t_ref[span, :] = (gate * jax.nn.sigmoid(gate) * up_ref[span, :]).astype(BF)
        inner_ref[...] = inner_t_ref[...].T


def inner_grad_body(j, last, left, ins, outs, scratch, heads):
    (wd_ref, gate_ref, up_ref), (ggt_ref, gut_ref, gg_ref, gu_ref), (acc_ref,) = ins, outs, scratch
    accumulate(j, acc_ref, dot_tt(wd_ref[0], left))

    @pl.when(j == last)
    def _():
        @pl.loop(0, gate_ref.shape[0] // 32)
        def _(i):
            span = pl.ds(pl.multiple_of(i * 32, 32), 32)
            gate, up = gate_ref[span, :], up_ref[span, :]
            sig = jax.nn.sigmoid(gate)
            gi = acc_ref[span, :].astype(BF).astype(F32)
            gut_ref[span, :] = (gi * (gate * sig)).astype(BF)
            ggt_ref[span, :] = (gi * up * sig * (1.0 + gate * (1.0 - sig))).astype(BF)
        gg_ref[...] = ggt_ref[...].T
        gu_ref[...] = gut_ref[...].T


def mix_grad_body(j, last, left, ins, outs, scratch, heads):
    (wo_ref, qkv_ref), (out_ref,), (acc_ref, do_ref, dk_ref, dv_ref) = ins, outs, scratch
    rows, groups, hd, scale = heads
    accumulate(j, acc_ref, dot_tt(left, wo_ref[0]))

    @pl.when(j == last)
    def _():
        do_ref[...] = acc_ref[...].astype(BF)
        attention_backward_into(qkv_ref, do_ref, out_ref, dk_ref, dv_ref, rows, groups, hd, scale)


def whole(shape):
    return pl.BlockSpec(shape, lambda i: (0,) * len(shape), pipeline_mode=pl.Buffered(1))


def whole_out(shape):
    return pl.BlockSpec(shape, lambda i: (0,) * len(shape))


ANY = pl.BlockSpec(memory_space=pl.ANY)


class Segment:
    def __init__(self, kind, layer_idx, seq, groups, hd, operands, chunk=512):
        self.kind, self.operands, self.chunk = kind, list(operands), chunk
        self.heads = (min(128, seq), groups, hd, hd ** -0.5)
        slots, q_cols = groups + 2, groups * hd
        first = operands[0]
        cols = first.shape[1]

        def chunk_spec(at, major):
            return pl.BlockSpec((1, major, chunk), lambda i: (layer_idx, 0, at(i)))
        if kind == 'qkv_attn':
            self.body = qkv_attn_body
            self.specs = lambda at: [pl.BlockSpec((1, slots, chunk, hd), lambda i: (layer_idx, 0, at(i), 0))]
            self.outs = [((seq, slots * hd), BF), ((seq, q_cols), BF)]
            self.scratch = [pltpu.VMEM((seq, slots * hd), F32)]
        elif kind == 'gate_up':
            self.body = gate_up_body
            self.specs = lambda at: [chunk_spec(at, cols)] * 2
            self.outs = [((cols, seq), F32), ((cols, seq), F32), ((cols, seq), BF), ((seq, cols), BF)]
            self.scratch = []
        elif kind == 'inner_grad':
            self.body = inner_grad_body
            self.specs = lambda at: [chunk_spec(at, cols), whole((cols, seq)), whole((cols, seq))]
            self.outs = [((cols, seq), BF), ((cols, seq), BF), ((seq, cols), BF), ((seq, cols), BF)]
            self.scratch = [pltpu.VMEM((cols, seq), F32)]
        else:
            self.body = mix_grad_body
            self.specs = lambda at: [chunk_spec(at, q_cols), whole((seq, slots * hd))]
            self.outs = [((seq, slots * hd), BF)]
            self.scratch = [pltpu.VMEM((seq, q_cols), F32), pltpu.VMEM((seq, q_cols), BF), pltpu.VMEM((seq, hd), F32), pltpu.VMEM((seq, hd), F32)]


def run_segment(seg, full):
    seq, width = full.shape
    steps = width // seg.chunk
    count, outs = len(seg.operands), len(seg.outs)

    def kernel(left_ref, *refs):
        seg.body(pl.program_id(0), steps - 1, left_ref[...], refs[:count], refs[count:count + outs], refs[count + outs:], seg.heads)
    return pl.pallas_call(
        kernel, grid=(steps,), out_shape=[jax.ShapeDtypeStruct(*o) for o in seg.outs],
        in_specs=[pl.BlockSpec((seq, seg.chunk), lambda i: (0, i))] + seg.specs(lambda i: i),
        out_specs=[whole_out(o[0]) for o in seg.outs], scratch_shapes=seg.scratch, name=seg.kind,
    )(full, *seg.operands)


class WeightGrad:
    def __init__(self, lefts, rights, stacked, layer_idx, layer_count, slots=0, flipped=False, tile=256):
        self.lefts, self.rights, self.stacked = list(lefts), list(rights), stacked
        self.layer_idx, self.slots, self.tile = layer_idx, slots, tile
        self.flipped = flipped
        self.seq = rights[0].shape[0]
        self.rows = rows = lefts[0].shape[0 if flipped else 1]
        cols = rights[0].shape[1]
        self.steps = (rows if slots else cols) // tile
        self.shape = (layer_count, slots, rows, cols // slots) if slots else (layer_count, rows, cols)
        self.flops = 2 * len(self.lefts) * self.seq * rows * cols
        self.ref_count = len(self.lefts) * 2 + (stacked is not None)

    def specs(self, at):
        rows, cols = self.rows, self.rights[0].shape[1]
        count, layer_idx = len(self.lefts), self.layer_idx
        part = pl.BlockSpec((self.seq, self.tile), lambda i: (0, at(i)))
        if self.slots:
            ins = [part] * count + [whole((self.seq, cols))] * count
            out = pl.BlockSpec((1, self.slots, self.tile, cols // self.slots), lambda i: (layer_idx, 0, at(i), 0))
        else:
            ins = [whole(self.lefts[0].shape)] * count + [part] * count
            out = pl.BlockSpec((1, rows, self.tile), lambda i: (layer_idx, 0, at(i)))
        args = self.lefts + self.rights
        if self.stacked is not None:
            ins.append(ANY)
            args = args + [self.stacked]
        return ins, args, out

    def compute(self, refs, out_ref):
        count = len(self.lefts)
        total = None
        for m in range(count):
            lhs_dim = 1 if self.flipped else 0
            term = lax.dot_general(refs[m][...], refs[count + m][...], (((lhs_dim,), (0,)), ((), ())), preferred_element_type=F32)
            total = term if total is None else total + term
        if self.slots:
            hd = total.shape[1] // self.slots
            for j in range(self.slots):
                out_ref[0, j] = total[:, j * hd:(j + 1) * hd].astype(BF)
        else:
            out_ref[0] = total.astype(BF)


def weight_grad(job):
    ins, args, out = job.specs(lambda i: i)

    def kernel(*refs):
        job.compute(refs[:-1], refs[-1])
    return pl.pallas_call(
        kernel, grid=(job.steps,), out_shape=jax.ShapeDtypeStruct(job.shape, BF), in_specs=ins, out_specs=out,
        input_output_aliases={len(args) - 1: 0} if job.stacked is not None else {}, name='weight_grad',
        cost_estimate=pl.CostEstimate(flops=8 * job.flops, bytes_accessed=0, transcendentals=0),
    )(*args)


TAIL_INS = {'add': 1, 'norm': 2, 'back': 3}
TAIL_OUTS = {'add': 1, 'norm': 2, 'back': 2}


def row_tail(tail, sum_ref, ins, outs):
    chunk = 16

    @pl.loop(0, sum_ref.shape[0] // chunk)
    def _(i):
        span = pl.ds(pl.multiple_of(i * chunk, chunk), chunk)
        value = sum_ref[span, :].astype(F32)
        row = ins[0][span, :].astype(F32)
        if tail == 'back':
            gain = ins[2][...]
            x = ins[1][span, :].astype(F32)
            r = lax.rsqrt(jnp.mean(x * x, axis=-1, keepdims=True) + NORM_EPS)
            scaled = value * gain
            slope = jnp.mean(x * scaled, axis=-1, keepdims=True)
            outs[0][span, :] = (row + (r * scaled - x * (r * r * r * slope))).astype(BF)
            part = jnp.sum(value * (x * r), axis=0, keepdims=True)

            @pl.when(i == 0)
            def _():
                outs[1][...] = part

            @pl.when(i > 0)
            def _():
                outs[1][...] += part
        else:
            total = (row + value).astype(BF)
            outs[0][span, :] = total
            if tail == 'norm':
                x = total.astype(F32)
                r = lax.rsqrt(jnp.mean(x * x, axis=-1, keepdims=True) + NORM_EPS)
                outs[1][span, :] = (x * r * ins[1][...]).astype(BF)


def half_step_kernel(*refs, left_count, slots, shard, tile, steps, y_first, tail, seg, jobs):
    taken = 0

    def take(count):
        nonlocal taken
        taken += count
        return refs[taken - count:taken]
    lefts, weights = take(left_count), take(2 * left_count)
    tail_ins = take(TAIL_INS[tail])
    rows_ref, = take(1) if seg else (None,)
    seg_ins = take(len(seg.operands)) if seg else ()
    job_refs = [take(job.ref_count) for job in jobs]
    tail_outs = take(TAIL_OUTS[tail])
    full_out, = take(1) if seg else (None,)
    seg_outs = take(len(seg.outs)) if seg else ()
    job_outs = take(len(jobs))
    sorted_refs = take(left_count)
    acc, send1, recv1, send2, recv2, send3, recv3, sum_ref, sem = take(9)
    full_ref, gsem, out_sem = take(3) if seg else (None,) * 3
    seg_scratch = take(len(seg.scratch)) if seg else ()
    step = pl.program_id(0)
    me = lax.axis_index('tp')
    core, xpos, ypos = lax.rem(me, 2), lax.rem(me // 2, 2), me // 4
    pair, xpeer, ypeer = me + 1 - 2 * core, me + 2 - 4 * xpos, me + 4 - 8 * ypos

    def route(side, g):
        flag = jnp.where(g < y_first, side, 0) if not isinstance(g, int) else side * int(g < y_first)
        mine, other = xpos + flag * (ypos - xpos), ypos + flag * (xpos - ypos)
        first, second = xpeer + flag * (ypeer - xpeer), ypeer + flag * (xpeer - ypeer)
        return flag, mine, other, first, second

    def copy(stage, side, g):
        flag, mine, other, first, second = route(side, g)
        src, dst, to = ((send1, recv1, pair), (send2, recv2, first), (send3, recv3, second))[stage]
        return pltpu.make_async_remote_copy(src_ref=src.at[side, g], dst_ref=dst.at[side, g], send_sem=sem.at[2 * stage, side, g],
                                            recv_sem=sem.at[2 * stage + 1, side, g], device_id={'tp': to},
                                            device_id_type=pl.DeviceIdType.MESH)

    def chip(flag, mine, other):
        return (1 + flag) * mine + (2 - flag) * other

    def block(owner, side=None):
        span = pl.ds(pl.multiple_of(owner * shard, shard), shard)
        half = full_ref.shape[1] // 2
        return full_ref.at[span, :] if side is None else full_ref.at[span, side * half:(side + 1) * half]

    def gather_copy(n):
        half = rows_ref.shape[1] // 2 if rows_ref is not None else 0
        diag = xpeer + ypeer - me
        peers = (xpeer, ypeer)
        if n < 4:
            side = n % 2
            src, dst, to = rows_ref.at[:, side * half:(side + 1) * half], block(me, side), peers[side if n < 2 else 1 - side]
        elif n < 6:
            side = n % 2
            src, dst, to = block(peers[side], side), block(peers[side], side), peers[1 - side]
        elif n == 6:
            src, dst, to = rows_ref, block(me), pair
        else:
            side = (n - 7) % 2
            owner = (peers[side], peers[1 - side], diag)[(n - 7) // 2]
            src, dst, to = block(owner, side), block(owner, side), pair
        return pltpu.make_async_remote_copy(src_ref=src, dst_ref=dst, send_sem=gsem.at[0, n], recv_sem=gsem.at[1, n],
                                            device_id={'tp': to}, device_id_type=pl.DeviceIdType.MESH)

    def gather_start():
        for n in (0, 1, 6, 2, 3):
            gather_copy(n).start()
        full_ref[pl.ds(pl.multiple_of(me * shard, shard), shard), :] = rows_ref[...]

    def gather_relay():
        for side in range(2):
            gather_copy(side).wait_recv()
            gather_copy(4 + side).start()
            gather_copy(7 + side).start()

    def gather_finish():
        for n in (2, 3, 4, 5):
            gather_copy(n).wait_recv()
            gather_copy(7 + n).start()
        for n in range(6, 13):
            gather_copy(n).wait_recv()
        for n in range(13):
            gather_copy(n).wait_send()
        pltpu.make_async_copy(full_ref, full_out, out_sem).start()

    @pl.when(step == 0)
    def _():
        barrier = pltpu.get_barrier_semaphore()
        for peer in (pair, xpeer, ypeer):
            pl.semaphore_signal(barrier, inc=1, device_id={'tp': peer}, device_id_type=pl.DeviceIdType.MESH)
        pl.semaphore_wait(barrier, 3)
        if seg:
            gather_start()
        for i in range(left_count):
            for c in range(4):
                for part, which in ((0, 1 - core), (1, core)):
                    start = pl.multiple_of(c * 2 * shard + which * shard, shard)
                    sorted_refs[i][(part * 4 + c) * shard:(part * 4 + c + 1) * shard, :] = lefts[i][pl.ds(start, shard), :]

    def produce():
        for side in range(2):
            total = None
            for i in range(left_count):
                w_ref = weights[2 * i + side]
                if slots:
                    w = jnp.concatenate([w_ref[0, j] for j in range(slots)], axis=1)
                    term = dot_tt(sorted_refs[i][...], w)
                else:
                    term = jnp.dot(sorted_refs[i][...], w_ref[0], preferred_element_type=F32)
                total = term if total is None else total + term
            for c in range(4):
                send1[side, step, c] = total[c * shard:(c + 1) * shard]
                acc[side, step, c] = total[(4 + c) * shard:(5 + c) * shard]
            copy(0, side, step).start()

    def chip_sum(g):
        for side in range(2):
            copy(0, side, g).wait_recv()
            flag, mine = route(side, g)[:2]
            for other in range(2):
                away, keep = chip(flag, 1 - mine, other), chip(flag, mine, other)
                send2[side, g, other] = acc[side, g, away] + recv1[side, g, away]
                acc[side, g, keep] = acc[side, g, keep] + recv1[side, g, keep]
            copy(1, side, g).start()

    def second_link(g):
        for side in range(2):
            copy(1, side, g).wait_recv()
            flag, mine, other = route(side, g)[:3]
            send3[side, g] = acc[side, g, chip(flag, mine, 1 - other)] + recv2[side, g, 1 - other]
            acc[side, g, chip(flag, mine, other)] = acc[side, g, chip(flag, mine, other)] + recv2[side, g, other]
            copy(2, side, g).start()

    def finish():
        for g in range(steps):
            for side in range(2):
                copy(2, side, g).wait_recv()
                flag, mine, other = route(side, g)[:3]
                col = (side * steps + g) * tile
                sum_ref[:, col:col + tile] = (acc[side, g, chip(flag, mine, other)] + recv3[side, g]).astype(BF)
        row_tail(tail, sum_ref, tail_ins, tail_outs)
        for stage in range(3):
            for g in range(steps):
                for side in range(2):
                    copy(stage, side, g).wait_send()

    @pl.when(step < steps)
    def _():
        produce()

    if not seg:
        @pl.when((step > 0) & (step < steps))
        def _():
            chip_sum(step - 1)

    @pl.when(step == steps - 1)
    def _():
        if seg:
            gather_relay()
            for g in range(steps - 1):
                chip_sum(g)
        chip_sum(steps - 1)

    start = steps
    for n, job in enumerate(jobs):
        @pl.when((step >= start) & (step < start + job.steps))
        def _(job=job, n=n):
            job.compute(job_refs[n], job_outs[n])
        start += job.steps

    if seg:
        @pl.when(step == start)
        def _():
            gather_finish()

        @pl.when(step >= start)
        def _():
            j = step - start
            left = full_ref[:, pl.ds(pl.multiple_of(j * seg.chunk, seg.chunk), seg.chunk)]
            seg.body(j, steps - 1, left, seg_ins, seg_outs, seg_scratch, seg.heads)
            second_link(j)
        start += steps

    @pl.when(step == start - 1)
    def _():
        if seg:
            pltpu.make_async_copy(full_ref, full_out, out_sem).wait()
        else:
            for g in range(steps):
                second_link(g)
        finish()


def half_step(lefts, weights, layer_idx, shard, call_id, tail, tail_ins, slots=0, seg=None, rows=None, jobs=(), y_first=5, tile=256):
    seq = lefts[0].shape[0]
    width = weights[0].shape[2]
    steps = width // tile // 2
    in_specs = [whole(a.shape) for a in lefts]
    args = list(lefts)
    for w in weights:
        for side in range(2):
            if slots:
                in_specs.append(pl.BlockSpec((1, slots, tile, w.shape[3]),
                                             lambda i, s=side: (layer_idx, 0, s * steps + jnp.minimum(i, steps - 1), 0)))
            else:
                in_specs.append(pl.BlockSpec((1, w.shape[1], tile), lambda i, s=side: (layer_idx, 0, s * steps + jnp.minimum(i, steps - 1))))
            args.append(w)
    in_specs += [whole(a.shape) for a in tail_ins]
    args += list(tail_ins)
    seg_start = steps + sum(job.steps for job in jobs)
    if seg:
        in_specs += [whole(rows.shape)] + seg.specs(lambda i: jnp.clip(i - seg_start, 0, steps - 1))
        args += [rows] + seg.operands
    second = {'add': [], 'norm': [((shard, width), BF)], 'back': [((1, width), F32)]}[tail]
    out_shapes = [jax.ShapeDtypeStruct(*o) for o in [((shard, width), BF)] + second]
    out_specs, aliases = [whole_out(o.shape) for o in out_shapes], {}
    if seg:
        out_shapes += [jax.ShapeDtypeStruct((seq, width), BF)] + [jax.ShapeDtypeStruct(*o) for o in seg.outs]
        out_specs += [ANY] + [whole_out(o[0]) for o in seg.outs]
    start = steps
    for job in jobs:
        ins, job_args, out = job.specs(lambda i, start=start, last=job.steps - 1: jnp.clip(i - start, 0, last))
        in_specs += ins
        args += job_args
        if job.stacked is not None:
            aliases[len(args) - 1] = len(out_shapes)
        out_specs.append(out)
        out_shapes.append(jax.ShapeDtypeStruct(job.shape, BF))
        start += job.steps
    big = pltpu.VMEM((2, steps, 4, shard, tile), F32)
    mid = pltpu.VMEM((2, steps, 2, shard, tile), F32)
    small = pltpu.VMEM((2, steps, shard, tile), F32)
    scratch = [pltpu.VMEM(a.shape, BF) for a in lefts] + [big, big, big, mid, mid, small, small, pltpu.VMEM((shard, width), BF),
                                                          pltpu.SemaphoreType.DMA((6, 2, steps))]
    if seg:
        scratch += [pltpu.VMEM((seq, width), BF), pltpu.SemaphoreType.DMA((2, 13)), pltpu.SemaphoreType.DMA] + seg.scratch
    return pl.pallas_call(
        functools.partial(half_step_kernel, left_count=len(lefts), slots=slots, shard=shard, tile=tile, steps=steps,
                          y_first=y_first, tail=tail, seg=seg, jobs=tuple(jobs)),
        grid=(seg_start + (steps if seg else 0),),
        out_shape=out_shapes,
        in_specs=in_specs,
        out_specs=out_specs,
        input_output_aliases=aliases,
        scratch_shapes=scratch,
        compiler_params=pltpu.CompilerParams(collective_id=call_id, has_side_effects=True, vmem_limit_bytes=67000000),
        name='half_step',
    )(*args)


def solution(mesh):
    row_spec = P(None, ('dp', 'tp'), None)
    gain_spec = P(None, None)
    qkv_spec = P(None, None, 'tp', None, None)
    head_spec = P(None, 'tp', None, None)
    col_spec = P(None, None, 'tp')
    row_shard_spec = P(None, 'tp', None)
    tp = mesh.shape['tp']
    swap = {flip: [(t, t ^ flip) for t in range(tp)] for flip in (1, 2, 4)}

    def device_program(x_in, y_cot, gain_attn, gain_mlp, w_qkv, w_out, w_gate, w_up, w_down):
        micro_count, shard, width = x_in.shape
        layer_count = w_qkv.shape[0]
        groups = w_qkv.shape[3] - 2
        hd = w_qkv.shape[4]
        slots = groups + 2
        wq = jnp.transpose(w_qkv[:, :, 0], (0, 2, 1, 3))
        wo = w_out.reshape(layer_count, groups * hd, width)
        wg, wu = jnp.swapaxes(w_gate, 1, 2), jnp.swapaxes(w_up, 1, 2)

        def gather(rows):
            return lax.all_gather(rows, 'tp', axis=0, tiled=True)
        micros = range(micro_count)
        gain_a, gain_b = gain_attn[:, None], gain_mlp[:, None]
        top = layer_count - 1
        plan = [(kind, l) for l in range(layer_count) for kind in ('qkv_attn', 'gate_up')]
        plan += [(kind, l) for l in reversed(range(layer_count)) for kind in ('inner_grad', 'mix_grad')]
        kept = [[{} for l in range(layer_count)] for m in micros]
        rows_in = [norm_apply(x_in[m], gain_attn[0]) for m in micros]
        for m in micros:
            kept[m][0]['x'] = x_in[m]
        y_rows, grad_x = [None] * micro_count, [None] * micro_count
        gains_a = [[None] * micro_count for l in range(layer_count)]
        gains_b = [[None] * micro_count for l in range(layer_count)]
        stacks = [None] * 5
        waiting = []

        def segment(m, s):
            kind, l = plan[s]
            keep = kept[m][l]
            operands = {'qkv_attn': lambda: [wq], 'gate_up': lambda: [wg, wu], 'inner_grad': lambda: [w_down, keep['gate'], keep['up']],
                        'mix_grad': lambda: [wo, keep['qkv']]}[kind]()
            return Segment(kind, l, shard * tp, groups, hd, operands)

        def store(m, s, full, outs):
            kind, l = plan[s]
            keep = kept[m][l]
            names = {'qkv_attn': ('u', 'qkv', 'mix'), 'gate_up': ('v', 'gate', 'up', 'inner_t', 'inner'),
                     'inner_grad': ('gy', 'gg_t', 'gu_t', 'gg', 'gu'), 'mix_grad': ('gh', 'gq')}[kind]
            keep.update(zip(names, [full] + list(outs)))
            if m == micro_count - 1 and kind == 'inner_grad':
                for which, left, right in ((2, 'gg_t', 'v'), (3, 'gu_t', 'v'), (4, 'inner_t', 'gy')):
                    waiting.append((which, [kept[i][l][left] for i in micros], [kept[i][l][right] for i in micros], l, 0, True))
            if m == micro_count - 1 and kind == 'mix_grad':
                waiting.append((1, [kept[i][l]['mix'] for i in micros], [kept[i][l]['gh'] for i in micros], l))
                waiting.append((0, [kept[i][l]['u'] for i in micros], [kept[i][l]['gq'] for i in micros], l, slots))

        def scatter(call, m, s, next_m, next_s, job_count):
            kind, l = plan[s]
            keep = kept[m][l]
            lefts, weights, slot_count = {'qkv_attn': ([keep.get('mix')], [wo], 0), 'gate_up': ([keep.get('inner')], [w_down], 0),
                                          'inner_grad': ([keep.get('gg'), keep.get('gu')], [wg, wu], 0),
                                          'mix_grad': ([keep.get('gq')], [wq], slots)}[kind]
            if kind == 'qkv_attn':
                tail, tail_ins = 'norm', [keep['x'], gain_b[l]]
            elif kind == 'gate_up' and l < top:
                tail, tail_ins = 'norm', [keep['h'], gain_a[l + 1]]
            elif kind == 'gate_up':
                tail, tail_ins = 'add', [keep['h']]
            elif kind == 'inner_grad':
                tail, tail_ins = 'back', [rows_in[m], keep['h'], gain_b[l]]
            else:
                tail, tail_ins = 'back', [rows_in[m], keep['x'], gain_a[l]]
            seg = segment(next_m, next_s) if next_m is not None else None
            picked = [waiting.pop(0) for i in range(min(job_count, len(waiting)))]
            jobs = [WeightGrad(p[1], p[2], stacks[p[0]], p[3], layer_count, *p[4:]) for p in picked]
            outs = half_step(lefts, weights, l, shard, call, tail, tail_ins, slot_count, seg,
                             rows_in[next_m] if seg else None, jobs)
            head, outs = outs[:TAIL_OUTS[tail]], outs[TAIL_OUTS[tail]:]
            if seg:
                seg_outs, outs = outs[:1 + len(seg.outs)], outs[1 + len(seg.outs):]
                store(next_m, next_s, seg_outs[0], seg_outs[1:])
            for p, arr in zip(picked, outs):
                stacks[p[0]] = arr
            if kind == 'qkv_attn':
                keep['h'], rows_in[m] = head
            elif kind == 'gate_up' and l < top:
                kept[m][l + 1]['x'], rows_in[m] = head
            elif kind == 'gate_up':
                y_rows[m], rows_in[m] = head[0], y_cot[m]
            else:
                rows_in[m] = head[0]
                (gains_b if kind == 'inner_grad' else gains_a)[l][m] = head[1]
                grad_x[m] = head[0]

        full = gather(rows_in[0])
        store(0, 0, full, run_segment(segment(0, 0), full))
        job_counts = {9: 1, 10: 1, 11: 1, 12: 2, 13: 1, 14: 2, 15: 2}
        total = micro_count * len(plan)
        for call in range(total):
            m, s = call % micro_count, call // micro_count
            next_m, next_s = (call + 1) % micro_count, (call + 1) // micro_count
            scatter(call + 1, m, s, next_m if call + 1 < total else None, next_s, job_counts.get(call, 0))
        grad_in = grad_x
        for p in waiting:
            stacks[p[0]] = weight_grad(WeightGrad(p[1], p[2], stacks[p[0]], p[3], layer_count, *p[4:]))
        gains_a = [sum(parts[1:], parts[0]) for parts in gains_a]
        gains_b = [sum(parts[1:], parts[0]) for parts in gains_b]

        def sum_all(vec):
            for flip in (1, 2, 4):
                vec = vec + lax.ppermute(vec, 'tp', swap[flip])
            return vec
        gains = sum_all(jnp.concatenate(gains_a + gains_b))
        return (jnp.stack(y_rows), jnp.stack(grad_in), jnp.transpose(stacks[0], (0, 2, 1, 3))[:, :, None], stacks[1].reshape(w_out.shape),
                jnp.swapaxes(stacks[2], 1, 2), jnp.swapaxes(stacks[3], 1, 2), stacks[4], gains[:layer_count], gains[layer_count:])

    return jax.shard_map(device_program, mesh=mesh,
                         in_specs=(row_spec, row_spec, gain_spec, gain_spec, qkv_spec, head_spec, col_spec, col_spec, row_shard_spec),
                         out_specs=(row_spec, row_spec, P('dp', None, 'tp', None, None), P('dp', 'tp', None, None), P('dp', None, 'tp'), P('dp', None, 'tp'), P('dp', 'tp', None), P('dp', None), P('dp', None)),
                         check_vma=False)
```

```python
import functools

import jax
import jax.numpy as jnp
from jax import lax
from jax.experimental import pallas as pl
from jax.experimental.pallas import tpu as pltpu
from jax.sharding import PartitionSpec as P

NORM_EPS = 1e-5
BF = jnp.bfloat16
F32 = jnp.float32


def rms_scale(row_vals, gain_vec):
    return row_vals * lax.rsqrt(jnp.mean(row_vals * row_vals, axis=-1, keepdims=True) + NORM_EPS) * gain_vec


def norm_apply(row_vals, gain_vec):
    return rms_scale(row_vals.astype(F32), gain_vec).astype(BF)


def block_probs(qkv_ref, blk, rows, groups, hd, scale):
    limit = (blk + 1) * rows
    span = pl.ds(blk * rows, rows)
    q = jnp.concatenate([qkv_ref[span, j * hd:(j + 1) * hd] for j in range(groups)], axis=0)
    k = qkv_ref[0:limit, groups * hd:(groups + 1) * hd]
    s = lax.dot_general(q, k, (((1,), (1,)), ((), ())), preferred_element_type=F32) * scale
    row_pos = lax.rem(lax.broadcasted_iota(jnp.int32, s.shape, 0), rows) + blk * rows
    col_pos = lax.broadcasted_iota(jnp.int32, s.shape, 1)
    s = jnp.where(row_pos >= col_pos, s, -1e30)
    e = jnp.exp(s - jnp.max(s, axis=-1, keepdims=True))
    p = e * (1.0 / jnp.sum(e, axis=-1, keepdims=True))
    return q, k, p, limit, span


def attention_forward_into(qkv_ref, o_ref, rows, groups, hd, scale):
    seq = qkv_ref.shape[0]
    for blk in range(seq // rows):
        q, k, p, limit, span = block_probs(qkv_ref, blk, rows, groups, hd, scale)
        v = qkv_ref[0:limit, (groups + 1) * hd:(groups + 2) * hd]
        o = jnp.dot(p.astype(BF), v, preferred_element_type=F32).astype(BF)
        for j in range(groups):
            o_ref[span, j * hd:(j + 1) * hd] = o[j * rows:(j + 1) * rows]


def attention_backward_into(qkv_ref, do_ref, out_ref, dk_ref, dv_ref, rows, groups, hd, scale):
    seq = qkv_ref.shape[0]
    blocks = seq // rows
    for blk in reversed(range(blocks)):
        q, k, p, limit, span = block_probs(qkv_ref, blk, rows, groups, hd, scale)
        v = qkv_ref[0:limit, (groups + 1) * hd:(groups + 2) * hd]
        do = jnp.concatenate([do_ref[span, j * hd:(j + 1) * hd] for j in range(groups)], axis=0)
        dp = lax.dot_general(do, v, (((1,), (1,)), ((), ())), preferred_element_type=F32).astype(BF).astype(F32)
        row_dot = jnp.sum(dp * p, axis=-1, keepdims=True)
        ds = (p * (dp - row_dot) * scale).astype(BF)
        dq = jnp.dot(ds, k, preferred_element_type=F32).astype(BF)
        for j in range(groups):
            out_ref[span, j * hd:(j + 1) * hd] = dq[j * rows:(j + 1) * rows]
        dk = lax.dot_general(ds, q, (((0,), (0,)), ((), ())), preferred_element_type=F32)
        dv = lax.dot_general(p.astype(BF), do, (((0,), (0,)), ((), ())), preferred_element_type=F32)
        if blk == blocks - 1:
            dk_ref[...] = dk
            dv_ref[...] = dv
        else:
            dk_ref[0:limit] += dk
            dv_ref[0:limit] += dv
    out_ref[:, groups * hd:(groups + 1) * hd] = dk_ref[...].astype(BF)
    out_ref[:, (groups + 1) * hd:(groups + 2) * hd] = dv_ref[...].astype(BF)


def accumulate(step, acc_ref, term):
    @pl.when(step == 0)
    def _():
        acc_ref[...] = term

    @pl.when(step > 0)
    def _():
        acc_ref[...] += term


def dot_tt(a, b):
    return lax.dot_general(a, b, (((1,), (1,)), ((), ())), preferred_element_type=F32)


def qkv_attn_body(j, left, ins, outs, scratch, heads):
    (w_ref,), (qkv_ref, o_ref), (acc_ref,) = ins, outs, scratch
    rows, groups, hd, scale = heads
    w = jnp.concatenate([w_ref[0, i] for i in range(groups + 2)], axis=1)
    accumulate(j, acc_ref, jnp.dot(left, w, preferred_element_type=F32))

    def epilogue():
        qkv_ref[...] = acc_ref[...].astype(BF)
        attention_forward_into(qkv_ref, o_ref, rows, groups, hd, scale)
    return epilogue


def gate_up_body(j, left, ins, outs, scratch, heads):
    (wg_ref, wu_ref), (gate_ref, up_ref, inner_t_ref, inner_ref) = ins, outs
    accumulate(j, gate_ref, dot_tt(wg_ref[0], left))
    accumulate(j, up_ref, dot_tt(wu_ref[0], left))

    def epilogue():
        @pl.loop(0, gate_ref.shape[0] // 32)
        def _(i):
            span = pl.ds(pl.multiple_of(i * 32, 32), 32)
            gate = gate_ref[span, :]
            inner_t_ref[span, :] = (gate * jax.nn.sigmoid(gate) * up_ref[span, :]).astype(BF)
        inner_ref[...] = inner_t_ref[...].T
    return epilogue


def inner_grad_body(j, left, ins, outs, scratch, heads):
    (wd_ref, gate_ref, up_ref), (ggt_ref, gut_ref, gg_ref, gu_ref), (acc_ref,) = ins, outs, scratch
    accumulate(j, acc_ref, dot_tt(wd_ref[0], left))

    def epilogue():
        @pl.loop(0, gate_ref.shape[0] // 32)
        def _(i):
            span = pl.ds(pl.multiple_of(i * 32, 32), 32)
            gate, up = gate_ref[span, :], up_ref[span, :]
            sig = jax.nn.sigmoid(gate)
            gi = acc_ref[span, :].astype(BF).astype(F32)
            gut_ref[span, :] = (gi * (gate * sig)).astype(BF)
            ggt_ref[span, :] = (gi * up * sig * (1.0 + gate * (1.0 - sig))).astype(BF)
        gg_ref[...] = ggt_ref[...].T
        gu_ref[...] = gut_ref[...].T
    return epilogue


def mix_grad_body(j, left, ins, outs, scratch, heads):
    (wo_ref, qkv_ref), (out_ref,), (acc_ref, do_ref, dk_ref, dv_ref) = ins, outs, scratch
    rows, groups, hd, scale = heads
    accumulate(j, acc_ref, dot_tt(left, wo_ref[0]))

    def epilogue():
        do_ref[...] = acc_ref[...].astype(BF)
        attention_backward_into(qkv_ref, do_ref, out_ref, dk_ref, dv_ref, rows, groups, hd, scale)
    return epilogue


def whole(shape):
    return pl.BlockSpec(shape, lambda i: (0,) * len(shape), pipeline_mode=pl.Buffered(1))


def whole_out(shape):
    return pl.BlockSpec(shape, lambda i: (0,) * len(shape))


ANY = pl.BlockSpec(memory_space=pl.ANY)


class Segment:
    def __init__(self, kind, layer_idx, seq, groups, hd, operands, chunk=512):
        self.kind, self.operands, self.chunk, self.seq = kind, list(operands), chunk, seq
        self.heads = (min(128, seq), groups, hd, hd ** -0.5)
        slots, q_cols = groups + 2, groups * hd
        first = operands[0]
        cols = first.shape[1]

        def chunk_spec(at, major):
            return pl.BlockSpec((1, major, chunk), lambda i: (layer_idx, 0, at(i)))
        if kind == 'qkv_attn':
            self.body = qkv_attn_body
            self.specs = lambda at: [pl.BlockSpec((1, slots, chunk, hd), lambda i: (layer_idx, 0, at(i), 0))]
            self.outs = [((seq, slots * hd), BF), ((seq, q_cols), BF)]
            self.scratch = [pltpu.VMEM((seq, slots * hd), F32)]
        elif kind == 'gate_up':
            self.body = gate_up_body
            self.specs = lambda at: [chunk_spec(at, cols)] * 2
            self.outs = [((cols, seq), F32), ((cols, seq), F32), ((cols, seq), BF), ((seq, cols), BF)]
            self.scratch = []
        elif kind == 'inner_grad':
            self.body = inner_grad_body
            self.specs = lambda at: [chunk_spec(at, cols), whole((cols, seq)), whole((cols, seq))]
            self.outs = [((cols, seq), BF), ((cols, seq), BF), ((seq, cols), BF), ((seq, cols), BF)]
            self.scratch = [pltpu.VMEM((cols, seq), F32)]
        else:
            self.body = mix_grad_body
            self.specs = lambda at: [chunk_spec(at, q_cols), whole((seq, slots * hd))]
            self.outs = [((seq, slots * hd), BF)]
            self.scratch = [pltpu.VMEM((seq, q_cols), F32), pltpu.VMEM((seq, q_cols), BF), pltpu.VMEM((seq, hd), F32), pltpu.VMEM((seq, hd), F32)]


class WeightGrad:
    def __init__(self, lefts, rights, stacked, layer_idx, layer_count, slots=0, flipped=False, tile=256):
        self.lefts, self.rights, self.stacked = list(lefts), list(rights), stacked
        self.layer_idx, self.slots, self.tile = layer_idx, slots, tile
        self.flipped = flipped
        self.seq = rights[0].shape[0]
        self.rows = rows = lefts[0].shape[0 if flipped else 1]
        cols = rights[0].shape[1]
        self.steps = (rows if slots else cols) // tile
        self.shape = (layer_count, slots, rows, cols // slots) if slots else (layer_count, rows, cols)
        self.flops = 2 * len(self.lefts) * self.seq * rows * cols
        self.ref_count = len(self.lefts) * 2 + (stacked is not None)

    def specs(self, at):
        rows, cols = self.rows, self.rights[0].shape[1]
        count, layer_idx = len(self.lefts), self.layer_idx
        part = pl.BlockSpec((self.seq, self.tile), lambda i: (0, at(i)))
        if self.slots:
            ins = [part] * count + [whole((self.seq, cols))] * count
            out = pl.BlockSpec((1, self.slots, self.tile, cols // self.slots), lambda i: (layer_idx, 0, at(i), 0))
        else:
            ins = [whole(self.lefts[0].shape)] * count + [part] * count
            out = pl.BlockSpec((1, rows, self.tile), lambda i: (layer_idx, 0, at(i)))
        args = self.lefts + self.rights
        if self.stacked is not None:
            ins.append(ANY)
            args = args + [self.stacked]
        return ins, args, out

    def compute(self, refs, out_ref):
        count = len(self.lefts)
        total = None
        for m in range(count):
            lhs_dim = 1 if self.flipped else 0
            term = lax.dot_general(refs[m][...], refs[count + m][...], (((lhs_dim,), (0,)), ((), ())), preferred_element_type=F32)
            total = term if total is None else total + term
        if self.slots:
            hd = total.shape[1] // self.slots
            for j in range(self.slots):
                out_ref[0, j] = total[:, j * hd:(j + 1) * hd].astype(BF)
        else:
            out_ref[0] = total.astype(BF)


def weight_grad_stack(job, upper):
    ins, args, out = job.specs(lambda i: i)
    slots, rows, tile = job.slots, job.rows, job.tile
    hd = upper.shape[-1]
    if slots:
        upper_spec = out
        out_spec = pl.BlockSpec((2, slots, tile, hd), lambda i: (0, 0, i, 0))
    else:
        upper_spec = out
        out_spec = pl.BlockSpec((2, rows, tile), lambda i: (0, 0, i))

    def kernel(*refs):
        job.compute(refs[:-2], refs[-1])
        refs[-1][1] = refs[-2][0]
    return pl.pallas_call(
        kernel, grid=(job.steps,), out_shape=jax.ShapeDtypeStruct((2,) + upper.shape[1:], BF), in_specs=ins + [upper_spec], out_specs=out_spec,
        name='weight_grad', cost_estimate=pl.CostEstimate(flops=8 * job.flops, bytes_accessed=0, transcendentals=0),
    )(*args, upper)


TAIL_INS = {'none': 0, 'add': 1, 'norm': 2, 'back': 3}
TAIL_OUTS = {'none': 0, 'add': 1, 'norm': 2, 'back': 2}


def row_tail(tail, sum_ref, ins, outs):
    chunk = 16

    @pl.loop(0, sum_ref.shape[0] // chunk)
    def _(i):
        span = pl.ds(pl.multiple_of(i * chunk, chunk), chunk)
        value = sum_ref[span, :].astype(F32)
        row = ins[0][span, :].astype(F32)
        if tail == 'back':
            gain = ins[2][...]
            x = ins[1][span, :].astype(F32)
            r = lax.rsqrt(jnp.mean(x * x, axis=-1, keepdims=True) + NORM_EPS)
            scaled = value * gain
            slope = jnp.mean(x * scaled, axis=-1, keepdims=True)
            outs[0][span, :] = (row + (r * scaled - x * (r * r * r * slope))).astype(BF)
            part = jnp.sum(value * (x * r), axis=0, keepdims=True)

            @pl.when(i == 0)
            def _():
                outs[1][...] = part

            @pl.when(i > 0)
            def _():
                outs[1][...] += part
        else:
            total = (row + value).astype(BF)
            outs[0][span, :] = total
            if tail == 'norm':
                x = total.astype(F32)
                r = lax.rsqrt(jnp.mean(x * x, axis=-1, keepdims=True) + NORM_EPS)
                outs[1][span, :] = (x * r * ins[1][...]).astype(BF)


def half_step_kernel(*refs, left_count, slots, shard, tile, steps, y_first, tail, seg, jobs):
    taken = 0

    def take(count):
        nonlocal taken
        taken += count
        return refs[taken - count:taken]
    lefts, weights = take(left_count), take(2 * left_count)
    tail_ins = take(TAIL_INS[tail])
    rows_ref, = take(1) if seg else (None,)
    seg_ins = take(len(seg.operands)) if seg else ()
    job_refs = [take(job.ref_count) for job in jobs]
    tail_outs = take(TAIL_OUTS[tail])
    full_out, = take(1) if seg else (None,)
    seg_outs = take(len(seg.outs)) if seg else ()
    job_outs = take(len(jobs))
    sorted_refs = take(left_count)
    acc, send1, recv1, send2, recv2, send3, recv3, sum_ref, sem = take(9) if left_count else (None,) * 9
    full_ref, gsem, out_sem = take(3) if seg else (None,) * 3
    seg_scratch = take(len(seg.scratch)) if seg else ()
    step = pl.program_id(0)
    me = lax.axis_index('tp')
    core, xpos, ypos = lax.rem(me, 2), lax.rem(me // 2, 2), me // 4
    pair, xpeer, ypeer = me + 1 - 2 * core, me + 2 - 4 * xpos, me + 4 - 8 * ypos

    def route(side, g):
        flag = jnp.where(g < y_first, side, 0) if not isinstance(g, int) else side * int(g < y_first)
        mine, other = xpos + flag * (ypos - xpos), ypos + flag * (xpos - ypos)
        first, second = xpeer + flag * (ypeer - xpeer), ypeer + flag * (xpeer - ypeer)
        return flag, mine, other, first, second

    def copy(stage, side, g):
        flag, mine, other, first, second = route(side, g)
        src, dst, to = ((send1, recv1, pair), (send2, recv2, first), (send3, recv3, second))[stage]
        return pltpu.make_async_remote_copy(src_ref=src.at[side, g], dst_ref=dst.at[side, g], send_sem=sem.at[2 * stage, side, g],
                                            recv_sem=sem.at[2 * stage + 1, side, g], device_id={'tp': to},
                                            device_id_type=pl.DeviceIdType.MESH)

    def chip(flag, mine, other):
        return (1 + flag) * mine + (2 - flag) * other

    def block(owner, side=None):
        span = pl.ds(pl.multiple_of(owner * shard, shard), shard)
        half = full_ref.shape[1] // 2
        return full_ref.at[span, :] if side is None else full_ref.at[span, side * half:(side + 1) * half]

    def gather_copy(n):
        half = rows_ref.shape[1] // 2 if rows_ref is not None else 0
        diag = xpeer + ypeer - me
        peers = (xpeer, ypeer)
        if n < 4:
            side = n % 2
            src, dst, to = rows_ref.at[:, side * half:(side + 1) * half], block(me, side), peers[side if n < 2 else 1 - side]
        elif n < 6:
            side = n % 2
            src, dst, to = block(peers[side], side), block(peers[side], side), peers[1 - side]
        elif n == 6:
            src, dst, to = rows_ref, block(me), pair
        else:
            side = (n - 7) % 2
            owner = (peers[side], peers[1 - side], diag)[(n - 7) // 2]
            src, dst, to = block(owner, side), block(owner, side), pair
        return pltpu.make_async_remote_copy(src_ref=src, dst_ref=dst, send_sem=gsem.at[0, n], recv_sem=gsem.at[1, n],
                                            device_id={'tp': to}, device_id_type=pl.DeviceIdType.MESH)

    def gather_start():
        for n in (0, 1, 6, 2, 3):
            gather_copy(n).start()
        full_ref[pl.ds(pl.multiple_of(me * shard, shard), shard), :] = rows_ref[...]

    def gather_relay():
        for side in range(2):
            gather_copy(side).wait_recv()
            gather_copy(4 + side).start()
            gather_copy(7 + side).start()

    def gather_finish():
        for n in (2, 3, 4, 5):
            gather_copy(n).wait_recv()
            gather_copy(7 + n).start()
        for n in range(6, 13):
            gather_copy(n).wait_recv()
        for n in range(13):
            gather_copy(n).wait_send()
        pltpu.make_async_copy(full_ref, full_out, out_sem).start()

    @pl.when(step == 0)
    def _():
        barrier = pltpu.get_barrier_semaphore()
        for peer in (pair, xpeer, ypeer):
            pl.semaphore_signal(barrier, inc=1, device_id={'tp': peer}, device_id_type=pl.DeviceIdType.MESH)
        pl.semaphore_wait(barrier, 3)
        if seg:
            gather_start()
        for i in range(left_count):
            for c in range(4):
                for part, which in ((0, 1 - core), (1, core)):
                    start = pl.multiple_of(c * 2 * shard + which * shard, shard)
                    sorted_refs[i][(part * 4 + c) * shard:(part * 4 + c + 1) * shard, :] = lefts[i][pl.ds(start, shard), :]

    def produce():
        for side in range(2):
            total = None
            for i in range(left_count):
                w_ref = weights[2 * i + side]
                if slots:
                    w = jnp.concatenate([w_ref[0, j] for j in range(slots)], axis=1)
                    term = dot_tt(sorted_refs[i][...], w)
                else:
                    term = jnp.dot(sorted_refs[i][...], w_ref[0], preferred_element_type=F32)
                total = term if total is None else total + term
            for c in range(4):
                send1[side, step, c] = total[c * shard:(c + 1) * shard]
                acc[side, step, c] = total[(4 + c) * shard:(5 + c) * shard]
            copy(0, side, step).start()

    def chip_sum(g):
        for side in range(2):
            copy(0, side, g).wait_recv()
            flag, mine = route(side, g)[:2]
            for other in range(2):
                away, keep = chip(flag, 1 - mine, other), chip(flag, mine, other)
                send2[side, g, other] = acc[side, g, away] + recv1[side, g, away]
                acc[side, g, keep] = acc[side, g, keep] + recv1[side, g, keep]
            copy(1, side, g).start()

    def second_link(g):
        for side in range(2):
            copy(1, side, g).wait_recv()
            flag, mine, other = route(side, g)[:3]
            send3[side, g] = acc[side, g, chip(flag, mine, 1 - other)] + recv2[side, g, 1 - other]
            acc[side, g, chip(flag, mine, other)] = acc[side, g, chip(flag, mine, other)] + recv2[side, g, other]
            copy(2, side, g).start()

    def finish():
        for g in range(steps):
            for side in range(2):
                copy(2, side, g).wait_recv()
                flag, mine, other = route(side, g)[:3]
                col = (side * steps + g) * tile
                sum_ref[:, col:col + tile] = (acc[side, g, chip(flag, mine, other)] + recv3[side, g]).astype(BF)
        row_tail(tail, sum_ref, tail_ins, tail_outs)
        for stage in range(3):
            for g in range(steps):
                for side in range(2):
                    copy(stage, side, g).wait_send()

    if left_count:
        relay_step = 2 if seg else 0

        @pl.when(step < steps)
        def _():
            produce()

        if seg:
            @pl.when(step == relay_step)
            def _():
                gather_relay()
                for g in range(relay_step):
                    chip_sum(g)

        @pl.when((step > relay_step) & (step < steps))
        def _():
            chip_sum(step - 1)

        @pl.when(step == steps - 1)
        def _():
            chip_sum(steps - 1)
    else:
        @pl.when(step == 0)
        def _():
            gather_relay()

    start = steps if left_count else 0
    for n, job in enumerate(jobs):
        @pl.when((step >= start) & (step < start + job.steps))
        def _(job=job, n=n):
            job.compute(job_refs[n], job_outs[n])
        start += job.steps

    if seg:
        @pl.when(step == start)
        def _():
            gather_finish()

        @pl.when(step >= start)
        def _():
            j = step - start
            left = full_ref[:, pl.ds(pl.multiple_of(j * seg.chunk, seg.chunk), seg.chunk)]
            epilogue = seg.body(j, left, seg_ins, seg_outs, seg_scratch, seg.heads)
            if left_count:
                second_link(j)

            @pl.when(j == steps - 1)
            def _():
                epilogue()
        start += steps

    @pl.when(step == start - 1)
    def _():
        if seg:
            pltpu.make_async_copy(full_ref, full_out, out_sem).wait()
        else:
            for g in range(steps):
                second_link(g)
        if left_count:
            finish()


def half_step(lefts, weights, layer_idx, shard, call_id, tail, tail_ins, slots=0, seg=None, rows=None, jobs=(), y_first=5, tile=256):
    width = weights[0].shape[2] if lefts else rows.shape[1]
    steps = width // tile // 2
    seq = lefts[0].shape[0] if lefts else seg.seq
    in_specs = [whole(a.shape) for a in lefts]
    args = list(lefts)
    for w in weights:
        for side in range(2):
            if slots:
                in_specs.append(pl.BlockSpec((1, slots, tile, w.shape[3]),
                                             lambda i, s=side: (layer_idx, 0, s * steps + jnp.minimum(i, steps - 1), 0)))
            else:
                in_specs.append(pl.BlockSpec((1, w.shape[1], tile), lambda i, s=side: (layer_idx, 0, s * steps + jnp.minimum(i, steps - 1))))
            args.append(w)
    in_specs += [whole(a.shape) for a in tail_ins]
    args += list(tail_ins)
    seg_start = (steps if lefts else 0) + sum(job.steps for job in jobs)
    if seg:
        in_specs += [whole(rows.shape)] + seg.specs(lambda i: jnp.clip(i - seg_start, 0, steps - 1))
        args += [rows] + seg.operands
    second = {'none': [], 'add': [], 'norm': [((shard, width), BF)], 'back': [((1, width), F32)]}[tail]
    out_shapes = [jax.ShapeDtypeStruct(*o) for o in ([((shard, width), BF)] if lefts else []) + second]
    out_specs, aliases = [whole_out(o.shape) for o in out_shapes], {}
    if seg:
        out_shapes += [jax.ShapeDtypeStruct((seq, width), BF)] + [jax.ShapeDtypeStruct(*o) for o in seg.outs]
        out_specs += [ANY] + [whole_out(o[0]) for o in seg.outs]
    start = steps
    for job in jobs:
        ins, job_args, out = job.specs(lambda i, start=start, last=job.steps - 1: jnp.clip(i - start, 0, last))
        in_specs += ins
        args += job_args
        if job.stacked is not None:
            aliases[len(args) - 1] = len(out_shapes)
        out_specs.append(out)
        out_shapes.append(jax.ShapeDtypeStruct(job.shape, BF))
        start += job.steps
    big = pltpu.VMEM((2, steps, 4, shard, tile), F32)
    mid = pltpu.VMEM((2, steps, 2, shard, tile), F32)
    small = pltpu.VMEM((2, steps, shard, tile), F32)
    scratch = [pltpu.VMEM(a.shape, BF) for a in lefts]
    if lefts:
        scratch += [big, big, big, mid, mid, small, small, pltpu.VMEM((shard, width), BF), pltpu.SemaphoreType.DMA((6, 2, steps))]
    if seg:
        scratch += [pltpu.VMEM((seq, width), BF), pltpu.SemaphoreType.DMA((2, 13)), pltpu.SemaphoreType.DMA] + seg.scratch
    return pl.pallas_call(
        functools.partial(half_step_kernel, left_count=len(lefts), slots=slots, shard=shard, tile=tile, steps=steps,
                          y_first=y_first, tail=tail, seg=seg, jobs=tuple(jobs)),
        grid=(seg_start + (steps if seg else 0),),
        out_shape=out_shapes,
        in_specs=in_specs,
        out_specs=out_specs,
        input_output_aliases=aliases,
        scratch_shapes=scratch,
        compiler_params=pltpu.CompilerParams(collective_id=call_id, has_side_effects=True, vmem_limit_bytes=67000000),
        name='half_step',
    )(*args)


def solution(mesh):
    row_spec = P(None, ('dp', 'tp'), None)
    gain_spec = P(None, None)
    qkv_spec = P(None, None, 'tp', None, None)
    head_spec = P(None, 'tp', None, None)
    col_spec = P(None, None, 'tp')
    row_shard_spec = P(None, 'tp', None)
    tp = mesh.shape['tp']
    swap = {flip: [(t, t ^ flip) for t in range(tp)] for flip in (1, 2, 4)}

    def device_program(x_in, y_cot, gain_attn, gain_mlp, w_qkv, w_out, w_gate, w_up, w_down):
        micro_count, shard, width = x_in.shape
        layer_count = w_qkv.shape[0]
        groups = w_qkv.shape[3] - 2
        hd = w_qkv.shape[4]
        slots = groups + 2
        wq = jnp.transpose(w_qkv[:, :, 0], (0, 2, 1, 3))
        wo = w_out.reshape(layer_count, groups * hd, width)
        wg, wu = jnp.swapaxes(w_gate, 1, 2), jnp.swapaxes(w_up, 1, 2)

        micros = range(micro_count)
        gain_a, gain_b = gain_attn[:, None], gain_mlp[:, None]
        top = layer_count - 1
        plan = [(kind, l) for l in range(layer_count) for kind in ('qkv_attn', 'gate_up')]
        plan += [(kind, l) for l in reversed(range(layer_count)) for kind in ('inner_grad', 'mix_grad')]
        kept = [[{} for l in range(layer_count)] for m in micros]
        rows_in = [norm_apply(x_in[m], gain_attn[0]) for m in micros]
        for m in micros:
            kept[m][0]['x'] = x_in[m]
        y_rows, grad_x = [None] * micro_count, [None] * micro_count
        gains_a = [[None] * micro_count for l in range(layer_count)]
        gains_b = [[None] * micro_count for l in range(layer_count)]
        stacks = [None] * 5
        waiting = []

        def segment(m, s):
            kind, l = plan[s]
            keep = kept[m][l]
            operands = {'qkv_attn': lambda: [wq], 'gate_up': lambda: [wg, wu], 'inner_grad': lambda: [w_down, keep['gate'], keep['up']],
                        'mix_grad': lambda: [wo, keep['qkv']]}[kind]()
            return Segment(kind, l, shard * tp, groups, hd, operands)

        def store(m, s, full, outs):
            kind, l = plan[s]
            keep = kept[m][l]
            names = {'qkv_attn': ('u', 'qkv', 'mix'), 'gate_up': ('v', 'gate', 'up', 'inner_t', 'inner'),
                     'inner_grad': ('gy', 'gg_t', 'gu_t', 'gg', 'gu'), 'mix_grad': ('gh', 'gq')}[kind]
            keep.update(zip(names, [full] + list(outs)))
            if m == micro_count - 1 and kind == 'inner_grad':
                for which, left, right in ((2, 'gg_t', 'v'), (3, 'gu_t', 'v'), (4, 'inner_t', 'gy')):
                    waiting.append((which, [kept[i][l][left] for i in micros], [kept[i][l][right] for i in micros], l, 0, True))
            if m == micro_count - 1 and kind == 'mix_grad':
                waiting.append((1, [kept[i][l]['mix'] for i in micros], [kept[i][l]['gh'] for i in micros], l))
                waiting.append((0, [kept[i][l]['u'] for i in micros], [kept[i][l]['gq'] for i in micros], l, slots))

        def scatter(call, m, s, next_m, next_s, job_count):
            kind, l = plan[s]
            keep = kept[m][l]
            lefts, weights, slot_count = {'qkv_attn': ([keep.get('mix')], [wo], 0), 'gate_up': ([keep.get('inner')], [w_down], 0),
                                          'inner_grad': ([keep.get('gg'), keep.get('gu')], [wg, wu], 0),
                                          'mix_grad': ([keep.get('gq')], [wq], slots)}[kind]
            if kind == 'qkv_attn':
                tail, tail_ins = 'norm', [keep['x'], gain_b[l]]
            elif kind == 'gate_up' and l < top:
                tail, tail_ins = 'norm', [keep['h'], gain_a[l + 1]]
            elif kind == 'gate_up':
                tail, tail_ins = 'add', [keep['h']]
            elif kind == 'inner_grad':
                tail, tail_ins = 'back', [rows_in[m], keep['h'], gain_b[l]]
            else:
                tail, tail_ins = 'back', [rows_in[m], keep['x'], gain_a[l]]
            seg = segment(next_m, next_s) if next_m is not None else None
            picked = [waiting.pop(0) for i in range(min(job_count, len(waiting)))]
            jobs = [WeightGrad(p[1], p[2], None, 0, 1, *p[4:]) for p in picked]
            outs = half_step(lefts, weights, l, shard, call, tail, tail_ins, slot_count, seg,
                             rows_in[next_m] if seg else None, jobs)
            head, outs = outs[:TAIL_OUTS[tail]], outs[TAIL_OUTS[tail]:]
            if seg:
                seg_outs, outs = outs[:1 + len(seg.outs)], outs[1 + len(seg.outs):]
                store(next_m, next_s, seg_outs[0], seg_outs[1:])
            for p, arr in zip(picked, outs):
                stacks[p[0]] = arr
            if kind == 'qkv_attn':
                keep['h'], rows_in[m] = head
            elif kind == 'gate_up' and l < top:
                kept[m][l + 1]['x'], rows_in[m] = head
            elif kind == 'gate_up':
                y_rows[m], rows_in[m] = head[0], y_cot[m]
            else:
                rows_in[m] = head[0]
                (gains_b if kind == 'inner_grad' else gains_a)[l][m] = head[1]
                grad_x[m] = head[0]

        first_full, *first_outs = half_step([], [], 0, shard, micro_count * len(plan) + 1, 'none', [], 0, segment(0, 0), rows_in[0])
        store(0, 0, first_full, first_outs)
        job_counts = {10: 2, 11: 1, 12: 1, 13: 1}
        total = micro_count * len(plan)
        for call in range(total):
            m, s = call % micro_count, call // micro_count
            next_m, next_s = (call + 1) % micro_count, (call + 1) // micro_count
            scatter(call + 1, m, s, next_m if call + 1 < total else None, next_s, job_counts.get(call, 0))
        grad_in = grad_x
        for p in waiting:
            stacks[p[0]] = weight_grad_stack(WeightGrad(p[1], p[2], None, 0, 1, *p[4:]), stacks[p[0]])
        gains_a = [sum(parts[1:], parts[0]) for parts in gains_a]
        gains_b = [sum(parts[1:], parts[0]) for parts in gains_b]

        def sum_all(vec):
            for flip in (1, 2, 4):
                vec = vec + lax.ppermute(vec, 'tp', swap[flip])
            return vec
        gains = sum_all(jnp.concatenate(gains_a + gains_b))
        return (jnp.stack(y_rows), jnp.stack(grad_in), jnp.transpose(stacks[0], (0, 2, 1, 3))[:, :, None], stacks[1].reshape(w_out.shape),
                jnp.swapaxes(stacks[2], 1, 2), jnp.swapaxes(stacks[3], 1, 2), stacks[4], gains[:layer_count], gains[layer_count:])

    return jax.shard_map(device_program, mesh=mesh,
                         in_specs=(row_spec, row_spec, gain_spec, gain_spec, qkv_spec, head_spec, col_spec, col_spec, row_shard_spec),
                         out_specs=(row_spec, row_spec, P('dp', None, 'tp', None, None), P('dp', 'tp', None, None), P('dp', None, 'tp'), P('dp', None, 'tp'), P('dp', 'tp', None), P('dp', None), P('dp', None)),
                         check_vma=False)
```

```python
import functools

import jax
import jax.numpy as jnp
from jax import lax
from jax.experimental import pallas as pl
from jax.experimental.pallas import tpu as pltpu
from jax.sharding import PartitionSpec as P

NORM_EPS = 1e-5
BF = jnp.bfloat16
F32 = jnp.float32


def rms_scale(row_vals, gain_vec):
    return row_vals * lax.rsqrt(jnp.mean(row_vals * row_vals, axis=-1, keepdims=True) + NORM_EPS) * gain_vec


def norm_apply(row_vals, gain_vec):
    return rms_scale(row_vals.astype(F32), gain_vec).astype(BF)


def block_probs(qkv_ref, blk, rows, groups, hd, scale):
    limit = (blk + 1) * rows
    span = pl.ds(blk * rows, rows)
    q = jnp.concatenate([qkv_ref[span, j * hd:(j + 1) * hd] for j in range(groups)], axis=0)
    k = qkv_ref[0:limit, groups * hd:(groups + 1) * hd]
    s = lax.dot_general(q, k, (((1,), (1,)), ((), ())), preferred_element_type=F32) * scale
    row_pos = lax.rem(lax.broadcasted_iota(jnp.int32, s.shape, 0), rows) + blk * rows
    col_pos = lax.broadcasted_iota(jnp.int32, s.shape, 1)
    s = jnp.where(row_pos >= col_pos, s, -1e30)
    e = jnp.exp(s - jnp.max(s, axis=-1, keepdims=True))
    p = e * (1.0 / jnp.sum(e, axis=-1, keepdims=True))
    return q, k, p, limit, span


def attention_forward_into(qkv_ref, o_ref, rows, groups, hd, scale):
    seq = qkv_ref.shape[0]
    for blk in range(seq // rows):
        q, k, p, limit, span = block_probs(qkv_ref, blk, rows, groups, hd, scale)
        v = qkv_ref[0:limit, (groups + 1) * hd:(groups + 2) * hd]
        o = jnp.dot(p.astype(BF), v, preferred_element_type=F32).astype(BF)
        for j in range(groups):
            o_ref[span, j * hd:(j + 1) * hd] = o[j * rows:(j + 1) * rows]


def attention_backward_into(qkv_ref, do_ref, out_ref, dk_ref, dv_ref, rows, groups, hd, scale):
    seq = qkv_ref.shape[0]
    blocks = seq // rows
    for blk in reversed(range(blocks)):
        q, k, p, limit, span = block_probs(qkv_ref, blk, rows, groups, hd, scale)
        v = qkv_ref[0:limit, (groups + 1) * hd:(groups + 2) * hd]
        do = jnp.concatenate([do_ref[span, j * hd:(j + 1) * hd] for j in range(groups)], axis=0)
        dp = lax.dot_general(do, v, (((1,), (1,)), ((), ())), preferred_element_type=F32).astype(BF).astype(F32)
        row_dot = jnp.sum(dp * p, axis=-1, keepdims=True)
        ds = (p * (dp - row_dot) * scale).astype(BF)
        dq = jnp.dot(ds, k, preferred_element_type=F32).astype(BF)
        for j in range(groups):
            out_ref[span, j * hd:(j + 1) * hd] = dq[j * rows:(j + 1) * rows]
        dk = lax.dot_general(ds, q, (((0,), (0,)), ((), ())), preferred_element_type=F32)
        dv = lax.dot_general(p.astype(BF), do, (((0,), (0,)), ((), ())), preferred_element_type=F32)
        if blk == blocks - 1:
            dk_ref[...] = dk
            dv_ref[...] = dv
        else:
            dk_ref[0:limit] += dk
            dv_ref[0:limit] += dv
    out_ref[:, groups * hd:(groups + 1) * hd] = dk_ref[...].astype(BF)
    out_ref[:, (groups + 1) * hd:(groups + 2) * hd] = dv_ref[...].astype(BF)


def accumulate(step, acc_ref, term):
    @pl.when(step == 0)
    def _():
        acc_ref[...] = term

    @pl.when(step > 0)
    def _():
        acc_ref[...] += term


def dot_tt(a, b):
    return lax.dot_general(a, b, (((1,), (1,)), ((), ())), preferred_element_type=F32)


def qkv_attn_body(j, left, ins, outs, scratch, heads):
    (w_ref,), (qkv_ref, o_ref), (acc_ref,) = ins, outs, scratch
    rows, groups, hd, scale = heads
    w = jnp.concatenate([w_ref[0, i] for i in range(groups + 2)], axis=1)
    accumulate(j, acc_ref, jnp.dot(left, w, preferred_element_type=F32))

    def epilogue():
        qkv_ref[...] = acc_ref[...].astype(BF)
        attention_forward_into(qkv_ref, o_ref, rows, groups, hd, scale)
    return epilogue


def gate_up_body(j, left, ins, outs, scratch, heads):
    (wg_ref, wu_ref), (gate_ref, up_ref, inner_t_ref, inner_ref) = ins, outs
    accumulate(j, gate_ref, dot_tt(wg_ref[0], left))
    accumulate(j, up_ref, dot_tt(wu_ref[0], left))

    def epilogue():
        @pl.loop(0, gate_ref.shape[0] // 32)
        def _(i):
            span = pl.ds(pl.multiple_of(i * 32, 32), 32)
            gate = gate_ref[span, :]
            inner_t_ref[span, :] = (gate * jax.nn.sigmoid(gate) * up_ref[span, :]).astype(BF)
        inner_ref[...] = inner_t_ref[...].T
    return epilogue


def inner_grad_body(j, left, ins, outs, scratch, heads):
    (wd_ref, gate_ref, up_ref), (ggt_ref, gut_ref, gg_ref, gu_ref), (acc_ref,) = ins, outs, scratch
    accumulate(j, acc_ref, dot_tt(wd_ref[0], left))

    def epilogue():
        @pl.loop(0, gate_ref.shape[0] // 32)
        def _(i):
            span = pl.ds(pl.multiple_of(i * 32, 32), 32)
            gate, up = gate_ref[span, :], up_ref[span, :]
            sig = jax.nn.sigmoid(gate)
            gi = acc_ref[span, :].astype(BF).astype(F32)
            gut_ref[span, :] = (gi * (gate * sig)).astype(BF)
            ggt_ref[span, :] = (gi * up * sig * (1.0 + gate * (1.0 - sig))).astype(BF)
        gg_ref[...] = ggt_ref[...].T
        gu_ref[...] = gut_ref[...].T
    return epilogue


def mix_grad_body(j, left, ins, outs, scratch, heads):
    (wo_ref, qkv_ref), (out_ref,), (acc_ref, do_ref, dk_ref, dv_ref) = ins, outs, scratch
    rows, groups, hd, scale = heads
    accumulate(j, acc_ref, dot_tt(left, wo_ref[0]))

    def epilogue():
        do_ref[...] = acc_ref[...].astype(BF)
        attention_backward_into(qkv_ref, do_ref, out_ref, dk_ref, dv_ref, rows, groups, hd, scale)
    return epilogue


def whole(shape):
    return pl.BlockSpec(shape, lambda i: (0,) * len(shape), pipeline_mode=pl.Buffered(1))


def whole_out(shape):
    return pl.BlockSpec(shape, lambda i: (0,) * len(shape))


ANY = pl.BlockSpec(memory_space=pl.ANY)


class Segment:
    def __init__(self, kind, layer_idx, seq, groups, hd, operands, chunk=512):
        self.kind, self.operands, self.chunk, self.seq = kind, list(operands), chunk, seq
        self.heads = (min(128, seq), groups, hd, hd ** -0.5)
        slots, q_cols = groups + 2, groups * hd
        first = operands[0]
        cols = first.shape[1]

        def chunk_spec(at, major):
            return pl.BlockSpec((1, major, chunk), lambda i: (layer_idx, 0, at(i)))
        if kind == 'qkv_attn':
            self.body = qkv_attn_body
            self.specs = lambda at: [pl.BlockSpec((1, slots, chunk, hd), lambda i: (layer_idx, 0, at(i), 0))]
            self.outs = [((seq, slots * hd), BF), ((seq, q_cols), BF)]
            self.scratch = [pltpu.VMEM((seq, slots * hd), F32)]
        elif kind == 'gate_up':
            self.body = gate_up_body
            self.specs = lambda at: [chunk_spec(at, cols)] * 2
            self.outs = [((cols, seq), F32), ((cols, seq), F32), ((cols, seq), BF), ((seq, cols), BF)]
            self.scratch = []
        elif kind == 'inner_grad':
            self.body = inner_grad_body
            self.specs = lambda at: [chunk_spec(at, cols), whole((cols, seq)), whole((cols, seq))]
            self.outs = [((cols, seq), BF), ((cols, seq), BF), ((seq, cols), BF), ((seq, cols), BF)]
            self.scratch = [pltpu.VMEM((cols, seq), F32)]
        else:
            self.body = mix_grad_body
            self.specs = lambda at: [chunk_spec(at, q_cols), whole((seq, slots * hd))]
            self.outs = [((seq, slots * hd), BF)]
            self.scratch = [pltpu.VMEM((seq, q_cols), F32), pltpu.VMEM((seq, q_cols), BF), pltpu.VMEM((seq, hd), F32), pltpu.VMEM((seq, hd), F32)]


class WeightGrad:
    def __init__(self, lefts, rights, stacked, layer_idx, layer_count, slots=0, flipped=False, tile=512):
        self.lefts, self.rights, self.stacked = list(lefts), list(rights), stacked
        self.layer_idx, self.slots, self.tile = layer_idx, slots, tile
        self.flipped = flipped
        self.seq = rights[0].shape[0]
        self.rows = rows = lefts[0].shape[0 if flipped else 1]
        cols = rights[0].shape[1]
        self.steps = (rows if slots else cols) // tile
        self.shape = (layer_count, slots, rows, cols // slots) if slots else (layer_count, rows, cols)
        self.flops = 2 * len(self.lefts) * self.seq * rows * cols
        self.ref_count = len(self.lefts) * 2 + (stacked is not None)

    def specs(self, at):
        rows, cols = self.rows, self.rights[0].shape[1]
        count, layer_idx = len(self.lefts), self.layer_idx
        part = pl.BlockSpec((self.seq, self.tile), lambda i: (0, at(i)))
        if self.slots:
            ins = [part] * count + [whole((self.seq, cols))] * count
            out = pl.BlockSpec((1, self.slots, self.tile, cols // self.slots), lambda i: (layer_idx, 0, at(i), 0))
        else:
            ins = [whole(self.lefts[0].shape)] * count + [part] * count
            out = pl.BlockSpec((1, rows, self.tile), lambda i: (layer_idx, 0, at(i)))
        args = self.lefts + self.rights
        if self.stacked is not None:
            ins.append(ANY)
            args = args + [self.stacked]
        return ins, args, out

    def compute(self, refs, out_ref):
        count = len(self.lefts)
        depth = 1 if self.flipped else 0
        left = jnp.concatenate([refs[m][...] for m in range(count)], axis=depth)
        right = jnp.concatenate([refs[count + m][...] for m in range(count)], axis=0)
        total = lax.dot_general(left, right, (((depth,), (0,)), ((), ())), preferred_element_type=F32)
        if self.slots:
            hd = total.shape[1] // self.slots
            for j in range(self.slots):
                out_ref[0, j] = total[:, j * hd:(j + 1) * hd].astype(BF)
        else:
            out_ref[0] = total.astype(BF)


def weight_grad_stack(job, upper, tokens):
    ins, args, out = job.specs(lambda i: i)
    slots, rows, tile = job.slots, job.rows, job.tile
    hd = upper.shape[-1]
    if slots:
        upper_spec = out
        out_spec = pl.BlockSpec((2, slots, tile, hd), lambda i: (0, 0, i, 0))
    else:
        upper_spec = out
        out_spec = pl.BlockSpec((2, rows, tile), lambda i: (0, 0, i))

    count = len(args)

    def kernel(*refs):
        job.compute(refs[:count], refs[-1])
        refs[-1][1] = refs[count][0]
    return pl.pallas_call(
        kernel, grid=(job.steps,), out_shape=jax.ShapeDtypeStruct((2,) + upper.shape[1:], BF), in_specs=ins + [upper_spec] + [ANY] * len(tokens), out_specs=out_spec,
        name='weight_grad', cost_estimate=pl.CostEstimate(flops=8 * job.flops, bytes_accessed=0, transcendentals=0),
    )(*args, upper, *tokens)


TAIL_INS = {'none': 0, 'add': 1, 'norm': 2, 'back': 3}
TAIL_OUTS = {'none': 0, 'add': 1, 'norm': 2, 'back': 2}


class RowTail:
    def __init__(self, tail, ins, outs, sum_ref):
        self.tail, self.ins, self.outs, self.sum_ref = tail, ins, outs, sum_ref
        self.square = self.slope = None

    def tile(self, cols, value):
        value = value.astype(BF)
        if self.tail == 'back':
            self.sum_ref[:, cols] = value
            x = self.ins[1][:, cols].astype(F32)
            term = x * (value.astype(F32) * self.ins[2][:, cols])
            self.slope = term if self.slope is None else self.slope + term
        else:
            total = (self.ins[0][:, cols].astype(F32) + value.astype(F32)).astype(BF)
            self.outs[0][:, cols] = total
            x = total.astype(F32)
        self.square = x * x if self.square is None else self.square + x * x

    def end(self, width, tile):
        if self.tail == 'add':
            return
        r = lax.rsqrt(jnp.sum(self.square, axis=-1, keepdims=True) / width + NORM_EPS)
        if self.tail == 'back':
            back = r * r * r * (jnp.sum(self.slope, axis=-1, keepdims=True) / width)
        for col in range(0, width, tile):
            cols = slice(col, col + tile)
            if self.tail == 'back':
                value = self.sum_ref[:, cols].astype(F32)
                x = self.ins[1][:, cols].astype(F32)
                row = self.ins[0][:, cols].astype(F32)
                self.outs[0][:, cols] = (row + (r * (value * self.ins[2][:, cols]) - x * back)).astype(BF)
                self.outs[1][:, cols] = jnp.sum(value * (x * r), axis=0, keepdims=True)
            else:
                x = self.outs[0][:, cols].astype(F32)
                self.outs[1][:, cols] = (x * r * self.ins[1][:, cols]).astype(BF)


def half_step_kernel(*refs, left_count, slots, shard, tile, steps, y_first, tail, seg, jobs):
    taken = 0

    def take(count):
        nonlocal taken
        taken += count
        return refs[taken - count:taken]
    lefts, weights = take(left_count), take(2 * left_count)
    tail_ins = take(TAIL_INS[tail])
    rows_ref, = take(1) if seg else (None,)
    seg_ins = take(len(seg.operands)) if seg else ()
    job_refs = [take(job.ref_count) for job in jobs]
    tail_outs = take(TAIL_OUTS[tail])
    full_out, = take(1) if seg else (None,)
    seg_outs = take(len(seg.outs)) if seg else ()
    job_outs = take(len(jobs))
    sorted_refs = take(left_count)
    acc, send1, recv1, send2, recv2, send3, recv3, sum_ref, sem = take(9) if left_count else (None,) * 9
    full_ref, gsem, out_sem = take(3) if seg else (None,) * 3
    seg_scratch = take(len(seg.scratch)) if seg else ()
    step = pl.program_id(0)
    me = lax.axis_index('tp')
    core, xpos, ypos = lax.rem(me, 2), lax.rem(me // 2, 2), me // 4
    pair, xpeer, ypeer = me + 1 - 2 * core, me + 2 - 4 * xpos, me + 4 - 8 * ypos

    def route(side, g):
        flag = jnp.where(g < y_first, side, 0) if not isinstance(g, int) else side * int(g < y_first)
        mine, other = xpos + flag * (ypos - xpos), ypos + flag * (xpos - ypos)
        first, second = xpeer + flag * (ypeer - xpeer), ypeer + flag * (xpeer - ypeer)
        return flag, mine, other, first, second

    def copy(stage, side, g):
        flag, mine, other, first, second = route(side, g)
        src, dst, to = ((send1, recv1, pair), (send2, recv2, first), (send3, recv3, second))[stage]
        return pltpu.make_async_remote_copy(src_ref=src.at[side, g], dst_ref=dst.at[side, g], send_sem=sem.at[2 * stage, side, g],
                                            recv_sem=sem.at[2 * stage + 1, side, g], device_id={'tp': to},
                                            device_id_type=pl.DeviceIdType.MESH)

    def chip(flag, mine, other):
        return (1 + flag) * mine + (2 - flag) * other

    def block(owner, side=None):
        span = pl.ds(pl.multiple_of(owner * shard, shard), shard)
        half = full_ref.shape[1] // 2
        return full_ref.at[span, :] if side is None else full_ref.at[span, side * half:(side + 1) * half]

    def gather_copy(n):
        half = rows_ref.shape[1] // 2 if rows_ref is not None else 0
        diag = xpeer + ypeer - me
        peers = (xpeer, ypeer)
        if n < 4:
            side = n % 2
            src, dst, to = rows_ref.at[:, side * half:(side + 1) * half], block(me, side), peers[side if n < 2 else 1 - side]
        elif n < 6:
            side = n % 2
            src, dst, to = block(peers[side], side), block(peers[side], side), peers[1 - side]
        elif n == 6:
            src, dst, to = rows_ref, block(me), pair
        else:
            side = (n - 7) % 2
            owner = (peers[side], peers[1 - side], diag)[(n - 7) // 2]
            src, dst, to = block(owner, side), block(owner, side), pair
        return pltpu.make_async_remote_copy(src_ref=src, dst_ref=dst, send_sem=gsem.at[0, n], recv_sem=gsem.at[1, n],
                                            device_id={'tp': to}, device_id_type=pl.DeviceIdType.MESH)

    def gather_start():
        for n in (0, 1, 6, 2, 3):
            gather_copy(n).start()
        full_ref[pl.ds(pl.multiple_of(me * shard, shard), shard), :] = rows_ref[...]

    def gather_relay():
        for side in range(2):
            gather_copy(side).wait_recv()
            gather_copy(4 + side).start()
            gather_copy(7 + side).start()

    def gather_finish():
        for n in (2, 3, 4, 5):
            gather_copy(n).wait_recv()
            gather_copy(7 + n).start()
        for n in range(6, 13):
            gather_copy(n).wait_recv()
        for n in range(13):
            gather_copy(n).wait_send()
        pltpu.make_async_copy(full_ref, full_out, out_sem).start()

    @pl.when(step == 0)
    def _():
        barrier = pltpu.get_barrier_semaphore()
        for peer in (pair, xpeer, ypeer):
            pl.semaphore_signal(barrier, inc=1, device_id={'tp': peer}, device_id_type=pl.DeviceIdType.MESH)
        pl.semaphore_wait(barrier, 3)
        if seg:
            gather_start()
        for i in range(left_count):
            for c in range(4):
                for part, which in ((0, 1 - core), (1, core)):
                    start = pl.multiple_of(c * 2 * shard + which * shard, shard)
                    sorted_refs[i][(part * 4 + c) * shard:(part * 4 + c + 1) * shard, :] = lefts[i][pl.ds(start, shard), :]

    def produce():
        for side in range(2):
            total = None
            for i in range(left_count):
                w_ref = weights[2 * i + side]
                if slots:
                    w = jnp.concatenate([w_ref[0, j] for j in range(slots)], axis=1)
                    term = dot_tt(sorted_refs[i][...], w)
                else:
                    term = jnp.dot(sorted_refs[i][...], w_ref[0], preferred_element_type=F32)
                total = term if total is None else total + term
            for c in range(4):
                send1[side, step, c] = total[c * shard:(c + 1) * shard]
                acc[side, step, c] = total[(4 + c) * shard:(5 + c) * shard]
            copy(0, side, step).start()

    def chip_sum(g):
        for side in range(2):
            copy(0, side, g).wait_recv()
            flag, mine = route(side, g)[:2]
            for other in range(2):
                away, keep = chip(flag, 1 - mine, other), chip(flag, mine, other)
                send2[side, g, other] = acc[side, g, away] + recv1[side, g, away]
                acc[side, g, keep] = acc[side, g, keep] + recv1[side, g, keep]
            copy(1, side, g).start()

    def second_link(g):
        for side in range(2):
            copy(1, side, g).wait_recv()
            flag, mine, other = route(side, g)[:3]
            send3[side, g] = acc[side, g, chip(flag, mine, 1 - other)] + recv2[side, g, 1 - other]
            acc[side, g, chip(flag, mine, other)] = acc[side, g, chip(flag, mine, other)] + recv2[side, g, other]
            copy(2, side, g).start()

    def finish():
        rows_end = RowTail(tail, tail_ins, tail_outs, sum_ref)
        for g in range(steps):
            for side in range(2):
                copy(2, side, g).wait_recv()
                flag, mine, other = route(side, g)[:3]
                col = (side * steps + g) * tile
                rows_end.tile(slice(col, col + tile), acc[side, g, chip(flag, mine, other)] + recv3[side, g])
        rows_end.end(2 * steps * tile, tile)
        for stage in range(3):
            for g in range(steps):
                for side in range(2):
                    copy(stage, side, g).wait_send()

    if left_count:
        relay_step = 2 if seg else 0

        @pl.when(step < steps)
        def _():
            produce()

        if seg:
            @pl.when(step == relay_step)
            def _():
                gather_relay()
                for g in range(relay_step):
                    chip_sum(g)

        @pl.when((step > relay_step) & (step < steps))
        def _():
            chip_sum(step - 1)

        @pl.when(step == steps - 1)
        def _():
            chip_sum(steps - 1)
    else:
        @pl.when(step == 0)
        def _():
            gather_relay()

    start = steps if left_count else 0
    for n, job in enumerate(jobs):
        @pl.when((step >= start) & (step < start + job.steps))
        def _(job=job, n=n):
            job.compute(job_refs[n], job_outs[n])
        start += job.steps

    if seg:
        @pl.when(step == start)
        def _():
            gather_finish()

        @pl.when(step >= start)
        def _():
            j = step - start
            left = full_ref[:, pl.ds(pl.multiple_of(j * seg.chunk, seg.chunk), seg.chunk)]
            epilogue = seg.body(j, left, seg_ins, seg_outs, seg_scratch, seg.heads)
            if left_count:
                second_link(j)

            @pl.when(j == steps - 1)
            def _():
                epilogue()
        start += steps

    @pl.when(step == start - 1)
    def _():
        if seg:
            pltpu.make_async_copy(full_ref, full_out, out_sem).wait()
        else:
            for g in range(steps):
                second_link(g)
        if left_count:
            finish()


def half_step(lefts, weights, layer_idx, shard, call_id, tail, tail_ins, slots=0, seg=None, rows=None, jobs=(), y_first=5, tile=256):
    width = weights[0].shape[2] if lefts else rows.shape[1]
    steps = width // tile // 2
    seq = lefts[0].shape[0] if lefts else seg.seq
    in_specs = [whole(a.shape) for a in lefts]
    args = list(lefts)
    for w in weights:
        for side in range(2):
            if slots:
                in_specs.append(pl.BlockSpec((1, slots, tile, w.shape[3]),
                                             lambda i, s=side: (layer_idx, 0, s * steps + jnp.minimum(i, steps - 1), 0)))
            else:
                in_specs.append(pl.BlockSpec((1, w.shape[1], tile), lambda i, s=side: (layer_idx, 0, s * steps + jnp.minimum(i, steps - 1))))
            args.append(w)
    in_specs += [whole(a.shape) for a in tail_ins]
    args += list(tail_ins)
    seg_start = (steps if lefts else 0) + sum(job.steps for job in jobs)
    if seg:
        in_specs += [whole(rows.shape)] + seg.specs(lambda i: jnp.clip(i - seg_start, 0, steps - 1))
        args += [rows] + seg.operands
    second = {'none': [], 'add': [], 'norm': [((shard, width), BF)], 'back': [((1, width), F32)]}[tail]
    out_shapes = [jax.ShapeDtypeStruct(*o) for o in ([((shard, width), BF)] if lefts else []) + second]
    out_specs, aliases = [whole_out(o.shape) for o in out_shapes], {}
    if seg:
        out_shapes += [jax.ShapeDtypeStruct((seq, width), BF)] + [jax.ShapeDtypeStruct(*o) for o in seg.outs]
        out_specs += [ANY] + [whole_out(o[0]) for o in seg.outs]
    start = steps
    for job in jobs:
        ins, job_args, out = job.specs(lambda i, start=start, last=job.steps - 1: jnp.clip(i - start, 0, last))
        in_specs += ins
        args += job_args
        if job.stacked is not None:
            aliases[len(args) - 1] = len(out_shapes)
        out_specs.append(out)
        out_shapes.append(jax.ShapeDtypeStruct(job.shape, BF))
        start += job.steps
    big = pltpu.VMEM((2, steps, 4, shard, tile), F32)
    mid = pltpu.VMEM((2, steps, 2, shard, tile), F32)
    small = pltpu.VMEM((2, steps, shard, tile), F32)
    scratch = [pltpu.VMEM(a.shape, BF) for a in lefts]
    if lefts:
        scratch += [big, big, big, mid, mid, small, small, pltpu.VMEM((shard, width), BF), pltpu.SemaphoreType.DMA((6, 2, steps))]
    if seg:
        scratch += [pltpu.VMEM((seq, width), BF), pltpu.SemaphoreType.DMA((2, 13)), pltpu.SemaphoreType.DMA] + seg.scratch
    return pl.pallas_call(
        functools.partial(half_step_kernel, left_count=len(lefts), slots=slots, shard=shard, tile=tile, steps=steps,
                          y_first=y_first, tail=tail, seg=seg, jobs=tuple(jobs)),
        grid=(seg_start + (steps if seg else 0),),
        out_shape=out_shapes,
        in_specs=in_specs,
        out_specs=out_specs,
        input_output_aliases=aliases,
        scratch_shapes=scratch,
        compiler_params=pltpu.CompilerParams(collective_id=call_id, has_side_effects=True, vmem_limit_bytes=67000000),
        name='half_step',
    )(*args)


def solution(mesh):
    row_spec = P(None, ('dp', 'tp'), None)
    gain_spec = P(None, None)
    qkv_spec = P(None, None, 'tp', None, None)
    head_spec = P(None, 'tp', None, None)
    col_spec = P(None, None, 'tp')
    row_shard_spec = P(None, 'tp', None)
    tp = mesh.shape['tp']
    swap = {flip: [(t, t ^ flip) for t in range(tp)] for flip in (1, 2, 4)}

    def device_program(x_in, y_cot, gain_attn, gain_mlp, w_qkv, w_out, w_gate, w_up, w_down):
        micro_count, shard, width = x_in.shape
        layer_count = w_qkv.shape[0]
        groups = w_qkv.shape[3] - 2
        hd = w_qkv.shape[4]
        slots = groups + 2
        wq = jnp.transpose(w_qkv[:, :, 0], (0, 2, 1, 3))
        wo = w_out.reshape(layer_count, groups * hd, width)
        wg, wu = jnp.swapaxes(w_gate, 1, 2), jnp.swapaxes(w_up, 1, 2)

        micros = range(micro_count)
        gain_a, gain_b = gain_attn[:, None], gain_mlp[:, None]
        top = layer_count - 1
        plan = [(kind, l) for l in range(layer_count) for kind in ('qkv_attn', 'gate_up')]
        plan += [(kind, l) for l in reversed(range(layer_count)) for kind in ('inner_grad', 'mix_grad')]
        kept = [[{} for l in range(layer_count)] for m in micros]
        rows_in = [norm_apply(x_in[m], gain_attn[0]) for m in micros]
        for m in micros:
            kept[m][0]['x'] = x_in[m]
        y_rows, grad_x = [None] * micro_count, [None] * micro_count
        gains_a = [[None] * micro_count for l in range(layer_count)]
        gains_b = [[None] * micro_count for l in range(layer_count)]
        stacks = [None] * 5
        waiting = []

        def segment(m, s):
            kind, l = plan[s]
            keep = kept[m][l]
            operands = {'qkv_attn': lambda: [wq], 'gate_up': lambda: [wg, wu], 'inner_grad': lambda: [w_down, keep['gate'], keep['up']],
                        'mix_grad': lambda: [wo, keep['qkv']]}[kind]()
            return Segment(kind, l, shard * tp, groups, hd, operands)

        def store(m, s, full, outs):
            kind, l = plan[s]
            keep = kept[m][l]
            names = {'qkv_attn': ('u', 'qkv', 'mix'), 'gate_up': ('v', 'gate', 'up', 'inner_t', 'inner'),
                     'inner_grad': ('gy', 'gg_t', 'gu_t', 'gg', 'gu'), 'mix_grad': ('gh', 'gq')}[kind]
            keep.update(zip(names, [full] + list(outs)))
            if m == micro_count - 1 and kind == 'inner_grad':
                for which, left, right in ((2, 'gg_t', 'v'), (3, 'gu_t', 'v'), (4, 'inner_t', 'gy')):
                    waiting.append((which, [kept[i][l][left] for i in micros], [kept[i][l][right] for i in micros], l, 0, True))
            if m == micro_count - 1 and kind == 'mix_grad':
                waiting.append((1, [kept[i][l]['mix'] for i in micros], [kept[i][l]['gh'] for i in micros], l))
                waiting.append((0, [kept[i][l]['u'] for i in micros], [kept[i][l]['gq'] for i in micros], l, slots))

        def scatter(call, m, s, next_m, next_s, job_count):
            kind, l = plan[s]
            keep = kept[m][l]
            lefts, weights, slot_count = {'qkv_attn': ([keep.get('mix')], [wo], 0), 'gate_up': ([keep.get('inner')], [w_down], 0),
                                          'inner_grad': ([keep.get('gg'), keep.get('gu')], [wg, wu], 0),
                                          'mix_grad': ([keep.get('gq')], [wq], slots)}[kind]
            if kind == 'qkv_attn':
                tail, tail_ins = 'norm', [keep['x'], gain_b[l]]
            elif kind == 'gate_up' and l < top:
                tail, tail_ins = 'norm', [keep['h'], gain_a[l + 1]]
            elif kind == 'gate_up':
                tail, tail_ins = 'add', [keep['h']]
            elif kind == 'inner_grad':
                tail, tail_ins = 'back', [rows_in[m], keep['h'], gain_b[l]]
            else:
                tail, tail_ins = 'back', [rows_in[m], keep['x'], gain_a[l]]
            seg = segment(next_m, next_s) if next_m is not None else None
            picked = [waiting.pop(0) for i in range(min(job_count, len(waiting)))]
            jobs = [WeightGrad(p[1], p[2], None, 0, 1, *p[4:]) for p in picked]
            outs = half_step(lefts, weights, l, shard, call, tail, tail_ins, slot_count, seg,
                             rows_in[next_m] if seg else None, jobs)
            head, outs = outs[:TAIL_OUTS[tail]], outs[TAIL_OUTS[tail]:]
            if seg:
                seg_outs, outs = outs[:1 + len(seg.outs)], outs[1 + len(seg.outs):]
                store(next_m, next_s, seg_outs[0], seg_outs[1:])
            for p, arr in zip(picked, outs):
                stacks[p[0]] = arr
            if kind == 'qkv_attn':
                keep['h'], rows_in[m] = head
            elif kind == 'gate_up' and l < top:
                kept[m][l + 1]['x'], rows_in[m] = head
            elif kind == 'gate_up':
                y_rows[m], rows_in[m] = head[0], y_cot[m]
            else:
                rows_in[m] = head[0]
                (gains_b if kind == 'inner_grad' else gains_a)[l][m] = head[1]
                grad_x[m] = head[0]

        first_full, *first_outs = half_step([], [], 0, shard, micro_count * len(plan) + 1, 'none', [], 0, segment(0, 0), rows_in[0])
        store(0, 0, first_full, first_outs)
        job_counts = {10: 2, 11: 1, 12: 1, 13: 1}
        total = micro_count * len(plan)
        for call in range(total):
            m, s = call % micro_count, call // micro_count
            next_m, next_s = (call + 1) % micro_count, (call + 1) // micro_count
            scatter(call + 1, m, s, next_m if call + 1 < total else None, next_s, job_counts.get(call, 0))
        gains_a = [sum(parts[1:], parts[0]) for parts in gains_a]
        gains_b = [sum(parts[1:], parts[0]) for parts in gains_b]
        gains = jnp.concatenate(gains_a + gains_b)
        flips = [1, 2, 4]
        for n, p in enumerate(waiting):
            tokens = [gains] if n and flips else []
            stacks[p[0]] = weight_grad_stack(WeightGrad(p[1], p[2], None, 0, 1, *p[4:]), stacks[p[0]], tokens)
            if n % 2 == 0 and flips:
                gains = gains + lax.ppermute(gains, 'tp', swap[flips.pop(0)])
        for flip in flips:
            gains = gains + lax.ppermute(gains, 'tp', swap[flip])
        return (jnp.stack(y_rows), jnp.stack(grad_x), jnp.transpose(stacks[0], (0, 2, 1, 3))[:, :, None], stacks[1].reshape(w_out.shape),
                jnp.swapaxes(stacks[2], 1, 2), jnp.swapaxes(stacks[3], 1, 2), stacks[4], gains[:layer_count], gains[layer_count:])

    return jax.shard_map(device_program, mesh=mesh,
                         in_specs=(row_spec, row_spec, gain_spec, gain_spec, qkv_spec, head_spec, col_spec, col_spec, row_shard_spec),
                         out_specs=(row_spec, row_spec, P('dp', None, 'tp', None, None), P('dp', 'tp', None, None), P('dp', None, 'tp'), P('dp', None, 'tp'), P('dp', 'tp', None), P('dp', None), P('dp', None)),
                         check_vma=False)
```

```python
import functools

import jax
import jax.numpy as jnp
from jax import lax
from jax.experimental import pallas as pl
from jax.experimental.pallas import tpu as pltpu
from jax.sharding import PartitionSpec as P

NORM_EPS = 1e-5
BF = jnp.bfloat16
F32 = jnp.float32


def rms_scale(row_vals, gain_vec):
    return row_vals * lax.rsqrt(jnp.mean(row_vals * row_vals, axis=-1, keepdims=True) + NORM_EPS) * gain_vec


def norm_apply(row_vals, gain_vec):
    return rms_scale(row_vals.astype(F32), gain_vec).astype(BF)


def block_probs(qkv_ref, blk, rows, groups, hd, scale):
    limit = (blk + 1) * rows
    span = pl.ds(blk * rows, rows)
    q = jnp.concatenate([qkv_ref[span, j * hd:(j + 1) * hd] for j in range(groups)], axis=0)
    k = qkv_ref[0:limit, groups * hd:(groups + 1) * hd]
    s = lax.dot_general(q, k, (((1,), (1,)), ((), ())), preferred_element_type=F32) * scale
    row_pos = lax.rem(lax.broadcasted_iota(jnp.int32, s.shape, 0), rows) + blk * rows
    col_pos = lax.broadcasted_iota(jnp.int32, s.shape, 1)
    s = jnp.where(row_pos >= col_pos, s, -1e30)
    e = jnp.exp(s - jnp.max(s, axis=-1, keepdims=True))
    p = e * (1.0 / jnp.sum(e, axis=-1, keepdims=True))
    return q, k, p, limit, span


def attention_forward_into(qkv_ref, o_ref, rows, groups, hd, scale):
    seq = qkv_ref.shape[0]
    for blk in range(seq // rows):
        q, k, p, limit, span = block_probs(qkv_ref, blk, rows, groups, hd, scale)
        v = qkv_ref[0:limit, (groups + 1) * hd:(groups + 2) * hd]
        o = jnp.dot(p.astype(BF), v, preferred_element_type=F32).astype(BF)
        for j in range(groups):
            o_ref[span, j * hd:(j + 1) * hd] = o[j * rows:(j + 1) * rows]


def attention_backward_into(qkv_ref, do_ref, out_ref, dk_ref, dv_ref, rows, groups, hd, scale):
    seq = qkv_ref.shape[0]
    blocks = seq // rows
    for blk in reversed(range(blocks)):
        q, k, p, limit, span = block_probs(qkv_ref, blk, rows, groups, hd, scale)
        v = qkv_ref[0:limit, (groups + 1) * hd:(groups + 2) * hd]
        do = jnp.concatenate([do_ref[span, j * hd:(j + 1) * hd] for j in range(groups)], axis=0)
        dp = lax.dot_general(do, v, (((1,), (1,)), ((), ())), preferred_element_type=F32).astype(BF).astype(F32)
        row_dot = jnp.sum(dp * p, axis=-1, keepdims=True)
        ds = (p * (dp - row_dot) * scale).astype(BF)
        dq = jnp.dot(ds, k, preferred_element_type=F32).astype(BF)
        for j in range(groups):
            out_ref[span, j * hd:(j + 1) * hd] = dq[j * rows:(j + 1) * rows]
        dk = lax.dot_general(ds, q, (((0,), (0,)), ((), ())), preferred_element_type=F32)
        dv = lax.dot_general(p.astype(BF), do, (((0,), (0,)), ((), ())), preferred_element_type=F32)
        if blk == blocks - 1:
            dk_ref[...] = dk
            dv_ref[...] = dv
        else:
            dk_ref[0:limit] += dk
            dv_ref[0:limit] += dv
    out_ref[:, groups * hd:(groups + 1) * hd] = dk_ref[...].astype(BF)
    out_ref[:, (groups + 1) * hd:(groups + 2) * hd] = dv_ref[...].astype(BF)


def accumulate(step, acc_ref, term):
    @pl.when(step == 0)
    def _():
        acc_ref[...] = term

    @pl.when(step > 0)
    def _():
        acc_ref[...] += term


def dot_tt(a, b):
    return lax.dot_general(a, b, (((1,), (1,)), ((), ())), preferred_element_type=F32)


def qkv_attn_body(j, left, ins, outs, scratch, heads):
    (w_ref,), (qkv_ref, o_ref), (acc_ref,) = ins, outs, scratch
    rows, groups, hd, scale = heads
    w = jnp.concatenate([w_ref[0, i] for i in range(groups + 2)], axis=1)
    accumulate(j, acc_ref, jnp.dot(left, w, preferred_element_type=F32))

    def epilogue():
        qkv_ref[...] = acc_ref[...].astype(BF)
        attention_forward_into(qkv_ref, o_ref, rows, groups, hd, scale)
    return epilogue


def gate_up_body(j, left, ins, outs, scratch, heads):
    (wg_ref, wu_ref), (gate_ref, up_ref, inner_t_ref, inner_ref) = ins, outs
    accumulate(j, gate_ref, dot_tt(wg_ref[0], left))
    accumulate(j, up_ref, dot_tt(wu_ref[0], left))

    def epilogue():
        @pl.loop(0, gate_ref.shape[0] // 32)
        def _(i):
            span = pl.ds(pl.multiple_of(i * 32, 32), 32)
            gate = gate_ref[span, :]
            inner_t_ref[span, :] = (gate * jax.nn.sigmoid(gate) * up_ref[span, :]).astype(BF)
        inner_ref[...] = inner_t_ref[...].T
    return epilogue


def inner_grad_body(j, left, ins, outs, scratch, heads):
    (wd_ref, gate_hbm, up_hbm), (ggt_ref, gut_ref, gg_ref, gu_ref), (acc_ref, gate_ref, up_ref, in_sem) = ins, outs, scratch
    accumulate(j, acc_ref, dot_tt(wd_ref[0], left))

    def epilogue():
        pltpu.make_async_copy(gate_hbm, gate_ref, in_sem.at[0]).wait()
        pltpu.make_async_copy(up_hbm, up_ref, in_sem.at[1]).wait()

        @pl.loop(0, gate_ref.shape[0] // 32)
        def _(i):
            span = pl.ds(pl.multiple_of(i * 32, 32), 32)
            gate, up = gate_ref[span, :], up_ref[span, :]
            sig = jax.nn.sigmoid(gate)
            gi = acc_ref[span, :].astype(BF).astype(F32)
            gut_ref[span, :] = (gi * (gate * sig)).astype(BF)
            ggt_ref[span, :] = (gi * up * sig * (1.0 + gate * (1.0 - sig))).astype(BF)
        gg_ref[...] = ggt_ref[...].T
        gu_ref[...] = gut_ref[...].T
    return epilogue


def mix_grad_body(j, left, ins, outs, scratch, heads):
    (wo_ref, qkv_ref), (out_ref,), (acc_ref, do_ref, dk_ref, dv_ref) = ins, outs, scratch
    rows, groups, hd, scale = heads
    accumulate(j, acc_ref, dot_tt(left, wo_ref[0]))

    def epilogue():
        do_ref[...] = acc_ref[...].astype(BF)
        attention_backward_into(qkv_ref, do_ref, out_ref, dk_ref, dv_ref, rows, groups, hd, scale)
    return epilogue


def whole(shape):
    return pl.BlockSpec(shape, lambda i: (0,) * len(shape), pipeline_mode=pl.Buffered(1))


def whole_out(shape):
    return pl.BlockSpec(shape, lambda i: (0,) * len(shape))


ANY = pl.BlockSpec(memory_space=pl.ANY)


class Segment:
    def __init__(self, kind, layer_idx, seq, groups, hd, operands, chunk=512):
        self.kind, self.operands, self.chunk, self.seq = kind, list(operands), chunk, seq
        self.heads = (min(128, seq), groups, hd, hd ** -0.5)
        slots, q_cols = groups + 2, groups * hd
        first = operands[0]
        cols = first.shape[1]

        def chunk_spec(at, major):
            return pl.BlockSpec((1, major, chunk), lambda i: (layer_idx, 0, at(i)))
        if kind == 'qkv_attn':
            self.body = qkv_attn_body
            self.specs = lambda at: [pl.BlockSpec((1, slots, chunk, hd), lambda i: (layer_idx, 0, at(i), 0))]
            self.outs = [((seq, slots * hd), BF), ((seq, q_cols), BF)]
            self.scratch = [pltpu.VMEM((seq, slots * hd), F32)]
        elif kind == 'gate_up':
            self.body = gate_up_body
            self.specs = lambda at: [chunk_spec(at, cols)] * 2
            self.outs = [((cols, seq), F32), ((cols, seq), F32), ((cols, seq), BF), ((seq, cols), BF)]
            self.scratch = []
        elif kind == 'inner_grad':
            self.body = inner_grad_body
            self.specs = lambda at: [chunk_spec(at, cols), ANY, ANY]
            self.outs = [((cols, seq), BF), ((cols, seq), BF), ((seq, cols), BF), ((seq, cols), BF)]
            self.scratch = [pltpu.VMEM((cols, seq), F32)] * 3 + [pltpu.SemaphoreType.DMA((2,))]
        else:
            self.body = mix_grad_body
            self.specs = lambda at: [chunk_spec(at, q_cols), whole((seq, slots * hd))]
            self.outs = [((seq, slots * hd), BF)]
            self.scratch = [pltpu.VMEM((seq, q_cols), F32), pltpu.VMEM((seq, q_cols), BF), pltpu.VMEM((seq, hd), F32), pltpu.VMEM((seq, hd), F32)]


class WeightGrad:
    def __init__(self, lefts, rights, stacked, layer_idx, layer_count, slots=0, flipped=False, tile=512):
        self.lefts, self.rights, self.stacked = list(lefts), list(rights), stacked
        self.layer_idx, self.slots, self.tile = layer_idx, slots, tile
        self.flipped = flipped
        self.seq = rights[0].shape[0]
        self.rows = rows = lefts[0].shape[0 if flipped else 1]
        cols = rights[0].shape[1]
        self.steps = (rows if slots else cols) // tile
        self.shape = (layer_count, slots, rows, cols // slots) if slots else (layer_count, rows, cols)
        self.flops = 2 * len(self.lefts) * self.seq * rows * cols
        self.ref_count = len(self.lefts) * 2 + (stacked is not None)

    def specs(self, at):
        rows, cols = self.rows, self.rights[0].shape[1]
        count, layer_idx = len(self.lefts), self.layer_idx
        part = pl.BlockSpec((self.seq, self.tile), lambda i: (0, at(i)))
        if self.slots:
            ins = [part] * count + [whole((self.seq, cols))] * count
            out = pl.BlockSpec((1, self.slots, self.tile, cols // self.slots), lambda i: (layer_idx, 0, at(i), 0))
        else:
            ins = [whole(self.lefts[0].shape)] * count + [part] * count
            out = pl.BlockSpec((1, rows, self.tile), lambda i: (layer_idx, 0, at(i)))
        args = self.lefts + self.rights
        if self.stacked is not None:
            ins.append(ANY)
            args = args + [self.stacked]
        return ins, args, out

    def compute(self, refs, out_ref):
        count = len(self.lefts)
        depth = 1 if self.flipped else 0
        left = jnp.concatenate([refs[m][...] for m in range(count)], axis=depth)
        right = jnp.concatenate([refs[count + m][...] for m in range(count)], axis=0)
        total = lax.dot_general(left, right, (((depth,), (0,)), ((), ())), preferred_element_type=F32)
        if self.slots:
            hd = total.shape[1] // self.slots
            for j in range(self.slots):
                out_ref[0, j] = total[:, j * hd:(j + 1) * hd].astype(BF)
        else:
            out_ref[0] = total.astype(BF)


def weight_grad_stack(job, upper, tokens):
    ins, args, out = job.specs(lambda i: i)
    slots, rows, tile = job.slots, job.rows, job.tile
    hd = upper.shape[-1]
    if slots:
        upper_spec = out
        out_spec = pl.BlockSpec((2, slots, tile, hd), lambda i: (0, 0, i, 0))
    else:
        upper_spec = out
        out_spec = pl.BlockSpec((2, rows, tile), lambda i: (0, 0, i))

    count = len(args)

    def kernel(*refs):
        job.compute(refs[:count], refs[-1])
        refs[-1][1] = refs[count][0]
    return pl.pallas_call(
        kernel, grid=(job.steps,), out_shape=jax.ShapeDtypeStruct((2,) + upper.shape[1:], BF), in_specs=ins + [upper_spec] + [ANY] * len(tokens), out_specs=out_spec,
        name='weight_grad', cost_estimate=pl.CostEstimate(flops=8 * job.flops, bytes_accessed=0, transcendentals=0),
    )(*args, upper, *tokens)


TAIL_INS = {'none': 0, 'add': 1, 'norm': 2, 'back': 3}
TAIL_OUTS = {'none': 0, 'add': 1, 'norm': 2, 'back': 2}


class RowTail:
    def __init__(self, tail, ins, outs, sum_ref):
        self.tail, self.ins, self.outs, self.sum_ref = tail, ins, outs, sum_ref
        self.square = self.slope = None

    def tile(self, cols, value):
        value = value.astype(BF)
        if self.tail == 'back':
            self.sum_ref[:, cols] = value
            x = self.ins[1][:, cols].astype(F32)
            term = x * (value.astype(F32) * self.ins[2][:, cols])
            self.slope = term if self.slope is None else self.slope + term
        else:
            total = (self.ins[0][:, cols].astype(F32) + value.astype(F32)).astype(BF)
            self.outs[0][:, cols] = total
            x = total.astype(F32)
        self.square = x * x if self.square is None else self.square + x * x

    def end(self, width, tile):
        if self.tail == 'add':
            return
        r = lax.rsqrt(jnp.sum(self.square, axis=-1, keepdims=True) / width + NORM_EPS)
        if self.tail == 'back':
            back = r * r * r * (jnp.sum(self.slope, axis=-1, keepdims=True) / width)
        for col in range(0, width, tile):
            cols = slice(col, col + tile)
            if self.tail == 'back':
                value = self.sum_ref[:, cols].astype(F32)
                x = self.ins[1][:, cols].astype(F32)
                row = self.ins[0][:, cols].astype(F32)
                self.outs[0][:, cols] = (row + (r * (value * self.ins[2][:, cols]) - x * back)).astype(BF)
                self.outs[1][:, cols] = jnp.sum(value * (x * r), axis=0, keepdims=True)
            else:
                x = self.outs[0][:, cols].astype(F32)
                self.outs[1][:, cols] = (x * r * self.ins[1][:, cols]).astype(BF)


def half_step_kernel(*refs, left_count, slots, shard, tile, steps, y_first, tail, seg, jobs):
    taken = 0

    def take(count):
        nonlocal taken
        taken += count
        return refs[taken - count:taken]
    lefts, weights = take(left_count), take(2 * left_count)
    tail_ins = take(TAIL_INS[tail])
    rows_ref, = take(1) if seg else (None,)
    seg_ins = take(len(seg.operands)) if seg else ()
    job_refs = [take(job.ref_count) for job in jobs]
    tail_outs = take(TAIL_OUTS[tail])
    full_out, = take(1) if seg else (None,)
    seg_outs = take(len(seg.outs)) if seg else ()
    job_outs = take(len(jobs))
    sorted_refs = take(left_count)
    acc, send1, recv1, send2, recv2, send3, recv3, sum_ref, sem = take(9) if left_count else (None,) * 9
    full_ref, gsem, out_sem = take(3) if seg else (None,) * 3
    seg_scratch = take(len(seg.scratch)) if seg else ()
    step = pl.program_id(0)
    me = lax.axis_index('tp')
    core, xpos, ypos = lax.rem(me, 2), lax.rem(me // 2, 2), me // 4
    pair, xpeer, ypeer = me + 1 - 2 * core, me + 2 - 4 * xpos, me + 4 - 8 * ypos

    def route(side, g):
        flag = jnp.where(g < y_first, side, 0) if not isinstance(g, int) else side * int(g < y_first)
        mine, other = xpos + flag * (ypos - xpos), ypos + flag * (xpos - ypos)
        first, second = xpeer + flag * (ypeer - xpeer), ypeer + flag * (xpeer - ypeer)
        return flag, mine, other, first, second

    def copy(stage, side, g):
        flag, mine, other, first, second = route(side, g)
        src, dst, to = ((send1, recv1, pair), (send2, recv2, first), (send3, recv3, second))[stage]
        return pltpu.make_async_remote_copy(src_ref=src.at[side, g], dst_ref=dst.at[side, g], send_sem=sem.at[2 * stage, side, g],
                                            recv_sem=sem.at[2 * stage + 1, side, g], device_id={'tp': to},
                                            device_id_type=pl.DeviceIdType.MESH)

    def chip(flag, mine, other):
        return (1 + flag) * mine + (2 - flag) * other

    def block(owner, side=None):
        span = pl.ds(pl.multiple_of(owner * shard, shard), shard)
        half = full_ref.shape[1] // 2
        return full_ref.at[span, :] if side is None else full_ref.at[span, side * half:(side + 1) * half]

    def gather_copy(n):
        half = rows_ref.shape[1] // 2 if rows_ref is not None else 0
        diag = xpeer + ypeer - me
        peers = (xpeer, ypeer)
        if n < 4:
            side = n % 2
            src, dst, to = rows_ref.at[:, side * half:(side + 1) * half], block(me, side), peers[side if n < 2 else 1 - side]
        elif n < 6:
            side = n % 2
            src, dst, to = block(peers[side], side), block(peers[side], side), peers[1 - side]
        elif n == 6:
            src, dst, to = rows_ref, block(me), pair
        else:
            side = (n - 7) % 2
            owner = (peers[side], peers[1 - side], diag)[(n - 7) // 2]
            src, dst, to = block(owner, side), block(owner, side), pair
        return pltpu.make_async_remote_copy(src_ref=src, dst_ref=dst, send_sem=gsem.at[0, n], recv_sem=gsem.at[1, n],
                                            device_id={'tp': to}, device_id_type=pl.DeviceIdType.MESH)

    def gather_start():
        for n in (0, 1, 6, 2, 3):
            gather_copy(n).start()
        full_ref[pl.ds(pl.multiple_of(me * shard, shard), shard), :] = rows_ref[...]

    def gather_relay():
        for side in range(2):
            gather_copy(side).wait_recv()
            gather_copy(4 + side).start()
            gather_copy(7 + side).start()

    def gather_finish():
        for n in (2, 3, 4, 5):
            gather_copy(n).wait_recv()
            gather_copy(7 + n).start()
        for n in range(6, 13):
            gather_copy(n).wait_recv()
        for n in range(13):
            gather_copy(n).wait_send()
        pltpu.make_async_copy(full_ref, full_out, out_sem).start()

    @pl.when(step == 0)
    def _():
        barrier = pltpu.get_barrier_semaphore()
        for peer in (pair, xpeer, ypeer):
            pl.semaphore_signal(barrier, inc=1, device_id={'tp': peer}, device_id_type=pl.DeviceIdType.MESH)
        pl.semaphore_wait(barrier, 3)
        if seg:
            gather_start()
        if seg and seg.kind == 'inner_grad':
            for i in range(2):
                pltpu.make_async_copy(seg_ins[1 + i], seg_scratch[1 + i], seg_scratch[3].at[i]).start()
        for i in range(left_count):
            for c in range(4):
                for part, which in ((0, 1 - core), (1, core)):
                    start = pl.multiple_of(c * 2 * shard + which * shard, shard)
                    sorted_refs[i][(part * 4 + c) * shard:(part * 4 + c + 1) * shard, :] = lefts[i][pl.ds(start, shard), :]

    def produce():
        for side in range(2):
            total = None
            for i in range(left_count):
                w_ref = weights[2 * i + side]
                if slots:
                    w = jnp.concatenate([w_ref[0, j] for j in range(slots)], axis=1)
                    term = dot_tt(sorted_refs[i][...], w)
                else:
                    term = jnp.dot(sorted_refs[i][...], w_ref[0], preferred_element_type=F32)
                total = term if total is None else total + term
            for c in range(4):
                send1[side, step, c] = total[c * shard:(c + 1) * shard]
                acc[side, step, c] = total[(4 + c) * shard:(5 + c) * shard]
            copy(0, side, step).start()

    def chip_sum(g):
        for side in range(2):
            copy(0, side, g).wait_recv()
            flag, mine = route(side, g)[:2]
            for other in range(2):
                away, keep = chip(flag, 1 - mine, other), chip(flag, mine, other)
                send2[side, g, other] = acc[side, g, away] + recv1[side, g, away]
                acc[side, g, keep] = acc[side, g, keep] + recv1[side, g, keep]
            copy(1, side, g).start()

    def second_link(g):
        for side in range(2):
            copy(1, side, g).wait_recv()
            flag, mine, other = route(side, g)[:3]
            send3[side, g] = acc[side, g, chip(flag, mine, 1 - other)] + recv2[side, g, 1 - other]
            acc[side, g, chip(flag, mine, other)] = acc[side, g, chip(flag, mine, other)] + recv2[side, g, other]
            copy(2, side, g).start()

    def finish():
        rows_end = RowTail(tail, tail_ins, tail_outs, sum_ref)
        for g in range(steps):
            for side in range(2):
                copy(2, side, g).wait_recv()
                flag, mine, other = route(side, g)[:3]
                col = (side * steps + g) * tile
                rows_end.tile(slice(col, col + tile), acc[side, g, chip(flag, mine, other)] + recv3[side, g])
        rows_end.end(2 * steps * tile, tile)
        for stage in range(3):
            for g in range(steps):
                for side in range(2):
                    copy(stage, side, g).wait_send()

    if left_count:
        relay_step = 2 if seg else 0

        @pl.when(step < steps)
        def _():
            produce()

        if seg:
            @pl.when(step == relay_step)
            def _():
                gather_relay()
                for g in range(relay_step):
                    chip_sum(g)

        @pl.when((step > relay_step) & (step < steps))
        def _():
            chip_sum(step - 1)

        @pl.when(step == steps - 1)
        def _():
            chip_sum(steps - 1)
    else:
        @pl.when(step == 0)
        def _():
            gather_relay()

    start = steps if left_count else 0
    for n, job in enumerate(jobs):
        @pl.when((step >= start) & (step < start + job.steps))
        def _(job=job, n=n):
            job.compute(job_refs[n], job_outs[n])
        start += job.steps

    if seg:
        @pl.when(step == start)
        def _():
            gather_finish()

        @pl.when(step >= start)
        def _():
            j = step - start
            left = full_ref[:, pl.ds(pl.multiple_of(j * seg.chunk, seg.chunk), seg.chunk)]
            epilogue = seg.body(j, left, seg_ins, seg_outs, seg_scratch, seg.heads)
            if left_count:
                second_link(j)

            @pl.when(j == steps - 1)
            def _():
                epilogue()
        start += steps

    @pl.when(step == start - 1)
    def _():
        if seg:
            pltpu.make_async_copy(full_ref, full_out, out_sem).wait()
        else:
            for g in range(steps):
                second_link(g)
        if left_count:
            finish()


def half_step(lefts, weights, layer_idx, shard, call_id, tail, tail_ins, slots=0, seg=None, rows=None, jobs=(), y_first=5, tile=256):
    width = weights[0].shape[2] if lefts else rows.shape[1]
    steps = width // tile // 2
    seq = lefts[0].shape[0] if lefts else seg.seq
    in_specs = [whole(a.shape) for a in lefts]
    args = list(lefts)
    for w in weights:
        for side in range(2):
            if slots:
                in_specs.append(pl.BlockSpec((1, slots, tile, w.shape[3]),
                                             lambda i, s=side: (layer_idx, 0, s * steps + jnp.minimum(i, steps - 1), 0)))
            else:
                in_specs.append(pl.BlockSpec((1, w.shape[1], tile), lambda i, s=side: (layer_idx, 0, s * steps + jnp.minimum(i, steps - 1))))
            args.append(w)
    in_specs += [whole(a.shape) for a in tail_ins]
    args += list(tail_ins)
    seg_start = (steps if lefts else 0) + sum(job.steps for job in jobs)
    if seg:
        in_specs += [whole(rows.shape)] + seg.specs(lambda i: jnp.clip(i - seg_start, 0, steps - 1))
        args += [rows] + seg.operands
    second = {'none': [], 'add': [], 'norm': [((shard, width), BF)], 'back': [((1, width), F32)]}[tail]
    out_shapes = [jax.ShapeDtypeStruct(*o) for o in ([((shard, width), BF)] if lefts else []) + second]
    out_specs, aliases = [whole_out(o.shape) for o in out_shapes], {}
    if seg:
        out_shapes += [jax.ShapeDtypeStruct((seq, width), BF)] + [jax.ShapeDtypeStruct(*o) for o in seg.outs]
        out_specs += [ANY] + [whole_out(o[0]) for o in seg.outs]
    start = steps
    for job in jobs:
        ins, job_args, out = job.specs(lambda i, start=start, last=job.steps - 1: jnp.clip(i - start, 0, last))
        in_specs += ins
        args += job_args
        if job.stacked is not None:
            aliases[len(args) - 1] = len(out_shapes)
        out_specs.append(out)
        out_shapes.append(jax.ShapeDtypeStruct(job.shape, BF))
        start += job.steps
    big = pltpu.VMEM((2, steps, 4, shard, tile), F32)
    mid = pltpu.VMEM((2, steps, 2, shard, tile), F32)
    small = pltpu.VMEM((2, steps, shard, tile), F32)
    scratch = [pltpu.VMEM(a.shape, BF) for a in lefts]
    if lefts:
        scratch += [big, big, big, mid, mid, small, small, pltpu.VMEM((shard, width), BF), pltpu.SemaphoreType.DMA((6, 2, steps))]
    if seg:
        scratch += [pltpu.VMEM((seq, width), BF), pltpu.SemaphoreType.DMA((2, 13)), pltpu.SemaphoreType.DMA] + seg.scratch
    return pl.pallas_call(
        functools.partial(half_step_kernel, left_count=len(lefts), slots=slots, shard=shard, tile=tile, steps=steps,
                          y_first=y_first, tail=tail, seg=seg, jobs=tuple(jobs)),
        grid=(seg_start + (steps if seg else 0),),
        out_shape=out_shapes,
        in_specs=in_specs,
        out_specs=out_specs,
        input_output_aliases=aliases,
        scratch_shapes=scratch,
        compiler_params=pltpu.CompilerParams(collective_id=call_id, has_side_effects=True, vmem_limit_bytes=67000000),
        name='half_step',
    )(*args)


def solution(mesh):
    row_spec = P(None, ('dp', 'tp'), None)
    gain_spec = P(None, None)
    qkv_spec = P(None, None, 'tp', None, None)
    head_spec = P(None, 'tp', None, None)
    col_spec = P(None, None, 'tp')
    row_shard_spec = P(None, 'tp', None)
    tp = mesh.shape['tp']
    swap = {flip: [(t, t ^ flip) for t in range(tp)] for flip in (1, 2, 4)}

    def device_program(x_in, y_cot, gain_attn, gain_mlp, w_qkv, w_out, w_gate, w_up, w_down):
        micro_count, shard, width = x_in.shape
        layer_count = w_qkv.shape[0]
        groups = w_qkv.shape[3] - 2
        hd = w_qkv.shape[4]
        slots = groups + 2
        wq = jnp.transpose(w_qkv[:, :, 0], (0, 2, 1, 3))
        wo = w_out.reshape(layer_count, groups * hd, width)
        wg, wu = jnp.swapaxes(w_gate, 1, 2), jnp.swapaxes(w_up, 1, 2)

        micros = range(micro_count)
        gain_a, gain_b = gain_attn[:, None], gain_mlp[:, None]
        top = layer_count - 1
        plan = [(kind, l) for l in range(layer_count) for kind in ('qkv_attn', 'gate_up')]
        plan += [(kind, l) for l in reversed(range(layer_count)) for kind in ('inner_grad', 'mix_grad')]
        kept = [[{} for l in range(layer_count)] for m in micros]
        rows_in = [norm_apply(x_in[m], gain_attn[0]) for m in micros]
        for m in micros:
            kept[m][0]['x'] = x_in[m]
        y_rows, grad_x = [None] * micro_count, [None] * micro_count
        gains_a = [[None] * micro_count for l in range(layer_count)]
        gains_b = [[None] * micro_count for l in range(layer_count)]
        stacks = [None] * 5
        waiting = []

        def segment(m, s):
            kind, l = plan[s]
            keep = kept[m][l]
            operands = {'qkv_attn': lambda: [wq], 'gate_up': lambda: [wg, wu], 'inner_grad': lambda: [w_down, keep['gate'], keep['up']],
                        'mix_grad': lambda: [wo, keep['qkv']]}[kind]()
            return Segment(kind, l, shard * tp, groups, hd, operands)

        def store(m, s, full, outs):
            kind, l = plan[s]
            keep = kept[m][l]
            names = {'qkv_attn': ('u', 'qkv', 'mix'), 'gate_up': ('v', 'gate', 'up', 'inner_t', 'inner'),
                     'inner_grad': ('gy', 'gg_t', 'gu_t', 'gg', 'gu'), 'mix_grad': ('gh', 'gq')}[kind]
            keep.update(zip(names, [full] + list(outs)))
            if m == micro_count - 1 and kind == 'inner_grad':
                for which, left, right in ((2, 'gg_t', 'v'), (3, 'gu_t', 'v'), (4, 'inner_t', 'gy')):
                    waiting.append((which, [kept[i][l][left] for i in micros], [kept[i][l][right] for i in micros], l, 0, True))
            if m == micro_count - 1 and kind == 'mix_grad':
                waiting.append((1, [kept[i][l]['mix'] for i in micros], [kept[i][l]['gh'] for i in micros], l))
                waiting.append((0, [kept[i][l]['u'] for i in micros], [kept[i][l]['gq'] for i in micros], l, slots))

        def scatter(call, m, s, next_m, next_s, job_count):
            kind, l = plan[s]
            keep = kept[m][l]
            lefts, weights, slot_count = {'qkv_attn': ([keep.get('mix')], [wo], 0), 'gate_up': ([keep.get('inner')], [w_down], 0),
                                          'inner_grad': ([keep.get('gg'), keep.get('gu')], [wg, wu], 0),
                                          'mix_grad': ([keep.get('gq')], [wq], slots)}[kind]
            if kind == 'qkv_attn':
                tail, tail_ins = 'norm', [keep['x'], gain_b[l]]
            elif kind == 'gate_up' and l < top:
                tail, tail_ins = 'norm', [keep['h'], gain_a[l + 1]]
            elif kind == 'gate_up':
                tail, tail_ins = 'add', [keep['h']]
            elif kind == 'inner_grad':
                tail, tail_ins = 'back', [rows_in[m], keep['h'], gain_b[l]]
            else:
                tail, tail_ins = 'back', [rows_in[m], keep['x'], gain_a[l]]
            seg = segment(next_m, next_s) if next_m is not None else None
            picked = [waiting.pop(0) for i in range(min(job_count, len(waiting)))]
            jobs = [WeightGrad(p[1], p[2], None, 0, 1, *p[4:]) for p in picked]
            outs = half_step(lefts, weights, l, shard, call, tail, tail_ins, slot_count, seg,
                             rows_in[next_m] if seg else None, jobs)
            head, outs = outs[:TAIL_OUTS[tail]], outs[TAIL_OUTS[tail]:]
            if seg:
                seg_outs, outs = outs[:1 + len(seg.outs)], outs[1 + len(seg.outs):]
                store(next_m, next_s, seg_outs[0], seg_outs[1:])
            for p, arr in zip(picked, outs):
                stacks[p[0]] = arr
            if kind == 'qkv_attn':
                keep['h'], rows_in[m] = head
            elif kind == 'gate_up' and l < top:
                kept[m][l + 1]['x'], rows_in[m] = head
            elif kind == 'gate_up':
                y_rows[m], rows_in[m] = head[0], y_cot[m]
            else:
                rows_in[m] = head[0]
                (gains_b if kind == 'inner_grad' else gains_a)[l][m] = head[1]
                grad_x[m] = head[0]

        first_full, *first_outs = half_step([], [], 0, shard, micro_count * len(plan) + 1, 'none', [], 0, segment(0, 0), rows_in[0])
        store(0, 0, first_full, first_outs)
        job_counts = {10: 1, 11: 1, 14: 1, 15: 2}
        total = micro_count * len(plan)
        for call in range(total):
            m, s = call % micro_count, call // micro_count
            next_m, next_s = (call + 1) % micro_count, (call + 1) // micro_count
            scatter(call + 1, m, s, next_m if call + 1 < total else None, next_s, job_counts.get(call, 0))
        gains_a = [sum(parts[1:], parts[0]) for parts in gains_a]
        gains_b = [sum(parts[1:], parts[0]) for parts in gains_b]
        gains = jnp.concatenate(gains_a + gains_b)
        flips = [1, 2, 4]
        for n, p in enumerate(waiting):
            tokens = [gains] if n and flips else []
            stacks[p[0]] = weight_grad_stack(WeightGrad(p[1], p[2], None, 0, 1, *p[4:]), stacks[p[0]], tokens)
            if n % 2 == 0 and flips:
                gains = gains + lax.ppermute(gains, 'tp', swap[flips.pop(0)])
        for flip in flips:
            gains = gains + lax.ppermute(gains, 'tp', swap[flip])
        return (jnp.stack(y_rows), jnp.stack(grad_x), jnp.transpose(stacks[0], (0, 2, 1, 3))[:, :, None], stacks[1].reshape(w_out.shape),
                jnp.swapaxes(stacks[2], 1, 2), jnp.swapaxes(stacks[3], 1, 2), stacks[4], gains[:layer_count], gains[layer_count:])

    return jax.shard_map(device_program, mesh=mesh,
                         in_specs=(row_spec, row_spec, gain_spec, gain_spec, qkv_spec, head_spec, col_spec, col_spec, row_shard_spec),
                         out_specs=(row_spec, row_spec, P('dp', None, 'tp', None, None), P('dp', 'tp', None, None), P('dp', None, 'tp'), P('dp', None, 'tp'), P('dp', 'tp', None), P('dp', None), P('dp', None)),
                         check_vma=False)
```
